32 devices in a mesh: sub: 8 (over z, x), slab: 4 (over y, core).
Axes of the slice: x: 2, y: 2, z: 4, core: 2. Of those that a mesh axis runs over, the one named last changes fastest.
Arguments:
- residual: float32 [8, 4, 128, 1024], P('sub', 'slab'), may hold values from -6 to 6
- inverse_slab: float32 [8, 4, 1024, 1024], P('sub', 'slab'), may hold values from -1 to 2, as said below
- diagonal: float32 [8, 4, 1024], P('sub', 'slab'), may hold values from 0.2 to 0.6
- primal_index: int32 [8, 4, 32], P('sub', 'slab'), may hold values from 0 to 1023
- coarse_map: int32 [8, 32], P('sub'), may hold values from 0 to 127
- schur_small: float32 [8, 32, 32], P('sub'), may hold values from -1 to 2, as said below
- constraint_basis: float32 [8, 4, 32, 1024], P('sub', 'slab'), may hold values from -0.75 to 0.75
- coarse_basis: float32 [8, 4, 32, 1024], P('sub', 'slab'), may hold values from -0.75 to 0.75
- coarse_inverse: float32 [128, 128], P(None, 'sub'), may hold values from -1 to 2, as said below
Outputs:
- preconditioned: float32 [8, 4, 128, 1024], P('sub', 'slab')
The draws below stay inside these ranges and needn't reach their ends.
Inputs may be any that keep to these rules, and one draw needn't show every extreme that they name: `inverse_slab`: A diagonal near 0.5 with full off-diagonal entries of moderate size. `schur_small`: A diagonal near 1 with full off-diagonal entries of moderate size. `coarse_inverse`: A diagonal near 1 with full off-diagonal entries of moderate size.
All inputs are finite; a program needn't handle non-finite values.
Results may differ from the reference program's by a relative error of at most 0.0001.
Values sent between devices are 32-bit elements; how exact they have to be, the bound alone decides.
No kernel may reach another device: no remote copies, remote signals or barrier semaphores. Data moves between devices by JAX's collectives and lax.ppermute only.
A program may use at most 64 MiB of HBM per device.

```python
import math
import jax
import jax.numpy as jnp
from jax import lax

CXY = 32
RHS = 128
PRIM = 32
IFACE = 1024
SUBS = 8
SLABS = 4
NCOARSE = 128


def dominant(key, leading, order, spread):
    shape = leading + (order, order)
    noise = jnp.clip(jax.random.normal(key, shape, jnp.float32), -4.0, 4.0)
    return jnp.eye(order, dtype=jnp.float32) + spread * noise / math.sqrt(order)


def draw_inverse_slab(key, part):
    return 0.5 * dominant(jax.random.fold_in(key, 11), (SUBS, SLABS), CXY * CXY, 0.6)


def draw_schur_small(key, part):
    return dominant(jax.random.fold_in(key, 23), (SUBS,), PRIM, 0.6)


def draw_coarse_inverse(key, part):
    return dominant(jax.random.fold_in(key, 37), (), NCOARSE, 0.6)


def with_ends(entries, stream_key, low, top_value):
    extent = entries.shape
    spot = [jax.random.randint(jax.random.fold_in(stream_key, axis), (), 0, extent[axis]) for axis in range(len(extent))]
    entries = entries.at[tuple(spot)].set(low)
    longest = extent.index(max(extent))
    spot[longest] = (spot[longest] + 1) % extent[longest]
    return entries.at[tuple(spot)].set(top_value)


def level_of(own_key, shape, pieces, smallest, high):
    gain, own = 1.0, jax.random.fold_in(own_key, 6)
    for axis_at, parts in pieces:
        draws = jnp.exp(jax.random.uniform(jax.random.fold_in(own, axis_at), (parts,), jnp.float32, smallest / len(pieces), high / len(pieces)))
        gain = gain * jnp.repeat(draws, shape[axis_at] // parts).reshape([-1 if axis == axis_at else 1 for axis in range(len(shape))])
    return gain


def normal_values(key, dims, scale, most, shards=(), kind=jnp.bfloat16):
    values = scale * jax.random.normal(key, dims, jnp.float32)
    if shards:
        values = values * level_of(key, dims, shards, -0.22, 0.18)
    return jnp.clip(values, -most, most).astype(kind)


def setup_inputs(seed: int = 0) -> dict:
    seeds = jax.random.split(jax.random.key(seed), 10)
    residual = normal_values(seeds[0], (SUBS, SLABS, RHS, IFACE), 1.0, 6.0, ((0, 8), (1, 4)), jnp.float32)
    inverse_slab = draw_inverse_slab(jax.random.fold_in(seeds[9], 71), 0)
    diagonal = jnp.clip(0.2 + 0.400000021 * jax.random.uniform(seeds[2], (SUBS, SLABS, IFACE), jnp.float32) ** level_of(seeds[2], (SUBS, SLABS, IFACE), ((0, 8), (1, 4)), -0.2, 0.2), 0.2, 0.6)
    primal_index = with_ends(jax.random.randint(seeds[3], (SUBS, SLABS, PRIM), 0, IFACE), jax.random.fold_in(seeds[3], 1), 0, IFACE - 1).astype(jnp.int32)
    coarse_map = with_ends(jax.random.randint(seeds[4], (SUBS, PRIM), 0, NCOARSE), jax.random.fold_in(seeds[4], 1), 0, NCOARSE - 1).astype(jnp.int32)
    schur_small = draw_schur_small(jax.random.fold_in(seeds[9], 71), 0)
    constraint_basis = normal_values(seeds[6], (SUBS, SLABS, PRIM, IFACE), 0.05, 0.75, ((0, 8), (1, 4)), jnp.float32)
    coarse_basis = normal_values(seeds[7], (SUBS, SLABS, PRIM, IFACE), 0.05, 0.75, ((0, 8), (1, 4)), jnp.float32)
    coarse_inverse = draw_coarse_inverse(jax.random.fold_in(seeds[9], 71), 0)
    return dict(residual=residual, inverse_slab=inverse_slab, diagonal=diagonal, primal_index=primal_index, coarse_map=coarse_map, schur_small=schur_small, constraint_basis=constraint_basis, coarse_basis=coarse_basis, coarse_inverse=coarse_inverse)


highest = lax.Precision.HIGHEST


def slab_times(vector, matrix):
    return jnp.einsum('srw,swv->srv', vector, matrix, precision=highest)


def apply_once(vector, inverse_slab, primal_index, coarse_map, schur_small, constraint_basis, coarse_basis, coarse_inverse):
    forward = []
    carried = jnp.zeros_like(vector[:, 0])
    for level in range(SLABS):
        carried = slab_times(vector[:, level] + carried, inverse_slab[:, level])
        forward.append(carried)
    backward = [None] * SLABS
    carried = jnp.zeros_like(vector[:, 0])
    for level in reversed(range(SLABS)):
        carried = forward[level] + slab_times(carried, inverse_slab[:, level])
        backward[level] = carried
    neumann = jnp.stack(backward, axis=1)
    picks = jnp.take_along_axis(neumann, primal_index[:, :, None, :].astype(jnp.int32), axis=3)
    primal = jnp.sum(picks, axis=1)
    multiplier = jnp.einsum('srp,spq->srq', primal, schur_small, precision=highest)
    constrained = neumann - jnp.einsum('srp,skpw->skrw', multiplier, constraint_basis, precision=highest)
    onehot = (coarse_map[:, :, None] == jnp.arange(NCOARSE, dtype=jnp.int32)[None, None, :]).astype(jnp.float32)
    coarse_rhs = jnp.einsum('srp,spn->rn', primal, onehot, precision=highest)
    coarse_sol = jnp.dot(coarse_rhs, coarse_inverse, precision=highest)
    picked = jnp.einsum('rn,spn->srp', coarse_sol, onehot, precision=highest)
    return constrained + jnp.einsum('srp,skpw->skrw', picked, coarse_basis, precision=highest)


def reference(residual, inverse_slab, diagonal, primal_index, coarse_map, schur_small, constraint_basis, coarse_basis, coarse_inverse):
    first_pass = apply_once(residual, inverse_slab, primal_index, coarse_map, schur_small, constraint_basis, coarse_basis, coarse_inverse)
    defect = residual - diagonal[:, :, None, :] * first_pass
    second_pass = apply_once(defect, inverse_slab, primal_index, coarse_map, schur_small, constraint_basis, coarse_basis, coarse_inverse)
    return first_pass + second_pass
```

```python
import functools

import jax
import jax.numpy as jnp
from jax import lax
from jax.experimental import pallas as pl
from jax.experimental.pallas import tpu as pltpu
from jax.sharding import PartitionSpec as P


f32 = jnp.float32
bf16 = jnp.bfloat16
highest = lax.Precision.HIGHEST
LANES = 128
BLOCKS = 2
PIECES = 4


def halves(x):
    top = x.astype(bf16)
    return top, (x - top.astype(f32)).astype(bf16)


def dot(left, right):
    return jnp.dot(left, right, preferred_element_type=f32)


def times(x, weights, member):
    rows = x.shape[0]
    top, low = halves(x)
    both = dot(jnp.concatenate([top, low], axis=0), weights[member, 0])
    return both[:rows] + both[rows:] + dot(top, weights[member, 1])


def vmem():
    return pl.BlockSpec(memory_space=pltpu.VMEM)


def smem():
    return pl.BlockSpec(memory_space=pltpu.SMEM)


def call(body, outs, args, name, products=0.0, rows=1, aliases=None, scratch=(), spaces=None, width=1024):
    specs = [smem()] + [vmem() for _ in args[1:]]
    for place, space in (spaces or {}).items():
        specs[place] = pl.BlockSpec(memory_space=space)
    return pl.pallas_call(
        body,
        out_shape=outs,
        in_specs=specs,
        out_specs=[vmem() for _ in outs],
        input_output_aliases=aliases or {},
        scratch_shapes=list(scratch),
        cost_estimate=pl.CostEstimate(
            flops=int(6 * products * max(rows, 128) * width * width), bytes_accessed=0, transcendentals=0
        ),
        compiler_params=pltpu.CompilerParams(vmem_limit_bytes=24 << 20),
        name=name,
    )(*args)


def struct(shape, dtype=f32):
    return jax.ShapeDtypeStruct(shape, dtype)


def split_own(scal, matrix, vector, basis, aux, weights, keep, send, buffer, total, sems):
    member = scal[0]
    size = matrix.shape[0]
    step = size // PIECES
    copies = [
        pltpu.make_async_copy(
            matrix.at[pl.ds(i * step, step)], buffer.at[pl.ds(i * step, step)], sems.at[i]
        )
        for i in range(PIECES)
    ]
    for copy in copies:
        copy.start()
    rows, extra = vector.shape[0], basis.shape[0]
    for i, copy in enumerate(copies):
        cols = pl.ds(i * step, step)
        copy.wait()
        top, low = halves(buffer[cols, :])
        weights[0, cols, :] = top
        weights[1, cols, :] = low
        x = jnp.concatenate([vector[:, cols], basis[:, cols] * aux[0:1, cols]], axis=0)
        xt, xl = halves(x)
        both = dot(jnp.concatenate([xt, xl], axis=0), weights[0, cols, :])
        part = both[: rows + extra] + both[rows + extra :] + dot(xt, weights[1, cols, :])
        if i == 0:
            total[...] = part
        else:
            total[...] += part
    half, few = rows // 2, extra // 2
    other = 1 - member
    keep[0:half, :] = total[pl.ds(pl.multiple_of(member * half, 8), half), :]
    keep[half : half + few, :] = total[pl.ds(pl.multiple_of(rows + member * few, 8), few), :]
    send[0:half, :] = total[pl.ds(pl.multiple_of(other * half, 8), half), :]
    send[half : half + few, :] = total[pl.ds(pl.multiple_of(rows + other * few, 8), few), :]


def split_other(scal, *refs):
    pieces, own, weights = refs[:PIECES], refs[PIECES], refs[-1]
    other = 1 - scal[0]
    weights[scal[0]] = own[...]
    step = pieces[0].shape[0]
    for i, piece in enumerate(pieces):
        top, low = halves(piece[...])
        weights[other, 0, pl.ds(i * step, step), :] = top
        weights[other, 1, pl.ds(i * step, step), :] = low


def hold(idle, before, after):
    @pl.when(idle)
    def _():
        for old, new in zip(before, after):
            new[...] = old[...]


def pick(scal, own, oth):
    first = scal[0] == 0
    return jnp.where(first, own, oth), jnp.where(first, oth, own)


def chosen(n_first, n_second, scal, own_aux, oth_aux):
    size = n_first.shape[1]
    i_first, i_second = pick(scal, own_aux[1:2, :LANES], oth_aux[1:2, :LANES])
    place = lax.broadcasted_iota(jnp.int32, (size, LANES), 0).astype(f32)
    out = 0.0
    for n, i in ((n_first, i_first), (n_second, i_second)):
        spots = (place == i).astype(f32).astype(bf16)
        top, low = halves(n)
        both = dot(jnp.concatenate([top, low], axis=0), spots)
        out = out + both[: n.shape[0]] + both[n.shape[0] :]
    return out


def start_chain(at, scal, keep, recv, weights, f_first, f_second):
    rows = f_first.shape[0]

    @pl.when(scal[1] == 0)
    def _():
        first, second = pick(scal, keep[at : at + rows, :], recv[at : at + rows, :])
        f_first[...] = first
        f_second[...] = second + times(first, weights, 1)


def forward(at, position, scal, keep, recv, carried, weights, old_first, old_second, f_first, f_second):
    rows = f_first.shape[0]

    @pl.when(scal[1] == position)
    def _():
        first, second = pick(scal, keep[at : at + rows, :], recv[at : at + rows, :])
        first = first + times(carried[...], weights, 0)
        f_first[...] = first
        f_second[...] = second + times(first, weights, 1)

    hold(scal[1] != position, (old_first, old_second), (f_first, f_second))


def top_first(at, scal, keep, recv, carried, weights, own_aux, oth_aux, n_first, n_second, values):
    rows = n_first.shape[0]

    @pl.when(scal[1] == scal[2])
    def _():
        first, second = pick(scal, keep[at : at + rows, :], recv[at : at + rows, :])
        first = first + times(carried[...], weights, 0)
        second = second + times(first, weights, 1)
        first = first + times(second, weights, 0)
        n_second[...] = second
        n_first[...] = first
        values[...] = chosen(first, second, scal, own_aux, oth_aux)


def forward_second(position, scal, v_first, v_second, carried, weights, own_aux, oth_aux, old_first, old_second, f_first, f_second):
    @pl.when(scal[1] == position)
    def _():
        d_first, d_second = pick(scal, own_aux[0:1, :], oth_aux[0:1, :])
        first = times(d_first * v_first[...] + carried[...], weights, 0)
        f_first[...] = first
        f_second[...] = times(d_second * v_second[...] + first, weights, 1)

    hold(scal[1] != position, (old_first, old_second), (f_first, f_second))


def top_second(scal, v_first, v_second, carried, weights, own_aux, oth_aux, n_first, n_second, values):
    @pl.when(scal[1] == scal[2])
    def _():
        d_first, d_second = pick(scal, own_aux[0:1, :], oth_aux[0:1, :])
        first = times(d_first * v_first[...] + carried[...], weights, 0)
        second = times(d_second * v_second[...] + first, weights, 1)
        first = first + times(second, weights, 0)
        n_second[...] = second
        n_first[...] = first
        values[...] = chosen(first, second, scal, own_aux, oth_aux)


def back(position, scal, f_first, f_second, carried, weights, own_aux, oth_aux, *refs):
    n_first, n_second, values = refs[3:]

    @pl.when(scal[1] == position)
    def _():
        second = f_second[...] + times(carried[...], weights, 1)
        first = f_first[...] + times(second, weights, 0)
        n_second[...] = second
        n_first[...] = first
        values[...] = chosen(first, second, scal, own_aux, oth_aux)

    hold(scal[1] != position, refs[:3], refs[3:])


def turn(scal, f_first, f_second, carried, weights, own_aux, oth_aux, *refs):
    n_first, n_second, values, g_first, g_second = refs[3:]

    @pl.when(scal[1] == 0)
    def _():
        second = f_second[...] + times(carried[...], weights, 1)
        first = f_first[...] + times(second, weights, 0)
        n_second[...] = second
        n_first[...] = first
        d_first, d_second = pick(scal, own_aux[0:1, :], oth_aux[0:1, :])
        again = times(d_first * first, weights, 0)
        g_first[...] = again
        g_second[...] = times(d_second * second + again, weights, 1)
        values[...] = chosen(first, second, scal, own_aux, oth_aux)

    hold(scal[1] != 0, refs[:3], refs[3:6])


def combine(scal, q, own_first, own_second, oth_first, oth_second, *refs):
    blocks = refs[: 4 * BLOCKS]
    keep, send = refs[4 * BLOCKS :]
    rows = blocks[0].shape[0]
    first = scal[0] == 0
    top, low = halves(q[...])
    parts = []
    for own, oth in ((own_first, oth_first), (own_second, oth_second)):
        k_low = jnp.where(first, own[...], oth[...])
        k_high = jnp.where(first, oth[...], own[...])
        kt, kl = halves(jnp.concatenate([k_low, k_high], axis=0))
        parts.append(dot(top, kt) + dot(low, kt) + dot(top, kl))
    for i in range(BLOCKS):
        a1, b1, a2, b2 = (r[...] for r in blocks[4 * i : 4 * i + 4])
        here = slice(i * rows, (i + 1) * rows)
        a = 2.0 * a1 - a2 - parts[0][here]
        b = 2.0 * b1 - b2 - parts[1][here]
        keep[here, :] = jnp.where(first, a, b)
        send[here, :] = jnp.where(first, b, a)


def finish(scal, keep, recv, q_keep, q_recv, basis, out):
    rows = keep.shape[0]
    bt, bl = halves(basis[...])
    for n, q, which in ((keep, q_keep, scal[0]), (recv, q_recv, 1 - scal[0])):
        top, low = halves(q[...])
        out[pl.ds(pl.multiple_of(which * rows, 8), rows), :] = n[...] + (
            dot(top, bt) + dot(low, bt) + dot(top, bl)
        )


def product(left, right):
    return jnp.dot(left, right, precision=highest, preferred_element_type=f32)


def sum_over(x, axis):
    count = lax.axis_size(axis)
    if count & (count - 1):
        return lax.psum(x, axis)
    distance = 1
    while distance < count:
        x = x + lax.ppermute(x, axis, [(i, i ^ distance) for i in range(count)])
        distance *= 2
    return x


def on_device(
    residual,
    inverse_slab,
    diagonal,
    primal_index,
    coarse_map,
    schur_small,
    constraint_basis,
    coarse_basis,
    coarse_inverse,
):
    levels = lax.axis_size("slab")
    assert levels % 2 == 0 and levels >= 4
    groups = levels // 2
    slab = lax.axis_index("slab")
    scal = jnp.stack([slab % 2, slab // 2, jnp.full_like(slab, groups - 1)]).astype(jnp.int32)
    partner = [(i, i ^ 1) for i in range(levels)]

    def swap(x):
        return lax.ppermute(x, "slab", partner)

    def hop(x, source, target):
        return lax.ppermute(x, "slab", [(2 * source + i, 2 * target + i) for i in range(2)])

    def over_groups(x):
        out = x
        for by in range(1, groups):
            pairs = [(i, (i + 2 * by) % levels) for i in range(levels)]
            out = out + lax.ppermute(x, "slab", pairs)
        return out

    vector = residual[0, 0]
    matrix = inverse_slab[0, 0]
    rows, size = vector.shape
    prim = primal_index.shape[-1]
    coarse_count = coarse_inverse.shape[0]
    assert prim <= LANES and size >= LANES and size % PIECES == 0
    half = rows // 2
    block = half // BLOCKS
    basis = jnp.concatenate([-constraint_basis[0, 0], coarse_basis[0, 0]], axis=0)
    extra = basis.shape[0]
    few = extra // 2

    step = size // PIECES
    pieces = [swap(matrix[i * step : (i + 1) * step]) for i in range(PIECES)]
    spots = jnp.full((size,), -1.0, f32).at[:prim].set(primal_index[0, 0].astype(f32))
    own_aux = jnp.stack([diagonal[0, 0], spots])
    oth_aux = swap(own_aux)

    own, keep, send = call(
        split_own,
        [struct((2, size, size), bf16), struct((half + few, size)), struct((half + few, size))],
        [scal, matrix, vector, basis, own_aux],
        "split_own",
        products=1,
        rows=rows + extra,
        scratch=[
            pltpu.VMEM((size, size), f32),
            pltpu.VMEM((rows + extra, size), f32),
            pltpu.SemaphoreType.DMA((PIECES,)),
        ],
        spaces={1: pltpu.HBM},
    )
    recv = swap(send)
    (weights,) = call(
        split_other,
        [struct((2, 2, size, size), bf16)],
        [scal, *pieces, own],
        "split_other",
        products=0.5,
    )

    share = coarse_inverse.shape[1]
    sub = lax.axis_index("sub")
    whole = lax.dynamic_update_slice(
        jnp.zeros((coarse_count, coarse_count), f32), coarse_inverse.T, (sub * share, 0)
    )
    inverse_whole = sum_over(whole, "sub").T
    onehot = (coarse_map[0][:, None] == jnp.arange(coarse_count, dtype=jnp.int32)[None, :]).astype(f32)
    schur = schur_small[0]

    starts = [i * block for i in range(BLOCKS)] + [half]
    sizes = [block] * BLOCKS + [few]
    count = len(starts)

    def shapes(i, k):
        return [struct((sizes[i], size))] * k

    f = [
        call(
            functools.partial(start_chain, starts[i]),
            shapes(i, 2),
            [scal, keep, recv, weights],
            "start_chain",
            products=1,
        )
        for i in range(count)
    ]
    carried = [hop(f[i][1], 0, 1) for i in range(count)]
    for g in range(1, groups - 1):
        f = [
            call(
                functools.partial(forward, starts[i], g),
                shapes(i, 2),
                [scal, keep, recv, carried[i], weights, *f[i]],
                "forward",
                products=2,
                aliases={5: 0, 6: 1},
            )
            for i in range(count)
        ]
        carried = [hop(f[i][1], g, g + 1) for i in range(count)]
    n = [
        call(
            functools.partial(top_first, starts[i]),
            shapes(i, 2) + [struct((sizes[i], LANES))],
            [scal, keep, recv, carried[i], weights, own_aux, oth_aux],
            "top_first",
            products=3,
        )
        for i in range(count)
    ]
    carried = [hop(n[i][0], groups - 1, groups - 2) for i in range(count)]

    def go_back(g, f, carried, n, i):
        return call(
            functools.partial(back, g),
            shapes(i, 2) + [struct((sizes[i], LANES))],
            [scal, *f, carried, weights, own_aux, oth_aux, *n],
            "back",
            products=2,
            aliases={7: 0, 8: 1, 9: 2},
        )

    for g in range(groups - 2, 0, -1):
        n = [go_back(g, f[i], carried[i], n[i], i) for i in range(count)]
        carried = [hop(n[i][0], g, g - 1) for i in range(count)]
    turned = [
        call(
            turn,
            shapes(i, 2) + [struct((sizes[i], LANES))] + shapes(i, 2),
            [scal, *f[i], carried[i], weights, own_aux, oth_aux, *n[i]],
            "turn",
            products=4,
            aliases={7: 0, 8: 1, 9: 2},
        )
        for i in range(BLOCKS)
    ]
    n_one = [t[:3] for t in turned]
    g_two = [t[3:] for t in turned]
    carried_two = [hop(g_two[i][1], 0, 1) for i in range(BLOCKS)]
    last = count - 1
    k_own = go_back(0, f[last], carried[last], n[last], last)
    k_oth = [swap(k) for k in k_own[:2]]

    def solve(values):
        rhs = sum_over(product(values, onehot), "sub")
        picked = product(product(rhs, inverse_whole), onehot.T)
        return jnp.concatenate([product(values, schur), picked], axis=1)

    p_one = over_groups(jnp.concatenate([t[2] for t in n_one], axis=0))[:, :prim]
    q_one = solve(p_one)
    x_own = over_groups(k_own[2])
    x_oth = swap(x_own)
    low = jnp.where(scal[0] == 0, x_own, x_oth)
    high = jnp.where(scal[0] == 0, x_oth, x_own)
    x_whole = jnp.concatenate([low, high], axis=0)[:, :prim]
    p_shift = p_one - product(q_one, x_whole)

    for g in range(1, groups - 1):
        g_two = [
            call(
                functools.partial(forward_second, g),
                shapes(i, 2),
                [scal, *n_one[i][:2], carried_two[i], weights, own_aux, oth_aux, *g_two[i]],
                "forward_second",
                products=2,
                aliases={7: 0, 8: 1},
            )
            for i in range(BLOCKS)
        ]
        carried_two = [hop(g_two[i][1], g, g + 1) for i in range(BLOCKS)]
    n_two = [
        call(
            top_second,
            shapes(i, 2) + [struct((sizes[i], LANES))],
            [scal, *n_one[i][:2], carried_two[i], weights, own_aux, oth_aux],
            "top_second",
            products=3,
        )
        for i in range(BLOCKS)
    ]
    carried_two = [hop(n_two[i][0], groups - 1, groups - 2) for i in range(BLOCKS)]
    for g in range(groups - 2, 0, -1):
        n_two = [go_back(g, g_two[i], carried_two[i], n_two[i], i) for i in range(BLOCKS)]
        carried_two = [hop(n_two[i][0], g, g - 1) for i in range(BLOCKS)]
    n_two = [go_back(0, g_two[i], carried_two[i], n_two[i], i) for i in range(BLOCKS)]

    p_two = p_shift - over_groups(jnp.concatenate([t[2] for t in n_two], axis=0))[:, :prim]
    q_sum = q_one + solve(p_two)
    q_recv = swap(q_sum)

    parts = []
    for i in range(BLOCKS):
        parts += [*n_one[i][:2], *n_two[i][:2]]
    kept, sent = call(
        combine,
        [struct((half, size)), struct((half, size))],
        [scal, q_one, *k_own[:2], *k_oth, *parts],
        "combine",
        products=0.2,
    )
    (out,) = call(
        finish,
        [struct((rows, size))],
        [scal, kept, swap(sent), q_sum, q_recv, basis],
        "finish",
        products=0.2,
    )
    return out[None, None]


def solution(mesh):
    placed = (
        P("sub", "slab", None, None),
        P("sub", "slab", None, None),
        P("sub", "slab", None),
        P("sub", "slab", None),
        P("sub", None),
        P("sub", None, None),
        P("sub", "slab", None, None),
        P("sub", "slab", None, None),
        P(None, "sub"),
    )
    return jax.shard_map(
        on_device,
        mesh=mesh,
        in_specs=placed,
        out_specs=P("sub", "slab", None, None),
        check_vma=False,
    )
```

```python
import functools

import jax
import jax.numpy as jnp
from jax import lax
from jax.experimental import pallas as pl
from jax.experimental.pallas import tpu as pltpu
from jax.sharding import PartitionSpec as P


f32 = jnp.float32
bf16 = jnp.bfloat16
highest = lax.Precision.HIGHEST
LANES = 128
BLOCKS = 2
PIECES = 4


def halves(x):
    top = x.astype(bf16)
    return top, (x - top.astype(f32)).astype(bf16)


def dot(left, right):
    return jnp.dot(left, right, preferred_element_type=f32)


def dot_rows(left, right):
    return lax.dot_general(left, right, (((1,), (1,)), ((), ())), preferred_element_type=f32)


def three(x, top_right, low_right, how=dot):
    rows = x.shape[0]
    top, low = halves(x)
    both = how(jnp.concatenate([top, low], axis=0), top_right)
    return both[:rows] + both[rows:] + how(top, low_right)


def times(x, weights, member):
    return three(x, weights[member, 0], weights[member, 1])


def times_transposed(x, weights, member):
    return three(x, weights[member, 0], weights[member, 1], dot_rows)


def spec(space):
    return pl.BlockSpec(memory_space=space)


def call(body, outs, args, work, aliases=None, scratch=(), hbm=()):
    specs = [spec(pltpu.SMEM)] + [spec(pltpu.VMEM) for _ in args[1:]]
    args = list(args)
    for place in hbm:
        specs[place] = spec(pltpu.HBM)
        args[place] = pltpu.with_memory_space_constraint(args[place], pltpu.HBM)
    return pl.pallas_call(
        body,
        out_shape=outs,
        in_specs=specs,
        out_specs=[spec(pltpu.VMEM) for _ in outs],
        input_output_aliases=aliases or {},
        scratch_shapes=list(scratch),
        cost_estimate=pl.CostEstimate(flops=int(work * 8e8), bytes_accessed=0, transcendentals=0),
        compiler_params=pltpu.CompilerParams(vmem_limit_bytes=VMEM_LIMIT),
    )(*args)


VMEM_LIMIT = 20 << 20


def struct(shape, dtype=f32):
    return jax.ShapeDtypeStruct(shape, dtype)


def pick(scal, own, oth):
    first = scal[0] == 0
    return jnp.where(first, own, oth), jnp.where(first, oth, own)


def hold(idle, before, after):
    @pl.when(idle)
    def _():
        for old, new in zip(before, after):
            new[...] = old[...]


def split_own(scal, matrix, vector, one, two, aux, own, keep, send, buffer, x, total, sems):
    member = scal[0]
    size = matrix.shape[0]
    step = size // PIECES
    rows, prim = vector.shape[0], one.shape[0]
    copies = [
        pltpu.make_async_copy(vector, x.at[pl.ds(0, rows)], sems.at[0]),
        pltpu.make_async_copy(one, x.at[pl.ds(rows, prim)], sems.at[1]),
        pltpu.make_async_copy(two, x.at[pl.ds(rows + prim, prim)], sems.at[2]),
    ]
    pieces = [
        pltpu.make_async_copy(
            matrix.at[pl.ds(i * step, step)], buffer.at[pl.ds(i * step, step)], sems.at[3 + i]
        )
        for i in range(PIECES)
    ]
    for copy in copies + pieces:
        copy.start()
    for copy in copies:
        copy.wait()
    x[rows:, :] = x[rows:, :] * aux[0:1, :]
    for i, copy in enumerate(pieces):
        cols = pl.ds(i * step, step)
        copy.wait()
        top, low = halves(buffer[cols, :])
        own[0, cols, :] = top
        own[1, cols, :] = low
        part = three(x[:, cols], own[0, cols, :], own[1, cols, :])
        if i == 0:
            total[...] = part
        else:
            total[...] += part
    half = rows // 2
    keep[:half, :] = total[pl.ds(pl.multiple_of(member * half, 8), half), :]
    send[:half, :] = total[pl.ds(pl.multiple_of((1 - member) * half, 8), half), :]
    keep[half:, :] = total[rows:, :]
    send[half:, :] = total[rows:, :]


def split_other(scal, matrix, own, weights):
    other = 1 - scal[0]
    weights[scal[0]] = own[...]
    top, low = halves(matrix[...])
    weights[other, 0] = top
    weights[other, 1] = low


def start_chain(at, scal, keep, recv, weights, f_first, f_second):
    rows = f_first.shape[0]

    @pl.when(scal[1] == 0)
    def _():
        first, second = pick(scal, keep[at : at + rows, :], recv[at : at + rows, :])
        f_first[...] = first
        f_second[...] = second + times(first, weights, 1)


def start_basis(at, scal, keep, recv, weights, f_first, f_second, part):
    rows, few = f_first.shape[0], part.shape[0]

    @pl.when(scal[1] == 0)
    def _():
        first, second = pick(scal, keep[at : at + rows, :], recv[at : at + rows, :])
        f_first[...] = first
        f_second[...] = second + times(first, weights, 1)
        part[...] = f_second[pl.ds(pl.multiple_of(scal[0] * few, 8), few), :]


def up(first, second, weights):
    second = second + times(first, weights, 1)
    return first + times(second, weights, 0), second


def top_one(at, scal, keep, recv, carried, weights, n_first, n_second):
    rows = n_first.shape[0]

    @pl.when(scal[1] == 1)
    def _():
        first, second = pick(scal, keep[at : at + rows, :], recv[at : at + rows, :])
        n_first[...], n_second[...] = up(first + times(carried[...], weights, 0), second, weights)


def top_basis(at, scal, keep, recv, carried, weights, n_first, n_second):
    few = n_first.shape[0]

    @pl.when(scal[1] == 1)
    def _():
        here = pl.ds(pl.multiple_of(at + scal[0] * few, 8), few)
        first, second = pick(scal, keep[here, :], recv[here, :])
        n_first[...], n_second[...] = up(first + times(carried[...], weights, 0), second, weights)


def top_two(scal, v_first, v_second, carried, weights, own_aux, oth_aux, n_first, n_second):
    @pl.when(scal[1] == 1)
    def _():
        d_first, d_second = pick(scal, own_aux[0:1, :], oth_aux[0:1, :])
        first = times(d_first * v_first[...] + carried[...], weights, 0)
        second = times(d_second * v_second[...] + first, weights, 1)
        n_first[...] = first + times(second, weights, 0)
        n_second[...] = second


def down(f_first, f_second, carried, weights):
    second = f_second + times(carried, weights, 1)
    return f_first + times(second, weights, 0), second


def turn(scal, f_first, f_second, carried, weights, own_aux, oth_aux, *refs):
    old, (n_first, n_second, g_first, g_second) = refs[:2], refs[2:]

    @pl.when(scal[1] == 0)
    def _():
        first, second = down(f_first[...], f_second[...], carried[...], weights)
        n_second[...] = second
        n_first[...] = first
        d_first, d_second = pick(scal, own_aux[0:1, :], oth_aux[0:1, :])
        again = times(d_first * first, weights, 0)
        g_first[...] = again
        g_second[...] = times(d_second * second + again, weights, 1)

    hold(scal[1] != 0, old, (n_first, n_second))


def back_two(scal, f_first, f_second, carried, weights, *refs):
    old, (n_first, n_second) = refs[:2], refs[2:]

    @pl.when(scal[1] == 0)
    def _():
        n_first[...], n_second[...] = down(f_first[...], f_second[...], carried[...], weights)

    hold(scal[1] != 0, old, (n_first, n_second))


def back_basis(scal, f_first, f_second, carried, weights, *refs):
    old, (n_first, n_second) = refs[:2], refs[2:]
    few = n_first.shape[0]

    @pl.when(scal[1] == 0)
    def _():
        here = pl.ds(pl.multiple_of(scal[0] * few, 8), few)
        n_first[...], n_second[...] = down(f_first[here, :], f_second[here, :], carried[...], weights)

    hold(scal[1] != 0, old, (n_first, n_second))


def adjoint_start(scal, own_spots, oth_spots, weights, y_first, y_second, sent):
    @pl.when(scal[1] == 0)
    def _():
        first, second = pick(scal, own_spots[...], oth_spots[...])
        second = second + times_transposed(first, weights, 0)
        y_first[...] = first
        y_second[...] = second
        sent[...] = times_transposed(second, weights, 1)


def adjoint_top(scal, own_spots, oth_spots, carried, weights, *refs):
    old, (y_first, y_second, z_first, z_second) = refs[:2], refs[2:]

    @pl.when(scal[1] == 1)
    def _():
        first, second = pick(scal, own_spots[...], oth_spots[...])
        first = first + carried[...]
        second = second + times_transposed(first, weights, 0)
        y_first[...] = first
        y_second[...] = second
        last = times_transposed(second, weights, 1)
        z_second[...] = last
        z_first[...] = times_transposed(first + last, weights, 0)

    hold(scal[1] != 1, old, (y_first, y_second))


def placed(u, places, width):
    prim = u.shape[0]
    zero = jnp.zeros_like(u)
    rows = [u if i in places else zero for i in range(width // prim)]
    return jnp.concatenate(rows, axis=0)


def score(x, u):
    top, low = halves(u)
    return three(x, top, low, dot_rows)


def only(x, place, prim):
    lane = lax.broadcasted_iota(jnp.int32, x.shape, 1)
    return jnp.where((lane >= place * prim) & (lane < (place + 1) * prim), x, 0.0)


def score_top(scal, keep, recv, own_aux, oth_aux, y_first, y_second, z_first, z_second, *refs):
    blocks, values = refs[:-1], refs[-1]
    prim, width = y_first.shape[0], values.shape[1]
    half = values.shape[0]

    @pl.when(scal[1] == 1)
    def _():
        first, second = pick(scal, keep[...], recv[...])
        w = score(first, placed(y_first[...] + z_second[...], (0, 2), width)) + score(
            second, placed(y_second[...], (0, 2), width)
        )
        d_first, d_second = pick(scal, own_aux[0:1, :], oth_aux[0:1, :])
        n_first = jnp.concatenate([r[...] for r in blocks[0::2]], axis=0)
        n_second = jnp.concatenate([r[...] for r in blocks[1::2]], axis=0)
        g = score(d_first * n_first, placed(z_first[...], (1,), width)) + score(
            d_second * n_second, placed(z_second[...], (1,), width)
        )
        values[...] = only(w[:half], 0, prim) + g + only(w[half:], 2, prim)


def score_turn(scal, above, carried, y_first, y_second, k_first, k_second, *refs):
    blocks, values = refs[:-1], refs[-1]
    prim, width = y_first.shape[0], values.shape[1]
    half = values.shape[0]

    @pl.when(scal[1] == 0)
    def _():
        first = jnp.concatenate([r[...] for r in blocks[0::4]] + [k_first[...]] + [r[...] for r in blocks[2::4]], axis=0)
        second = jnp.concatenate([r[...] for r in blocks[1::4]] + [k_second[...]] + [r[...] for r in blocks[3::4]], axis=0)
        w = score(first, placed(y_first[...], (0, 1, 2), width)) + score(
            second, placed(y_second[...] + carried[...], (0, 1, 2), width)
        )
        extra = k_first.shape[0]
        values[...] = (
            above[...]
            + only(w[:half], 0, prim)
            + only(w[half : half + extra], 2, prim)
            + only(w[half + extra :], 1, prim)
        )


def settle(scal, k_first, k_second, *refs):
    blocks = refs[: 4 * BLOCKS]
    keep, send, k_keep, k_send = refs[4 * BLOCKS :]
    rows = blocks[0].shape[0]
    first = scal[0] == 0
    for i in range(BLOCKS):
        a1, b1, a2, b2 = (r[...] for r in blocks[4 * i : 4 * i + 4])
        here = slice(i * rows, (i + 1) * rows)
        a, b = 2.0 * a1 - a2, 2.0 * b1 - b2
        keep[here, :] = jnp.where(first, a, b)
        send[here, :] = jnp.where(first, b, a)
    k_keep[...] = jnp.where(first, k_first[...], k_second[...])
    k_send[...] = jnp.where(first, k_second[...], k_first[...])


def finish(scal, keep, recv, q_keep, q_recv, k_keep, k_recv, one, two, out):
    rows = keep.shape[0]
    k_low, k_high = pick(scal, k_keep[...], k_recv[...])
    right = jnp.concatenate([-k_low, -k_high, one[...], two[...]], axis=0)
    top, low = halves(right)
    for n, q, which in ((keep, q_keep, scal[0]), (recv, q_recv, 1 - scal[0])):
        out[pl.ds(pl.multiple_of(which * rows, 8), rows), :] = n[...] + three(q[...], top, low)


def on_device(
    residual,
    inverse_slab,
    diagonal,
    primal_index,
    coarse_map,
    schur_small,
    constraint_basis,
    coarse_basis,
    coarse_inverse,
):
    levels = lax.axis_size("slab")
    subs = lax.axis_size("sub")
    assert levels == 4 and subs & (subs - 1) == 0
    slab = lax.axis_index("slab")
    sub = lax.axis_index("sub")
    member = slab % 2
    scal = jnp.stack([member, slab // 2]).astype(jnp.int32)

    def swap(x):
        return lax.ppermute(x, "slab", [(i, i ^ 1) for i in range(levels)])

    def rise(x):
        return lax.ppermute(x, "slab", [(0, 2), (1, 3)])

    def fall(x):
        return lax.ppermute(x, "slab", [(2, 0), (3, 1)])

    def gather(x):
        distance = 1
        while distance < subs:
            other = lax.ppermute(x, "sub", [(i, i ^ distance) for i in range(subs)])
            x = jnp.concatenate([x, other], axis=0)
            distance *= 2
        return x

    vector = residual[0, 0]
    matrix = inverse_slab[0, 0]
    one, two = constraint_basis[0, 0], coarse_basis[0, 0]
    rows, size = vector.shape
    prim = primal_index.shape[-1]
    coarse_count, share = coarse_inverse.shape
    half = rows // 2
    block = half // BLOCKS
    extra = 2 * prim
    width = -(-3 * prim // LANES) * LANES
    assert half == extra and prim <= coarse_count

    other_matrix = swap(matrix)
    spots = jnp.full((size,), -1.0, f32).at[:prim].set(primal_index[0, 0].astype(f32))
    own_aux = jnp.stack([diagonal[0, 0], spots])
    oth_aux = swap(own_aux)

    fixed = jnp.concatenate(
        [
            coarse_inverse.T,
            jnp.pad(schur_small[0], ((0, 0), (0, coarse_count - prim))),
            jnp.pad(coarse_map.astype(f32), ((0, 7), (0, coarse_count - prim))),
        ],
        axis=0,
    )
    fixed = gather(fixed).reshape(subs, share + prim + 8, coarse_count)
    inverse_rows = fixed[:, :share].reshape(coarse_count, coarse_count)
    schur = fixed[:, share : share + prim, :prim]
    maps = fixed[:, share + prim, :prim]
    order = jnp.arange(subs, dtype=jnp.int32) ^ sub
    columns = (order[:, None] * share + jnp.arange(share, dtype=jnp.int32)).reshape(-1).astype(f32)
    onehot = (maps[:, :, None] == jnp.arange(coarse_count, dtype=jnp.int32).astype(f32)).astype(f32)
    onehot_there = (maps[:, :, None] == columns).astype(f32)

    own, keep, send = call(
        split_own,
        [struct((2, size, size), bf16), struct((half + extra, size)), struct((half + extra, size))],
        [scal, matrix, vector, one, two, own_aux],
        2,
        scratch=[
            pltpu.VMEM((size, size), f32),
            pltpu.VMEM((rows + extra, size), f32),
            pltpu.VMEM((rows + extra, size), f32),
            pltpu.SemaphoreType.DMA((3 + PIECES,)),
        ],
        hbm=(1, 2, 3, 4),
    )
    recv = swap(send)
    (weights,) = call(split_other, [struct((2, 2, size, size), bf16)], [scal, other_matrix, own], 1)
    place = jnp.arange(size, dtype=jnp.int32).astype(f32)[None, :]
    own_spots = (own_aux[1, :prim, None] == place).astype(f32)
    oth_spots = (oth_aux[1, :prim, None] == place).astype(f32)

    def like(count, *heights):
        return [struct((h, size)) for h in heights for _ in range(count)]

    span = range(BLOCKS)
    f, carried = [], []
    for i in span:
        f.append(
            call(
                functools.partial(start_chain, i * block),
                like(2, block),
                [scal, keep, recv, weights],
                1,
            )
        )
        carried.append(rise(f[i][1]))
    y_first, y_second, z_sent = call(
        adjoint_start, like(3, prim), [scal, own_spots, oth_spots, weights], 2
    )
    z_carried = rise(z_sent)
    k_first, k_second, k_part = call(
        functools.partial(start_basis, half),
        like(2, extra) + like(1, prim),
        [scal, keep, recv, weights],
        1,
    )
    k_carried = rise(k_part)

    n = []
    for i in span:
        n.append(
            call(
                functools.partial(top_one, i * block),
                like(2, block),
                [scal, keep, recv, carried[i], weights],
                3,
            )
        )
        carried[i] = fall(n[i][0])
    y_first, y_second, z_first, z_second = call(
        adjoint_top,
        like(4, prim),
        [scal, own_spots, oth_spots, z_carried, weights, y_first, y_second],
        3,
        aliases={5: 0, 6: 1},
    )
    z_back = fall(z_first)
    (upper,) = call(
        score_top,
        [struct((half, width))],
        [scal, keep, recv, own_aux, oth_aux, y_first, y_second, z_first, z_second, *n[0], *n[1]],
        1,
    )
    upper = fall(upper)

    n_one, g = [], []
    for i in span:
        turned = call(
            turn,
            like(4, block),
            [scal, *f[i], carried[i], weights, own_aux, oth_aux, *n[i]],
            4,
            aliases={7: 0, 8: 1},
        )
        n_one.append(turned[:2])
        g.append(turned[2:])
        carried[i] = rise(g[i][1])
    pieces = []
    for i in span:
        pieces += [*f[i], *g[i]]
    (values,) = call(
        score_turn,
        [struct((half, width))],
        [scal, upper, z_back, y_first, y_second, k_first, k_second, *pieces],
        1,
    )
    values = gather(values).reshape(subs, half, width)

    n_two = []
    for i in span:
        n_two.append(
            call(
                top_two, like(2, block), [scal, *n_one[i], carried[i], weights, own_aux, oth_aux], 3
            )
        )
        carried[i] = fall(n_two[i][0])
    k_n = call(
        functools.partial(top_basis, half), like(2, prim), [scal, keep, recv, k_carried, weights], 3
    )
    k_carried = fall(k_n[0])
    for i in span:
        n_two[i] = call(
            back_two,
            like(2, block),
            [scal, *g[i], carried[i], weights, *n_two[i]],
            2,
            aliases={5: 0, 6: 1},
        )
    k_n = call(
        back_basis,
        like(2, prim),
        [scal, k_first, k_second, k_carried, weights, *k_n],
        2,
        aliases={5: 0, 6: 1},
    )
    pieces = []
    for i in span:
        pieces += [*n_one[i], *n_two[i]]
    m_keep, m_send, k_keep, k_send = call(settle, like(2, half, prim), [scal, *k_n, *pieces], 0.5)
    m_recv = swap(m_send)
    k_recv = swap(k_send)

    def times_high(form, left, right):
        return jnp.einsum(form, left, right, precision=highest, preferred_element_type=f32)

    p_one = values[:, :, :prim]
    p_defect = p_one - values[:, :, prim : 2 * prim]
    x_one = values[:, :prim, 2 * prim : 3 * prim]
    x_two = values[:, prim : 2 * prim, 2 * prim : 3 * prim]
    sol = times_high("rn,mn->rm", times_high("srp,spn->rn", p_one, onehot), inverse_rows)
    picked = times_high("rm,spm->srp", sol, onehot_there)
    multiplier = times_high("srp,spq->srq", p_one, schur)
    p_two = p_defect + times_high("srp,spq->srq", multiplier, x_one) - times_high(
        "srp,spq->srq", picked, x_two
    )
    sol = times_high("rn,mn->rm", times_high("srp,spn->rn", p_two, onehot), inverse_rows)
    q_one = jnp.concatenate([-multiplier[0], picked[0]], axis=1)
    q_two = jnp.concatenate(
        [
            -times_high("rp,pq->rq", p_two[0], schur[0]),
            times_high("rm,pm->rp", sol, onehot_there[0]),
        ],
        axis=1,
    )
    q = jnp.concatenate([q_one, q_one + q_two], axis=1)
    q_upper = rise(q)
    q = jnp.where(scal[1] == 0, q, q_upper)
    q_recv = swap(q)
    (out,) = call(
        finish,
        [struct((rows, size))],
        [scal, m_keep, m_recv, q, q_recv, k_keep, k_recv, one, two],
        0.5,
    )
    return out[None, None]


def solution(mesh):
    placed_as = (
        P("sub", "slab", None, None),
        P("sub", "slab", None, None),
        P("sub", "slab", None),
        P("sub", "slab", None),
        P("sub", None),
        P("sub", None, None),
        P("sub", "slab", None, None),
        P("sub", "slab", None, None),
        P(None, "sub"),
    )

    return jax.shard_map(
        on_device,
        mesh=mesh,
        in_specs=placed_as,
        out_specs=P("sub", "slab", None, None),
        check_vma=False,
    )
```

```python
import functools

import jax
import jax.numpy as jnp
from jax import lax
from jax.experimental import pallas as pl
from jax.experimental.pallas import tpu as pltpu
from jax.sharding import PartitionSpec as P


f32 = jnp.float32
bf16 = jnp.bfloat16
highest = lax.Precision.HIGHEST
LANES = 128
BLOCKS = 2
PIECES = 4


def halves(x):
    top = x.astype(bf16)
    return top, (x - top.astype(f32)).astype(bf16)


def dot(left, right):
    return jnp.dot(left, right, preferred_element_type=f32)


def dot_rows(left, right):
    return lax.dot_general(left, right, (((1,), (1,)), ((), ())), preferred_element_type=f32)


def three(x, top_right, low_right, how=dot):
    rows = x.shape[0]
    top, low = halves(x)
    both = how(jnp.concatenate([top, low], axis=0), top_right)
    return both[:rows] + both[rows:] + how(top, low_right)


def times(x, weights, member):
    step = weights[0].shape[2]
    top, low = halves(x)
    both = jnp.concatenate([top, low], axis=0)
    rows = x.shape[0]
    first, second = 0.0, 0.0
    for i, piece in enumerate(weights):
        cols = slice(i * step, (i + 1) * step)
        first = first + dot(both[:, cols], piece[member, 0])
        second = second + dot(top[:, cols], piece[member, 1])
    return first[:rows] + first[rows:] + second


def times_transposed(x, weights, member):
    return jnp.concatenate(
        [three(x, piece[member, 0], piece[member, 1], dot_rows) for piece in weights], axis=1
    )


def member():
    return lax.axis_index("slab") & 1


def pair():
    return lax.axis_index("slab") >> 1


def spec(space):
    return pl.BlockSpec(memory_space=space)


def call(body, outs, args, work, aliases=None, scratch=(), hbm=()):
    specs = [spec(pltpu.VMEM) for _ in args]
    args = list(args)
    for place in hbm:
        specs[place] = spec(pltpu.HBM)
        args[place] = pltpu.with_memory_space_constraint(args[place], pltpu.HBM)
    return pl.pallas_call(
        body,
        out_shape=outs,
        in_specs=specs,
        out_specs=[spec(pltpu.VMEM) for _ in outs],
        input_output_aliases=aliases or {},
        scratch_shapes=list(scratch),
        cost_estimate=pl.CostEstimate(flops=int(work * 8e8), bytes_accessed=0, transcendentals=0),
        compiler_params=pltpu.CompilerParams(vmem_limit_bytes=VMEM_LIMIT),
    )(*args)


VMEM_LIMIT = 16 << 20


def struct(shape, dtype=f32):
    return jax.ShapeDtypeStruct(shape, dtype)


def pick(own, oth):
    first = member() == 0
    return jnp.where(first, own, oth), jnp.where(first, oth, own)


def hold(idle, before, after):
    @pl.when(idle)
    def _():
        for old, new in zip(before, after):
            new[...] = old[...]


def load(matrix, *refs):
    pieces, sems = refs[:PIECES], refs[PIECES]
    step = pieces[0].shape[0]
    copies = [
        pltpu.make_async_copy(matrix.at[pl.ds(i * step, step)], piece, sems.at[i])
        for i, piece in enumerate(pieces)
    ]
    for copy in copies:
        copy.start()
    for copy in copies:
        copy.wait()


def first_products(*refs):
    vector, one, two, diagonal, index = refs[:5]
    pieces = refs[5 : 5 + PIECES]
    keep, send, x, total, sems = refs[5 + PIECES :]
    rows, prim = vector.shape[0], one.shape[0]
    extra = 2 * prim
    copies = [
        pltpu.make_async_copy(vector, x.at[pl.ds(0, rows)], sems.at[0]),
        pltpu.make_async_copy(one, x.at[pl.ds(rows, prim)], sems.at[1]),
        pltpu.make_async_copy(two, x.at[pl.ds(rows + prim, prim)], sems.at[2]),
    ]
    for copy in copies:
        copy.start()
    for copy in copies:
        copy.wait()
    x[rows:, :] = x[rows:, :] * diagonal[...]
    step = pieces[0].shape[0]
    for i, piece in enumerate(pieces):
        top, low = halves(piece[...])
        part = three(x[:, i * step : (i + 1) * step], top, low)
        if i == 0:
            total[...] = part
        else:
            total[...] += part
    half = rows // 2
    here, there = member(), 1 - member()
    for out, which in ((keep, here), (send, there)):
        out[:half, :] = total[pl.ds(pl.multiple_of(which * half, 8), half), :]
        out[half : half + extra, :] = total[rows:, :]
        out[half + extra :, :] = jnp.zeros_like(out[half + extra :, :])
        out[half + extra : half + extra + 1, :] = diagonal[...]
        out[half + extra + 1 : half + extra + 2, :prim] = index[...].astype(f32)


def split(own, oth, weights):
    here = member()
    for which, piece in ((here, own), (1 - here, oth)):
        top, low = halves(piece[...])
        weights[which, 0] = top
        weights[which, 1] = low


def diagonals(keep, recv):
    place = keep.shape[0] - 8
    return pick(keep[place : place + 1, :], recv[place : place + 1, :])


def start_chain(keep, recv, *refs):
    weights, (f_first, f_second) = refs[:PIECES], refs[PIECES:]
    rows = f_first.shape[0]

    @pl.when(pair() == 0)
    def _():
        first, second = pick(keep[:rows, :], recv[:rows, :])
        f_first[...] = first
        f_second[...] = second + times(first, weights, 1)


def start_last(keep, recv, *refs):
    weights, (f_first, f_second, k_first, k_second) = refs[:PIECES], refs[PIECES:]
    rows, extra = f_first.shape[0], k_first.shape[0]
    stop = keep.shape[0] - 8

    @pl.when(pair() == 0)
    def _():
        at = stop - extra - rows
        first, second = pick(keep[at:stop, :], recv[at:stop, :])
        second = second + times(first, weights, 1)
        f_first[...] = first[:rows]
        f_second[...] = second[:rows]
        k_first[...] = first[rows:]
        k_second[...] = second[rows:]


def top_one(at, keep, recv, carried, *refs):
    weights, (n_first, n_second) = refs[:PIECES], refs[PIECES:]
    rows = n_first.shape[0]

    @pl.when(pair() == 1)
    def _():
        first, second = pick(keep[at : at + rows, :], recv[at : at + rows, :])
        first = first + times(carried[...], weights, 0)
        second = second + times(first, weights, 1)
        n_first[...] = first + times(second, weights, 0)
        n_second[...] = second


def top_two(with_basis, keep, recv, v_first, v_second, carried, *refs):
    riding, weights, (n_first, n_second) = refs[0], refs[1 : 1 + PIECES], refs[1 + PIECES :]
    rows = v_first.shape[0]
    few = riding.shape[0] // 2
    extra = 2 * few
    at = keep.shape[0] - 8 - extra

    @pl.when(pair() == 1)
    def _():
        d_first, d_second = diagonals(keep, recv)
        x = d_first * v_first[...] + carried[...]
        if with_basis:
            here = pl.ds(pl.multiple_of(at + member() * few, 8), few)
            k_first, k_second = pick(keep[here, :], recv[here, :])
            first = times(jnp.concatenate([x, riding[few:, :]], axis=0), weights, 0)
            k_first = first[rows:] + k_first
            y = d_second * v_second[...] + first[:rows]
            second = times(jnp.concatenate([y, k_first], axis=0), weights, 1)
            first = jnp.concatenate([first[:rows], k_first], axis=0)
            second = jnp.concatenate([second[:rows], second[rows:] + k_second], axis=0)
        else:
            first = times(x, weights, 0)
            second = times(d_second * v_second[...] + first, weights, 1)
        n_first[...] = first + times(second, weights, 0)
        n_second[...] = second


def down(f_first, f_second, carried, weights):
    second = f_second + times(carried, weights, 1)
    return f_first + times(second, weights, 0), second


def turn(keep, recv, f_first, f_second, carried, *refs):
    weights, old = refs[:PIECES], refs[PIECES : PIECES + 2]
    n_first, n_second, g_first, g_second = refs[PIECES + 2 :]

    @pl.when(pair() == 0)
    def _():
        first, second = down(f_first[...], f_second[...], carried[...], weights)
        n_second[...] = second
        n_first[...] = first
        d_first, d_second = diagonals(keep, recv)
        again = times(d_first * first, weights, 0)
        g_first[...] = again
        g_second[...] = times(d_second * second + again, weights, 1)

    hold(pair() != 0, old, (n_first, n_second))


def back(with_basis, f_first, f_second, k_first, k_second, carried, *refs):
    weights, old, (n_first, n_second) = refs[:PIECES], refs[PIECES : PIECES + 2], refs[PIECES + 2 :]
    few = k_first.shape[0] // 2

    @pl.when(pair() == 0)
    def _():
        first, second = f_first[...], f_second[...]
        if with_basis:
            here = pl.ds(pl.multiple_of(member() * few, 8), few)
            first = jnp.concatenate([first, k_first[here, :]], axis=0)
            second = jnp.concatenate([second, k_second[here, :]], axis=0)
        n_first[...], n_second[...] = down(first, second, carried[...], weights)

    hold(pair() != 0, old, (n_first, n_second))


def adjoint_start(own_spots, oth_spots, k_second, *refs):
    weights, (y_first, y_second, sent) = refs[:PIECES], refs[PIECES:]
    prim = y_first.shape[0]

    @pl.when(pair() == 0)
    def _():
        first, second = pick(own_spots[...], oth_spots[...])
        second = second + times_transposed(first, weights, 0)
        y_first[...] = first
        y_second[...] = second
        sent[:prim, :] = times_transposed(second, weights, 1)
        sent[prim:, :] = k_second[pl.ds(pl.multiple_of(member() * prim, 8), prim), :]


def placed(u, places, width):
    prim = u.shape[0]
    zero = jnp.zeros_like(u)
    rows = [u if i in places else zero for i in range(width // prim)]
    return jnp.concatenate(rows, axis=0)


def score(x, u):
    top, low = halves(u)
    return three(x, top, low, dot_rows)


def only(x, place, prim):
    lane = lax.broadcasted_iota(jnp.int32, x.shape, 1)
    return jnp.where((lane >= place * prim) & (lane < (place + 1) * prim), x, 0.0)


def pack(values, out, at):
    rows, width = values.shape
    per = out.shape[1] // width
    for j in range(rows // 8):
        row = at + (j // per) * 8
        out[row : row + 8, (j % per) * width : (j % per + 1) * width] = values[8 * j : 8 * j + 8, :]


def unpack(packed, at, rows, width):
    per = packed.shape[1] // width
    return jnp.concatenate(
        [
            packed[
                at + (j // per) * 8 : at + (j // per) * 8 + 8,
                (j % per) * width : (j % per + 1) * width,
            ]
            for j in range(rows // 8)
        ],
        axis=0,
    )


def adjoint_top(width, keep, recv, own_spots, oth_spots, carried, *refs):
    weights, refs = refs[:PIECES], refs[PIECES:]
    blocks, old, (y_first, y_second, sent) = refs[: 2 * BLOCKS], refs[2 * BLOCKS : -3], refs[-3:]
    prim = y_first.shape[0]

    @pl.when(pair() == 1)
    def _():
        first, second = pick(own_spots[...], oth_spots[...])
        first = first + carried[:prim, :]
        second = second + times_transposed(first, weights, 0)
        z_second = times_transposed(second, weights, 1)
        first = first + z_second
        z_first = times_transposed(first, weights, 0)
        sent[:prim, :] = z_first
        w_first, w_second = pick(keep[...], recv[...])
        stop = w_first.shape[0] - 8
        w = score(w_first[:stop], placed(first, (0, 2), width)) + score(
            w_second[:stop], placed(second, (0, 2), width)
        )
        d_first, d_second = diagonals(keep, recv)
        n_first = jnp.concatenate([r[...] for r in blocks[0::2]], axis=0)
        n_second = jnp.concatenate([r[...] for r in blocks[1::2]], axis=0)
        g = score(d_first * n_first, placed(z_first, (1,), width)) + score(
            d_second * n_second, placed(z_second, (1,), width)
        )
        half = n_first.shape[0]
        pack(only(w[:half], 0, prim) + g + only(w[half:], 2, prim), sent, prim)

    hold(pair() != 1, old, (y_first, y_second))


def score_turn(carried, y_first, y_second, k_first, k_second, *refs):
    blocks, values = refs[:-1], refs[-1]
    prim = y_first.shape[0]
    half, width = values.shape

    @pl.when(pair() == 0)
    def _():
        first = jnp.concatenate(
            [r[...] for r in blocks[0::4]] + [k_first[...]] + [r[...] for r in blocks[2::4]], axis=0
        )
        second = jnp.concatenate(
            [r[...] for r in blocks[1::4]] + [k_second[...]] + [r[...] for r in blocks[3::4]], axis=0
        )
        w = score(first, placed(y_first[...], (0, 1, 2), width)) + score(
            second, placed(y_second[...] + carried[:prim, :], (0, 1, 2), width)
        )
        extra = k_first.shape[0]
        values[...] = (
            unpack(carried, prim, half, width)
            + only(w[:half], 0, prim)
            + only(w[half : half + extra], 2, prim)
            + only(w[half + extra :], 1, prim)
        )


def settle(*refs):
    blocks, (keep, send) = refs[: 4 * BLOCKS], refs[4 * BLOCKS :]
    rows = blocks[0].shape[0]
    for i in range(BLOCKS):
        a1, b1, a2, b2 = blocks[4 * i : 4 * i + 4]
        here = slice(i * rows, (i + 1) * rows)
        keep[here, :], send[here, :] = pick(
            2.0 * a1[...] - a2[:rows, :], 2.0 * b1[...] - b2[:rows, :]
        )
    keep[BLOCKS * rows :, :], send[BLOCKS * rows :, :] = pick(blocks[2][rows:, :], blocks[3][rows:, :])


def finish(keep, recv, q_keep, q_recv, one, two, out):
    prim = one.shape[0]
    rows = keep.shape[0] - prim
    k_low, k_high = pick(keep[rows:, :], recv[rows:, :])
    right = jnp.concatenate([-k_low, -k_high, one[...], two[...]], axis=0)
    top, low = halves(right)
    here = member()
    for n, q, which in ((keep, q_keep, here), (recv, q_recv, 1 - here)):
        out[pl.ds(pl.multiple_of(which * rows, 8), rows), :] = n[:rows, :] + three(q[...], top, low)


def on_device(
    residual,
    inverse_slab,
    diagonal,
    primal_index,
    coarse_map,
    schur_small,
    constraint_basis,
    coarse_basis,
    coarse_inverse,
):
    levels = lax.axis_size("slab")
    subs = lax.axis_size("sub")
    assert levels == 4 and subs & (subs - 1) == 0
    sub = lax.axis_index("sub")

    def swap(x):
        return lax.ppermute(x, "slab", [(i, i ^ 1) for i in range(levels)])

    def rise(x):
        return lax.ppermute(x, "slab", [(0, 2), (1, 3)])

    def fall(x):
        return lax.ppermute(x, "slab", [(2, 0), (3, 1)])

    def gather(x):
        distance = 1
        while distance < subs:
            pairs = [
                (i * levels + k, (i ^ distance) * levels + k) for i in range(subs) for k in range(2)
            ]
            other = lax.ppermute(x, ("sub", "slab"), pairs)
            x = jnp.concatenate([x, other], axis=0)
            distance *= 2
        return x

    vector = residual[0, 0]
    matrix = inverse_slab[0, 0]
    one, two = constraint_basis[0, 0], coarse_basis[0, 0]
    rows, size = vector.shape
    prim = primal_index.shape[-1]
    coarse_count, share = coarse_inverse.shape
    half = rows // 2
    block = half // BLOCKS
    extra = 2 * prim
    width = -(-3 * prim // LANES) * LANES
    packed = -(-half * width // (8 * size)) * 8
    step = size // PIECES
    assert half == extra and prim <= coarse_count and size % width == 0

    def like(count, *heights):
        return [struct((h, size)) for h in heights for _ in range(count)]

    own = call(load, like(PIECES, step), [matrix], 1, scratch=[pltpu.SemaphoreType.DMA((PIECES,))], hbm=(0,))
    oth = [swap(piece) for piece in own]

    fixed = jnp.concatenate(
        [
            coarse_inverse.T,
            jnp.pad(schur_small[0], ((0, 0), (0, coarse_count - prim))),
            jnp.pad(coarse_map.astype(f32), ((0, 7), (0, coarse_count - prim))),
        ],
        axis=0,
    )
    fixed = gather(fixed).reshape(subs, share + prim + 8, coarse_count)
    inverse_rows = fixed[:, :share].reshape(coarse_count, coarse_count)
    schur = fixed[:, share : share + prim, :prim]
    maps = fixed[:, share + prim, :prim]
    order = jnp.arange(subs, dtype=jnp.int32) ^ sub
    columns = (order[:, None] * share + jnp.arange(share, dtype=jnp.int32)).reshape(-1).astype(f32)
    onehot = (maps[:, :, None] == jnp.arange(coarse_count, dtype=jnp.int32).astype(f32)).astype(f32)
    onehot_there = (maps[:, :, None] == columns).astype(f32)

    keep, send = call(
        first_products,
        like(2, half + extra + 8),
        [vector, one, two, diagonal[0], primal_index[0], *own],
        2,
        scratch=[
            pltpu.VMEM((rows + extra, size), f32),
            pltpu.VMEM((rows + extra, size), f32),
            pltpu.SemaphoreType.DMA((3,)),
        ],
        hbm=(0, 1, 2),
    )
    recv = swap(send)
    weights = [
        call(split, [struct((2, 2, step, size), bf16)], [own[i], oth[i]], 0.3)[0]
        for i in range(PIECES)
    ]
    place = jnp.arange(size, dtype=jnp.int32)
    own_spots = (primal_index[0, 0][:, None] == place).astype(f32)
    oth_spots = (recv[half + extra + 1, :prim][:, None] == place.astype(f32)).astype(f32)

    span = range(BLOCKS)
    f, carried = [], []
    for i in span[:-1]:
        f.append(call(start_chain, like(2, block), [keep, recv, *weights], 1))
        carried.append(rise(f[i][1]))
    *f_last, k_first, k_second = call(start_last, like(2, block, extra), [keep, recv, *weights], 1)
    f.append(f_last)
    carried.append(rise(f_last[1]))
    y_first, y_second, sent = call(
        adjoint_start,
        like(2, prim) + like(1, 2 * prim),
        [own_spots, oth_spots, k_second, *weights],
        2,
    )
    riding = rise(sent)

    n = []
    for i in span:
        n.append(
            call(
                functools.partial(top_one, i * block),
                like(2, block),
                [keep, recv, carried[i], *weights],
                3,
            )
        )
        carried[i] = fall(n[i][0])
    y_first, y_second, sent = call(
        functools.partial(adjoint_top, width),
        like(2, prim) + like(1, prim + packed),
        [keep, recv, own_spots, oth_spots, riding, *weights, *n[0], *n[1], y_first, y_second],
        4,
        aliases={5 + PIECES + 2 * BLOCKS: 0, 6 + PIECES + 2 * BLOCKS: 1},
    )
    z_back = fall(sent)

    n_one, g = [], []
    for i in span:
        turned = call(
            turn,
            like(4, block),
            [keep, recv, *f[i], carried[i], *weights, *n[i]],
            4,
            aliases={5 + PIECES: 0, 6 + PIECES: 1},
        )
        n_one.append(turned[:2])
        g.append(turned[2:])
        carried[i] = rise(g[i][1])
    pieces = []
    for i in span:
        pieces += [*f[i], *g[i]]
    (values,) = call(
        score_turn,
        [struct((half, width))],
        [z_back, y_first, y_second, k_first, k_second, *pieces],
        1,
    )
    values = gather(values).reshape(subs, half, width)

    n_two = []
    for i in span:
        n_two.append(
            call(
                functools.partial(top_two, i == 0),
                like(2, block + prim if i == 0 else block),
                [keep, recv, *n_one[i], carried[i], riding, *weights],
                3,
            )
        )
        carried[i] = fall(n_two[i][0])
    for i in span:
        n_two[i] = call(
            functools.partial(back, i == 0),
            like(2, block + prim if i == 0 else block),
            [*g[i], k_first, k_second, carried[i], *weights, *n_two[i]],
            2,
            aliases={5 + PIECES: 0, 6 + PIECES: 1},
        )
    pieces = []
    for i in span:
        pieces += [*n_one[i], *n_two[i]]
    m_keep, m_send = call(settle, like(2, half + prim), pieces, 0.5)
    m_recv = swap(m_send)

    def times_high(form, left, right):
        return jnp.einsum(form, left, right, precision=highest, preferred_element_type=f32)

    p_one = values[:, :, :prim]
    p_defect = p_one - values[:, :, prim : 2 * prim]
    x_one = values[:, :prim, 2 * prim : 3 * prim]
    x_two = values[:, prim : 2 * prim, 2 * prim : 3 * prim]
    sol = times_high("rn,mn->rm", times_high("srp,spn->rn", p_one, onehot), inverse_rows)
    picked = times_high("rm,spm->srp", sol, onehot_there)
    multiplier = times_high("srp,spq->srq", p_one, schur)
    p_two = p_defect + times_high("srp,spq->srq", multiplier, x_one) - times_high(
        "srp,spq->srq", picked, x_two
    )
    sol = times_high("rn,mn->rm", times_high("srp,spn->rn", p_two, onehot), inverse_rows)
    q_one = jnp.concatenate([-multiplier[0], picked[0]], axis=1)
    q_two = jnp.concatenate(
        [
            -times_high("rp,pq->rq", p_two[0], schur[0]),
            times_high("rm,pm->rp", sol, onehot_there[0]),
        ],
        axis=1,
    )
    q = jnp.concatenate([q_one, q_one + q_two], axis=1)
    q_upper = rise(q)
    q = jnp.where(pair() == 0, q, q_upper)
    q_recv = swap(q)
    (out,) = call(finish, [struct((rows, size))], [m_keep, m_recv, q, q_recv, one, two], 0.5)
    return out[None, None]


def solution(mesh):
    placed_as = (
        P("sub", "slab", None, None),
        P("sub", "slab", None, None),
        P("sub", "slab", None),
        P("sub", "slab", None),
        P("sub", None),
        P("sub", None, None),
        P("sub", "slab", None, None),
        P("sub", "slab", None, None),
        P(None, "sub"),
    )

    return jax.shard_map(
        on_device,
        mesh=mesh,
        in_specs=placed_as,
        out_specs=P("sub", "slab", None, None),
        check_vma=False,
    )
```

```python
import functools

import jax
import jax.numpy as jnp
from jax import lax
from jax.experimental import pallas as pl
from jax.experimental.pallas import tpu as pltpu
from jax.sharding import PartitionSpec as P


f32 = jnp.float32
bf16 = jnp.bfloat16
LANES = 128
BLOCKS = 2
PIECES = 4
PARTS = 1


def halves(x):
    top = x.astype(bf16)
    return top, (x - top.astype(f32)).astype(bf16)


def dot(left, right):
    return jnp.dot(left, right, preferred_element_type=f32)


def dot_rows(left, right):
    return lax.dot_general(left, right, (((1,), (1,)), ((), ())), preferred_element_type=f32)


def three(x, top_right, low_right, how=dot):
    rows = x.shape[0]
    top, low = halves(x)
    both = how(jnp.concatenate([top, low], axis=0), top_right)
    return both[:rows] + both[rows:] + how(top, low_right)


def times(x, weights, member):
    step = weights[0].shape[2]
    top, low = halves(x)
    both = jnp.concatenate([top, low], axis=0)
    rows = x.shape[0]
    first, second = 0.0, 0.0
    for i, piece in enumerate(weights):
        cols = slice(i * step, (i + 1) * step)
        first = first + dot(both[:, cols], piece[member, 0])
        second = second + dot(top[:, cols], piece[member, 1])
    return first[:rows] + first[rows:] + second


def times_transposed(x, weights, member):
    return jnp.concatenate(
        [three(x, piece[member, 0], piece[member, 1], dot_rows) for piece in weights], axis=1
    )


def member():
    return lax.axis_index("slab") & 1


def pair():
    return lax.axis_index("slab") >> 1


def spec(space):
    return pl.BlockSpec(memory_space=space)


def call(body, outs, args, work, aliases=None, scratch=(), hbm=(), limit=None):
    specs = [spec(pltpu.VMEM) for _ in args]
    args = list(args)
    for place in hbm:
        specs[place] = spec(pltpu.HBM)
        args[place] = pltpu.with_memory_space_constraint(args[place], pltpu.HBM)
    return pl.pallas_call(
        body,
        out_shape=outs,
        in_specs=specs,
        out_specs=[spec(pltpu.VMEM) for _ in outs],
        input_output_aliases=aliases or {},
        scratch_shapes=list(scratch),
        cost_estimate=pl.CostEstimate(flops=int(work * 8e8), bytes_accessed=0, transcendentals=0),
        compiler_params=pltpu.CompilerParams(vmem_limit_bytes=limit or VMEM_LIMIT),
    )(*args)


VMEM_LIMIT = 16 << 20


def struct(shape, dtype=f32):
    return jax.ShapeDtypeStruct(shape, dtype)


def pick(own, oth):
    first = member() == 0
    return jnp.where(first, own, oth), jnp.where(first, oth, own)


def hold(idle, before, after):
    @pl.when(idle)
    def _():
        for old, new in zip(before, after):
            new[...] = old[...]


def fix(inverse, schur, maps, out):
    share, prim = inverse.shape[1], schur.shape[0]
    unit = lax.broadcasted_iota(jnp.int32, (share, share), 0) == lax.broadcasted_iota(
        jnp.int32, (share, share), 1
    )
    unit = unit.astype(f32).astype(bf16)
    top, low = halves(inverse[...])
    rest = (inverse[...] - top.astype(f32) - low.astype(f32)).astype(bf16)
    out[:share, :] = dot_rows(unit, top) + dot_rows(unit, low) + dot_rows(unit, rest)
    out[share : share + prim, :] = jnp.zeros_like(out[share : share + prim, :])
    out[share : share + prim, :prim] = schur[...]
    out[share + prim :, :] = jnp.full_like(out[share + prim :, :], -1.0)
    out[share + prim : share + prim + 1, :prim] = maps[...].astype(f32)


def first_products(matrix, vector, one, two, diagonal, index, own, keep, send, buffer, x, total, sems):
    size = matrix.shape[0]
    step = size // PIECES
    rows, prim = vector.shape[0], one.shape[0]
    extra = 2 * prim
    copies = [
        pltpu.make_async_copy(vector, x.at[pl.ds(0, rows)], sems.at[0]),
        pltpu.make_async_copy(one, x.at[pl.ds(rows, prim)], sems.at[1]),
        pltpu.make_async_copy(two, x.at[pl.ds(rows + prim, prim)], sems.at[2]),
    ]
    pieces = [
        pltpu.make_async_copy(
            matrix.at[pl.ds(i * step, step)], buffer.at[pl.ds(i * step, step)], sems.at[3 + i]
        )
        for i in range(PIECES)
    ]
    for copy in copies + pieces:
        copy.start()
    for copy in copies:
        copy.wait()
    x[rows:, :] = x[rows:, :] * diagonal[...]
    for i, copy in enumerate(pieces):
        cols = pl.ds(i * step, step)
        copy.wait()
        top, low = halves(buffer[cols, :])
        own[0, cols, :] = top
        own[1, cols, :] = low
        part = three(x[:, cols], own[0, cols, :], own[1, cols, :])
        if i == 0:
            total[...] = part
        else:
            total[...] += part
    half = rows // 2
    here, there = member(), 1 - member()
    for out, which in ((keep, here), (send, there)):
        out[:half, :] = total[pl.ds(pl.multiple_of(which * half, 8), half), :]
        out[half : half + extra, :] = total[rows:, :]
        out[half + extra :, :] = jnp.zeros_like(out[half + extra :, :])
        out[half + extra : half + extra + 1, :] = diagonal[...]
        out[half + extra + 1 : half + extra + 2, :prim] = index[...].astype(f32)


def split(matrix, own, weights, buffer, sems):
    step = matrix.shape[0] // PIECES
    pieces = [
        pltpu.make_async_copy(
            matrix.at[pl.ds(i * step, step)], buffer.at[pl.ds(i * step, step)], sems.at[i]
        )
        for i in range(PIECES)
    ]
    for copy in pieces:
        copy.start()
    here = member()
    weights[here] = own[...]
    for i, copy in enumerate(pieces):
        cols = pl.ds(i * step, step)
        copy.wait()
        top, low = halves(buffer[cols, :])
        weights[1 - here, 0, cols, :] = top
        weights[1 - here, 1, cols, :] = low


def diagonals(keep, recv):
    place = keep.shape[0] - 8
    return pick(keep[place : place + 1, :], recv[place : place + 1, :])


def start_chain(keep, recv, *refs):
    weights, (f_first, f_second) = refs[:PARTS], refs[PARTS:]
    rows = f_first.shape[0]

    @pl.when(pair() == 0)
    def _():
        first, second = pick(keep[:rows, :], recv[:rows, :])
        f_first[...] = first
        f_second[...] = second + times(first, weights, 1)


def start_last(keep, recv, *refs):
    weights, (f_first, f_second, k_first, k_second) = refs[:PARTS], refs[PARTS:]
    rows, extra = f_first.shape[0], k_first.shape[0]
    stop = keep.shape[0] - 8

    @pl.when(pair() == 0)
    def _():
        at = stop - extra - rows
        first, second = pick(keep[at:stop, :], recv[at:stop, :])
        second = second + times(first, weights, 1)
        f_first[...] = first[:rows]
        f_second[...] = second[:rows]
        k_first[...] = first[rows:]
        k_second[...] = second[rows:]


def top_one(at, keep, recv, carried, *refs):
    weights, (n_first, n_second) = refs[:PARTS], refs[PARTS:]
    rows = n_first.shape[0]

    @pl.when(pair() == 1)
    def _():
        first, second = pick(keep[at : at + rows, :], recv[at : at + rows, :])
        first = first + times(carried[...], weights, 0)
        second = second + times(first, weights, 1)
        n_first[...] = first + times(second, weights, 0)
        n_second[...] = second


def top_two(with_basis, keep, recv, v_first, v_second, carried, *refs):
    riding, weights, (n_first, n_second) = refs[0], refs[1 : 1 + PARTS], refs[1 + PARTS :]
    rows = v_first.shape[0]
    few = riding.shape[0] // 2
    extra = 2 * few
    at = keep.shape[0] - 8 - extra

    @pl.when(pair() == 1)
    def _():
        d_first, d_second = diagonals(keep, recv)
        x = d_first * v_first[...] + carried[...]
        if with_basis:
            here = pl.ds(pl.multiple_of(at + member() * few, 8), few)
            k_first, k_second = pick(keep[here, :], recv[here, :])
            first = times(jnp.concatenate([x, riding[few:, :]], axis=0), weights, 0)
            k_first = first[rows:] + k_first
            y = d_second * v_second[...] + first[:rows]
            second = times(jnp.concatenate([y, k_first], axis=0), weights, 1)
            first = jnp.concatenate([first[:rows], k_first], axis=0)
            second = jnp.concatenate([second[:rows], second[rows:] + k_second], axis=0)
        else:
            first = times(x, weights, 0)
            second = times(d_second * v_second[...] + first, weights, 1)
        n_first[...] = first + times(second, weights, 0)
        n_second[...] = second


def down(f_first, f_second, carried, weights):
    second = f_second + times(carried, weights, 1)
    return f_first + times(second, weights, 0), second


def turn(keep, recv, f_first, f_second, carried, *refs):
    weights, old = refs[:PARTS], refs[PARTS : PARTS + 2]
    n_first, n_second, g_first, g_second = refs[PARTS + 2 :]

    @pl.when(pair() == 0)
    def _():
        first, second = down(f_first[...], f_second[...], carried[...], weights)
        n_second[...] = second
        n_first[...] = first
        d_first, d_second = diagonals(keep, recv)
        again = times(d_first * first, weights, 0)
        g_first[...] = again
        g_second[...] = times(d_second * second + again, weights, 1)

    hold(pair() != 0, old, (n_first, n_second))


def back(with_basis, f_first, f_second, k_first, k_second, carried, *refs):
    weights, old, (n_first, n_second) = refs[:PARTS], refs[PARTS : PARTS + 2], refs[PARTS + 2 :]
    few = k_first.shape[0] // 2

    @pl.when(pair() == 0)
    def _():
        first, second = f_first[...], f_second[...]
        if with_basis:
            here = pl.ds(pl.multiple_of(member() * few, 8), few)
            first = jnp.concatenate([first, k_first[here, :]], axis=0)
            second = jnp.concatenate([second, k_second[here, :]], axis=0)
        n_first[...], n_second[...] = down(first, second, carried[...], weights)

    hold(pair() != 0, old, (n_first, n_second))


def adjoint_start(own_spots, oth_spots, k_second, *refs):
    weights, (y_first, y_second, sent) = refs[:PARTS], refs[PARTS:]
    prim = y_first.shape[0]

    @pl.when(pair() == 0)
    def _():
        first, second = pick(own_spots[...], oth_spots[...])
        second = second + times_transposed(first, weights, 0)
        y_first[...] = first
        y_second[...] = second
        sent[:prim, :] = times_transposed(second, weights, 1)
        sent[prim:, :] = k_second[pl.ds(pl.multiple_of(member() * prim, 8), prim), :]


def placed(u, places, width):
    prim = u.shape[0]
    zero = jnp.zeros_like(u)
    rows = [u if i in places else zero for i in range(width // prim)]
    return jnp.concatenate(rows, axis=0)


def score(x, u):
    top, low = halves(u)
    return three(x, top, low, dot_rows)


def only(x, place, prim):
    lane = lax.broadcasted_iota(jnp.int32, x.shape, 1)
    return jnp.where((lane >= place * prim) & (lane < (place + 1) * prim), x, 0.0)


def pack(values, out, at):
    rows, width = values.shape
    per = out.shape[1] // width
    for j in range(rows // 8):
        row = at + (j // per) * 8
        out[row : row + 8, (j % per) * width : (j % per + 1) * width] = values[8 * j : 8 * j + 8, :]


def unpack(packed, at, rows, width):
    per = packed.shape[1] // width
    return jnp.concatenate(
        [
            packed[
                at + (j // per) * 8 : at + (j // per) * 8 + 8,
                (j % per) * width : (j % per + 1) * width,
            ]
            for j in range(rows // 8)
        ],
        axis=0,
    )


def adjoint_top(width, keep, recv, own_spots, oth_spots, carried, *refs):
    weights, refs = refs[:PARTS], refs[PARTS:]
    blocks, old, (y_first, y_second, sent) = refs[: 2 * BLOCKS], refs[2 * BLOCKS : -3], refs[-3:]
    prim = y_first.shape[0]

    @pl.when(pair() == 1)
    def _():
        first, second = pick(own_spots[...], oth_spots[...])
        first = first + carried[:prim, :]
        second = second + times_transposed(first, weights, 0)
        z_second = times_transposed(second, weights, 1)
        first = first + z_second
        z_first = times_transposed(first, weights, 0)
        sent[:prim, :] = z_first
        w_first, w_second = pick(keep[...], recv[...])
        stop = w_first.shape[0] - 8
        w = score(w_first[:stop], placed(first, (0, 2), width)) + score(
            w_second[:stop], placed(second, (0, 2), width)
        )
        d_first, d_second = diagonals(keep, recv)
        n_first = jnp.concatenate([r[...] for r in blocks[0::2]], axis=0)
        n_second = jnp.concatenate([r[...] for r in blocks[1::2]], axis=0)
        g = score(d_first * n_first, placed(z_first, (1,), width)) + score(
            d_second * n_second, placed(z_second, (1,), width)
        )
        half = n_first.shape[0]
        pack(only(w[:half], 0, prim) + g + only(w[half:], 2, prim), sent, prim)

    hold(pair() != 1, old, (y_first, y_second))


def score_turn(carried, y_first, y_second, k_first, k_second, *refs):
    blocks, values = refs[:-1], refs[-1]
    prim = y_first.shape[0]
    half, width = values.shape

    @pl.when(pair() == 0)
    def _():
        first = jnp.concatenate(
            [r[...] for r in blocks[0::4]] + [k_first[...]] + [r[...] for r in blocks[2::4]], axis=0
        )
        second = jnp.concatenate(
            [r[...] for r in blocks[1::4]] + [k_second[...]] + [r[...] for r in blocks[3::4]], axis=0
        )
        w = score(first, placed(y_first[...], (0, 1, 2), width)) + score(
            second, placed(y_second[...] + carried[:prim, :], (0, 1, 2), width)
        )
        extra = k_first.shape[0]
        values[...] = (
            unpack(carried, prim, half, width)
            + only(w[:half], 0, prim)
            + only(w[half : half + extra], 2, prim)
            + only(w[half + extra :], 1, prim)
        )


def settle(*refs):
    blocks, (keep, send) = refs[: 4 * BLOCKS], refs[4 * BLOCKS :]
    rows = blocks[0].shape[0]
    for i in range(BLOCKS):
        a1, b1, a2, b2 = blocks[4 * i : 4 * i + 4]
        here = slice(i * rows, (i + 1) * rows)
        keep[here, :], send[here, :] = pick(
            2.0 * a1[...] - a2[:rows, :], 2.0 * b1[...] - b2[:rows, :]
        )
    keep[BLOCKS * rows :, :], send[BLOCKS * rows :, :] = pick(blocks[2][rows:, :], blocks[3][rows:, :])


def wide(x, rows):
    return jnp.concatenate([x, jnp.zeros((rows - x.shape[0], x.shape[1]), f32)], axis=0)


def solve(subs, prim, values, fixed, q):
    half, width = q.shape
    count = fixed.shape[1]
    height = fixed.shape[0] // subs
    share = height - prim - 8
    me = lax.axis_index("sub")
    unknown = lax.broadcasted_iota(jnp.int32, (count, width), 0)
    there = ((unknown // share) ^ me) * share + unknown % share
    unknown, there = unknown.astype(f32), there.astype(f32)
    lane = lax.broadcasted_iota(jnp.int32, (half, width), 1)

    def at(ref, j, size, start=0, stop=None):
        stop = size if stop is None else stop
        base = j * size + start
        if not isinstance(base, int):
            base = pl.multiple_of(base, 8)
        return ref[pl.ds(base, stop - start), :]

    def loop(body, begin):
        if subs <= 8:
            for j in range(subs):
                begin = body(j, begin)
            return begin
        return lax.fori_loop(0, subs, body, begin)

    def times_rows(left, right):
        top, low = halves(right)
        return three(left, top, low, dot_rows)

    def times_plain(left, right):
        top, low = halves(right)
        return three(left, top, low)

    def map_of(j):
        return at(fixed, j, height, share + prim, height)[0:1, :width]

    def spot(row, ids):
        return (ids == row).astype(f32)

    def add_first(j, total):
        return total + times_rows(at(values, j, half), spot(map_of(j), unknown))

    inverse = jnp.concatenate([at(fixed, j, height, 0, share) for j in range(subs)], axis=0)
    zero = jnp.zeros((half, count), f32)
    found = times_rows(loop(add_first, zero), inverse)

    def parts(j):
        v = at(values, j, half)
        row = map_of(j)
        schur = at(fixed, j, height, share, share + prim)[:, :width]
        multiplier = times_plain(v, wide(schur, width))
        picked = times_plain(found, spot(row, there))
        change = times_plain(multiplier, wide(v[:prim], width)) - times_plain(
            picked, wide(v[prim : 2 * prim], width)
        )
        return row, schur, multiplier, picked, jnp.where(lane < 2 * prim, v, change)

    def add_second(j, total):
        row, _, _, _, p = parts(j)
        signs = (
            spot(row, unknown)
            - spot(pltpu.roll(row, prim, 1), unknown)
            + spot(pltpu.roll(row, 2 * prim, 1), unknown)
        )
        return total + times_rows(p, signs)

    found_two = times_rows(loop(add_second, zero), inverse)
    row, schur, multiplier, picked, p = parts(0)
    multiplier_two = times_plain(p, wide(jnp.concatenate([schur, -schur, schur], axis=0), width))
    picked_two = times_plain(found_two, spot(row, there))
    q[...] = (
        pltpu.roll(picked, prim, 1)
        - multiplier
        - pltpu.roll(multiplier + multiplier_two, 2 * prim, 1)
        + pltpu.roll(picked + picked_two, 3 * prim, 1)
    )


def finish(keep, recv, q_keep, q_recv, one, two, out):
    prim = one.shape[0]
    rows = keep.shape[0] - prim
    k_low, k_high = pick(keep[rows:, :], recv[rows:, :])
    right = jnp.concatenate([-k_low, -k_high, one[...], two[...]], axis=0)
    top, low = halves(right)
    here = member()
    for n, q, which in ((keep, q_keep, here), (recv, q_recv, 1 - here)):
        out[pl.ds(pl.multiple_of(which * rows, 8), rows), :] = n[:rows, :] + three(q[...], top, low)


def on_device(
    residual,
    inverse_slab,
    diagonal,
    primal_index,
    coarse_map,
    schur_small,
    constraint_basis,
    coarse_basis,
    coarse_inverse,
):
    levels = lax.axis_size("slab")
    subs = lax.axis_size("sub")
    assert levels == 4 and subs & (subs - 1) == 0

    def swap(x):
        return lax.ppermute(x, "slab", [(i, i ^ 1) for i in range(levels)])

    def rise(x):
        return lax.ppermute(x, "slab", [(0, 2), (1, 3)])

    def fall(x):
        return lax.ppermute(x, "slab", [(2, 0), (3, 1)])

    def gather(x):
        distance = 1
        while distance < subs:
            pairs = [
                (i * levels + k, (i ^ distance) * levels + k) for i in range(subs) for k in range(2)
            ]
            other = lax.ppermute(x, ("sub", "slab"), pairs)
            x = jnp.concatenate([x, other], axis=0)
            distance *= 2
        return x

    vector = residual[0, 0]
    matrix = inverse_slab[0, 0]
    one, two = constraint_basis[0, 0], coarse_basis[0, 0]
    rows, size = vector.shape
    prim = primal_index.shape[-1]
    coarse_count, share = coarse_inverse.shape
    half = rows // 2
    block = half // BLOCKS
    extra = 2 * prim
    width = -(-3 * prim // LANES) * LANES
    packed = -(-half * width // (8 * size)) * 8
    assert half == extra and prim <= coarse_count and size % width == 0 and 4 * prim <= width

    def like(count, *heights):
        return [struct((h, size)) for h in heights for _ in range(count)]

    other_matrix = swap(matrix)

    (fixed,) = call(
        fix,
        [struct((share + prim + 8, coarse_count))],
        [coarse_inverse, schur_small[0], coarse_map],
        0.1,
    )
    fixed = gather(fixed)

    own, keep, send = call(
        first_products,
        [struct((2, size, size), bf16)] + like(2, half + extra + 8),
        [matrix, vector, one, two, diagonal[0], primal_index[0]],
        2,
        scratch=[
            pltpu.VMEM((size, size), f32),
            pltpu.VMEM((rows + extra, size), f32),
            pltpu.VMEM((rows + extra, size), f32),
            pltpu.SemaphoreType.DMA((3 + PIECES,)),
        ],
        hbm=(0, 1, 2, 3),
    )
    recv = swap(send)
    weights = call(
        split,
        [struct((2, 2, size, size), bf16)],
        [other_matrix, own],
        1,
        scratch=[pltpu.VMEM((size, size), f32), pltpu.SemaphoreType.DMA((PIECES,))],
        hbm=(0,),
    )
    place = jnp.arange(size, dtype=jnp.int32)
    own_spots = (primal_index[0, 0][:, None] == place).astype(f32)
    oth_spots = (recv[half + extra + 1, :prim][:, None] == place.astype(f32)).astype(f32)

    span = range(BLOCKS)
    f, carried = [], []
    for i in span[:-1]:
        f.append(call(start_chain, like(2, block), [keep, recv, *weights], 1))
        carried.append(rise(f[i][1]))
    *f_last, k_first, k_second = call(start_last, like(2, block, extra), [keep, recv, *weights], 1)
    f.append(f_last)
    carried.append(rise(f_last[1]))
    y_first, y_second, sent = call(
        adjoint_start,
        like(2, prim) + like(1, 2 * prim),
        [own_spots, oth_spots, k_second, *weights],
        2,
    )
    riding = rise(sent)

    n = []
    for i in span:
        n.append(
            call(
                functools.partial(top_one, i * block),
                like(2, block),
                [keep, recv, carried[i], *weights],
                3,
            )
        )
        carried[i] = fall(n[i][0])
    n_one, g = [], []
    for i in span:
        turned = call(
            turn,
            like(4, block),
            [keep, recv, *f[i], carried[i], *weights, *n[i]],
            4,
            aliases={5 + PARTS: 0, 6 + PARTS: 1},
        )
        n_one.append(turned[:2])
        g.append(turned[2:])
        carried[i] = rise(g[i][1])
        if i == 0:
            passed = [x for j in span for x in (n_one[0] if j == 0 else n[j])]
            y_first, y_second, sent = call(
                functools.partial(adjoint_top, width),
                like(2, prim) + like(1, prim + packed),
                [keep, recv, own_spots, oth_spots, riding, *weights, *passed, y_first, y_second],
                4,
                aliases={5 + PARTS + 2 * BLOCKS: 0, 6 + PARTS + 2 * BLOCKS: 1},
            )
            z_back = fall(sent)
    pieces = []
    for i in span:
        pieces += [*f[i], *g[i]]
    (values,) = call(
        score_turn,
        [struct((half, width))],
        [z_back, y_first, y_second, k_first, k_second, *pieces],
        1,
    )
    values = gather(values)

    n_two = []
    for i in span:
        n_two.append(
            call(
                functools.partial(top_two, i == 0),
                like(2, block + prim if i == 0 else block),
                [keep, recv, *n_one[i], carried[i], riding, *weights],
                3,
            )
        )
        carried[i] = fall(n_two[i][0])
    for i in span:
        n_two[i] = call(
            functools.partial(back, i == 0),
            like(2, block + prim if i == 0 else block),
            [*g[i], k_first, k_second, carried[i], *weights, *n_two[i]],
            2,
            aliases={5 + PARTS: 0, 6 + PARTS: 1},
        )
    pieces = []
    for i in span:
        pieces += [*n_one[i], *n_two[i]]
    m_keep, m_send = call(settle, like(2, half + prim), pieces, 0.5)
    m_recv = swap(m_send)

    (q,) = call(
        functools.partial(solve, subs, prim),
        [struct((half, width))],
        [values, fixed],
        0.5,
        limit=VMEM_LIMIT + 8 * (values.size + fixed.size),
    )
    q_upper = rise(q)
    q = jnp.where(pair() == 0, q, q_upper)
    q_recv = swap(q)
    (out,) = call(finish, [struct((rows, size))], [m_keep, m_recv, q, q_recv, one, two], 0.5)
    return out[None, None]


def solution(mesh):
    placed_as = (
        P("sub", "slab", None, None),
        P("sub", "slab", None, None),
        P("sub", "slab", None),
        P("sub", "slab", None),
        P("sub", None),
        P("sub", None, None),
        P("sub", "slab", None, None),
        P("sub", "slab", None, None),
        P(None, "sub"),
    )

    return jax.shard_map(
        on_device,
        mesh=mesh,
        in_specs=placed_as,
        out_specs=P("sub", "slab", None, None),
        check_vma=False,
    )
```

```python
import functools

import jax
import jax.numpy as jnp
from jax import lax
from jax.experimental import pallas as pl
from jax.experimental.pallas import tpu as pltpu
from jax.sharding import PartitionSpec as P


f32 = jnp.float32
bf16 = jnp.bfloat16
LANES = 128
BLOCKS = 2
PIECES = 4
PARTS = 1


def halves(x):
    top = x.astype(bf16)
    return top, (x - top.astype(f32)).astype(bf16)


def dot(left, right):
    return jnp.dot(left, right, preferred_element_type=f32)


def dot_rows(left, right):
    return lax.dot_general(left, right, (((1,), (1,)), ((), ())), preferred_element_type=f32)


def three(x, top_right, low_right, how=dot):
    rows = x.shape[0]
    top, low = halves(x)
    both = how(jnp.concatenate([top, low], axis=0), top_right)
    return both[:rows] + both[rows:] + how(top, low_right)


def times(x, weights, member):
    step = weights[0].shape[2]
    top, low = halves(x)
    both = jnp.concatenate([top, low], axis=0)
    rows = x.shape[0]
    first, second = 0.0, 0.0
    for i, piece in enumerate(weights):
        cols = slice(i * step, (i + 1) * step)
        first = first + dot(both[:, cols], piece[member, 0])
        second = second + dot(top[:, cols], piece[member, 1])
    return first[:rows] + first[rows:] + second


def times_transposed(x, weights, member):
    return jnp.concatenate(
        [three(x, piece[member, 0], piece[member, 1], dot_rows) for piece in weights], axis=1
    )


def member():
    return lax.axis_index("slab") & 1


def pair():
    return lax.axis_index("slab") >> 1


def spec(space):
    return pl.BlockSpec(memory_space=space)


def call(body, outs, args, work, aliases=None, scratch=(), hbm=(), limit=None):
    specs = [spec(pltpu.VMEM) for _ in args]
    args = list(args)
    for place in hbm:
        specs[place] = spec(pltpu.HBM)
        args[place] = pltpu.with_memory_space_constraint(args[place], pltpu.HBM)
    return pl.pallas_call(
        body,
        out_shape=outs,
        in_specs=specs,
        out_specs=[spec(pltpu.VMEM) for _ in outs],
        input_output_aliases=aliases or {},
        scratch_shapes=list(scratch),
        cost_estimate=pl.CostEstimate(flops=int(work * 8e8), bytes_accessed=0, transcendentals=0),
        compiler_params=pltpu.CompilerParams(vmem_limit_bytes=limit or VMEM_LIMIT),
    )(*args)


VMEM_LIMIT = 16 << 20


def struct(shape, dtype=f32):
    return jax.ShapeDtypeStruct(shape, dtype)


def pick(own, oth):
    first = member() == 0
    return jnp.where(first, own, oth), jnp.where(first, oth, own)


def hold(idle, before, after):
    @pl.when(idle)
    def _():
        for old, new in zip(before, after):
            new[...] = old[...]


def fix(inverse_far, schur_far, maps_far, out, inverse, schur, maps, sems):
    copies = [
        pltpu.make_async_copy(far, near, sems.at[i])
        for i, (far, near) in enumerate(
            ((inverse_far, inverse), (schur_far, schur), (maps_far, maps))
        )
    ]
    for copy in copies:
        copy.start()
    for copy in copies:
        copy.wait()
    share, prim = inverse.shape[1], schur.shape[0]
    unit = lax.broadcasted_iota(jnp.int32, (share, share), 0) == lax.broadcasted_iota(
        jnp.int32, (share, share), 1
    )
    unit = unit.astype(f32).astype(bf16)
    top, low = halves(inverse[...])
    rest = (inverse[...] - top.astype(f32) - low.astype(f32)).astype(bf16)
    out[:share, :] = dot_rows(unit, top) + dot_rows(unit, low) + dot_rows(unit, rest)
    out[share : share + prim, :] = jnp.zeros_like(out[share : share + prim, :])
    out[share : share + prim, :prim] = schur[...]
    out[share + prim :, :] = jnp.full_like(out[share + prim :, :], -1.0)
    out[share + prim : share + prim + 1, :prim] = maps[...].astype(f32)


def first_products(
    matrix, vector, one, two, diagonal_far, index_far, own, keep, send, buffer, x, total, diagonal, index, sems
):
    size = matrix.shape[0]
    step = size // PIECES
    rows, prim = vector.shape[0], one.shape[0]
    extra = 2 * prim
    copies = [
        pltpu.make_async_copy(vector, x.at[pl.ds(0, rows)], sems.at[0]),
        pltpu.make_async_copy(one, x.at[pl.ds(rows, prim)], sems.at[1]),
        pltpu.make_async_copy(two, x.at[pl.ds(rows + prim, prim)], sems.at[2]),
        pltpu.make_async_copy(diagonal_far, diagonal, sems.at[3]),
        pltpu.make_async_copy(index_far, index, sems.at[4]),
    ]
    pieces = [
        pltpu.make_async_copy(
            matrix.at[pl.ds(i * step, step)], buffer.at[pl.ds(i * step, step)], sems.at[5 + i]
        )
        for i in range(PIECES)
    ]
    for copy in copies + pieces:
        copy.start()
    for copy in copies:
        copy.wait()
    x[rows:, :] = x[rows:, :] * diagonal[...]
    for i, copy in enumerate(pieces):
        cols = pl.ds(i * step, step)
        copy.wait()
        top, low = halves(buffer[cols, :])
        own[0, cols, :] = top
        own[1, cols, :] = low
        part = three(x[:, cols], own[0, cols, :], own[1, cols, :])
        if i == 0:
            total[...] = part
        else:
            total[...] += part
    half = rows // 2
    here, there = member(), 1 - member()
    for out, which in ((keep, here), (send, there)):
        out[:half, :] = total[pl.ds(pl.multiple_of(which * half, 8), half), :]
        out[half : half + extra, :] = total[rows:, :]
        out[half + extra :, :] = jnp.zeros_like(out[half + extra :, :])
        out[half + extra : half + extra + 1, :] = diagonal[...]
        out[half + extra + 1 : half + extra + 2, :prim] = index[...].astype(f32)


def split(matrix, own, weights, buffer, sems):
    step = matrix.shape[0] // PIECES
    pieces = [
        pltpu.make_async_copy(
            matrix.at[pl.ds(i * step, step)], buffer.at[pl.ds(i * step, step)], sems.at[i]
        )
        for i in range(PIECES)
    ]
    for copy in pieces:
        copy.start()
    here = member()
    weights[here] = own[...]
    for i, copy in enumerate(pieces):
        cols = pl.ds(i * step, step)
        copy.wait()
        top, low = halves(buffer[cols, :])
        weights[1 - here, 0, cols, :] = top
        weights[1 - here, 1, cols, :] = low


def diagonals(keep, recv):
    place = keep.shape[0] - 8
    return pick(keep[place : place + 1, :], recv[place : place + 1, :])


def start_chain(keep, recv, *refs):
    weights, (f_first, f_second) = refs[:PARTS], refs[PARTS:]
    rows = f_first.shape[0]

    @pl.when(pair() == 0)
    def _():
        first, second = pick(keep[:rows, :], recv[:rows, :])
        f_first[...] = first
        f_second[...] = second + times(first, weights, 1)


def start_last(keep, recv, *refs):
    weights, (f_first, f_second, k_first, k_second) = refs[:PARTS], refs[PARTS:]
    rows, extra = f_first.shape[0], k_first.shape[0]
    stop = keep.shape[0] - 8

    @pl.when(pair() == 0)
    def _():
        at = stop - extra - rows
        first, second = pick(keep[at:stop, :], recv[at:stop, :])
        second = second + times(first, weights, 1)
        f_first[...] = first[:rows]
        f_second[...] = second[:rows]
        k_first[...] = first[rows:]
        k_second[...] = second[rows:]


def top_one(at, keep, recv, carried, *refs):
    weights, (n_first, n_second) = refs[:PARTS], refs[PARTS:]
    rows = n_first.shape[0]

    @pl.when(pair() == 1)
    def _():
        first, second = pick(keep[at : at + rows, :], recv[at : at + rows, :])
        first = first + times(carried[...], weights, 0)
        second = second + times(first, weights, 1)
        n_first[...] = first + times(second, weights, 0)
        n_second[...] = second


def top_two(with_basis, keep, recv, v_first, v_second, carried, *refs):
    riding, weights, (n_first, n_second) = refs[0], refs[1 : 1 + PARTS], refs[1 + PARTS :]
    rows = v_first.shape[0]
    few = riding.shape[0] // 2
    extra = 2 * few
    at = keep.shape[0] - 8 - extra

    @pl.when(pair() == 1)
    def _():
        d_first, d_second = diagonals(keep, recv)
        x = d_first * v_first[...] + carried[...]
        if with_basis:
            here = pl.ds(pl.multiple_of(at + member() * few, 8), few)
            k_first, k_second = pick(keep[here, :], recv[here, :])
            first = times(jnp.concatenate([x, riding[few:, :]], axis=0), weights, 0)
            k_first = first[rows:] + k_first
            y = d_second * v_second[...] + first[:rows]
            second = times(jnp.concatenate([y, k_first], axis=0), weights, 1)
            first = jnp.concatenate([first[:rows], k_first], axis=0)
            second = jnp.concatenate([second[:rows], second[rows:] + k_second], axis=0)
        else:
            first = times(x, weights, 0)
            second = times(d_second * v_second[...] + first, weights, 1)
        n_first[...] = first + times(second, weights, 0)
        n_second[...] = second


def down(f_first, f_second, carried, weights):
    second = f_second + times(carried, weights, 1)
    return f_first + times(second, weights, 0), second


def turn(keep, recv, f_first, f_second, carried, *refs):
    weights, old = refs[:PARTS], refs[PARTS : PARTS + 2]
    n_first, n_second, g_first, g_second = refs[PARTS + 2 :]

    @pl.when(pair() == 0)
    def _():
        first, second = down(f_first[...], f_second[...], carried[...], weights)
        n_second[...] = second
        n_first[...] = first
        d_first, d_second = diagonals(keep, recv)
        again = times(d_first * first, weights, 0)
        g_first[...] = again
        g_second[...] = times(d_second * second + again, weights, 1)

    hold(pair() != 0, old, (n_first, n_second))


def back(with_basis, f_first, f_second, k_first, k_second, carried, *refs):
    weights, old, (n_first, n_second) = refs[:PARTS], refs[PARTS : PARTS + 2], refs[PARTS + 2 :]
    few = k_first.shape[0] // 2

    @pl.when(pair() == 0)
    def _():
        first, second = f_first[...], f_second[...]
        if with_basis:
            here = pl.ds(pl.multiple_of(member() * few, 8), few)
            first = jnp.concatenate([first, k_first[here, :]], axis=0)
            second = jnp.concatenate([second, k_second[here, :]], axis=0)
        n_first[...], n_second[...] = down(first, second, carried[...], weights)

    hold(pair() != 0, old, (n_first, n_second))


def adjoint_start(own_spots, oth_spots, k_second, *refs):
    weights, (y_first, y_second, sent) = refs[:PARTS], refs[PARTS:]
    prim = y_first.shape[0]

    @pl.when(pair() == 0)
    def _():
        first, second = pick(own_spots[...], oth_spots[...])
        second = second + times_transposed(first, weights, 0)
        y_first[...] = first
        y_second[...] = second
        sent[:prim, :] = times_transposed(second, weights, 1)
        sent[prim:, :] = k_second[pl.ds(pl.multiple_of(member() * prim, 8), prim), :]


def placed(u, places, width):
    prim = u.shape[0]
    zero = jnp.zeros_like(u)
    rows = [u if i in places else zero for i in range(width // prim)]
    return jnp.concatenate(rows, axis=0)


def score(x, u):
    top, low = halves(u)
    return three(x, top, low, dot_rows)


def only(x, place, prim):
    lane = lax.broadcasted_iota(jnp.int32, x.shape, 1)
    return jnp.where((lane >= place * prim) & (lane < (place + 1) * prim), x, 0.0)


def pack(values, out, at):
    rows, width = values.shape
    per = out.shape[1] // width
    for j in range(rows // 8):
        row = at + (j // per) * 8
        out[row : row + 8, (j % per) * width : (j % per + 1) * width] = values[8 * j : 8 * j + 8, :]


def unpack(packed, at, rows, width):
    per = packed.shape[1] // width
    return jnp.concatenate(
        [
            packed[
                at + (j // per) * 8 : at + (j // per) * 8 + 8,
                (j % per) * width : (j % per + 1) * width,
            ]
            for j in range(rows // 8)
        ],
        axis=0,
    )


def adjoint_top(width, keep, recv, own_spots, oth_spots, carried, *refs):
    weights, refs = refs[:PARTS], refs[PARTS:]
    blocks, old, (y_first, y_second, sent) = refs[: 2 * BLOCKS], refs[2 * BLOCKS : -3], refs[-3:]
    prim = y_first.shape[0]

    @pl.when(pair() == 1)
    def _():
        first, second = pick(own_spots[...], oth_spots[...])
        first = first + carried[:prim, :]
        second = second + times_transposed(first, weights, 0)
        z_second = times_transposed(second, weights, 1)
        first = first + z_second
        z_first = times_transposed(first, weights, 0)
        sent[:prim, :] = z_first
        w_first, w_second = pick(keep[...], recv[...])
        stop = w_first.shape[0] - 8
        w = score(w_first[:stop], placed(first, (0, 2), width)) + score(
            w_second[:stop], placed(second, (0, 2), width)
        )
        d_first, d_second = diagonals(keep, recv)
        n_first = jnp.concatenate([r[...] for r in blocks[0::2]], axis=0)
        n_second = jnp.concatenate([r[...] for r in blocks[1::2]], axis=0)
        g = score(d_first * n_first, placed(z_first, (1,), width)) + score(
            d_second * n_second, placed(z_second, (1,), width)
        )
        half = n_first.shape[0]
        pack(only(w[:half], 0, prim) + g + only(w[half:], 2, prim), sent, prim)

    hold(pair() != 1, old, (y_first, y_second))


def score_turn(carried, y_first, y_second, k_first, k_second, *refs):
    blocks, values = refs[:-1], refs[-1]
    prim = y_first.shape[0]
    half, width = values.shape

    @pl.when(pair() == 0)
    def _():
        first = jnp.concatenate(
            [r[...] for r in blocks[0::4]] + [k_first[...]] + [r[...] for r in blocks[2::4]], axis=0
        )
        second = jnp.concatenate(
            [r[...] for r in blocks[1::4]] + [k_second[...]] + [r[...] for r in blocks[3::4]], axis=0
        )
        w = score(first, placed(y_first[...], (0, 1, 2), width)) + score(
            second, placed(y_second[...] + carried[:prim, :], (0, 1, 2), width)
        )
        extra = k_first.shape[0]
        values[...] = (
            unpack(carried, prim, half, width)
            + only(w[:half], 0, prim)
            + only(w[half : half + extra], 2, prim)
            + only(w[half + extra :], 1, prim)
        )


def settle(*refs):
    blocks, (keep, send) = refs[: 4 * BLOCKS], refs[4 * BLOCKS :]
    rows = blocks[0].shape[0]
    for i in range(BLOCKS):
        a1, b1, a2, b2 = blocks[4 * i : 4 * i + 4]
        here = slice(i * rows, (i + 1) * rows)
        keep[here, :], send[here, :] = pick(
            2.0 * a1[...] - a2[:rows, :], 2.0 * b1[...] - b2[:rows, :]
        )
    keep[BLOCKS * rows :, :], send[BLOCKS * rows :, :] = pick(blocks[2][rows:, :], blocks[3][rows:, :])


def wide(x, rows):
    return jnp.concatenate([x, jnp.zeros((rows - x.shape[0], x.shape[1]), f32)], axis=0)


def solve(subs, prim, values, fixed, q):
    half, width = q.shape
    count = fixed.shape[1]
    height = fixed.shape[0] // subs
    share = height - prim - 8
    me = lax.axis_index("sub")
    unknown = lax.broadcasted_iota(jnp.int32, (count, width), 0)
    block = unknown // share
    far = jnp.zeros_like(block)
    for bit in range(subs.bit_length() - 1):
        far = far | (((block >> bit) & 1) << (subs.bit_length() - 2 - bit))
    there = (far ^ me) * share + unknown % share
    unknown, there = unknown.astype(f32), there.astype(f32)
    lane = lax.broadcasted_iota(jnp.int32, (half, width), 1)

    def at(ref, j, size, start=0, stop=None):
        stop = size if stop is None else stop
        base = j * size + start
        if not isinstance(base, int):
            base = pl.multiple_of(base, 8)
        return ref[pl.ds(base, stop - start), :]

    def loop(body, begin):
        if subs <= 8:
            for j in range(subs):
                begin = body(j, begin)
            return begin
        return lax.fori_loop(0, subs, body, begin)

    def times_rows(left, right):
        top, low = halves(right)
        return three(left, top, low, dot_rows)

    def times_plain(left, right):
        top, low = halves(right)
        return three(left, top, low)

    def map_of(j):
        return at(fixed, j, height, share + prim, height)[0:1, :width]

    def spot(row, ids):
        return (ids == row).astype(f32)

    def pick_plain(left, spots):
        top, low = halves(left)
        both = dot(jnp.concatenate([top, low], axis=0), spots.astype(bf16))
        return both[:half] + both[half:]

    def pick_rows(left, spots):
        top, low = halves(left)
        both = dot_rows(jnp.concatenate([top, low], axis=0), spots.astype(bf16))
        return both[:half] + both[half:]

    def add_first(j, total):
        return total + pick_rows(at(values, j, half), spot(map_of(j), unknown))

    inverse = jnp.concatenate([at(fixed, j, height, 0, share) for j in range(subs)], axis=0)
    zero = jnp.zeros((half, count), f32)
    found = times_rows(loop(add_first, zero), inverse)

    def parts(j):
        v = at(values, j, half)
        row = map_of(j)
        schur = at(fixed, j, height, share, share + prim)[:, :width]
        first = pick_plain(found, spot(pltpu.roll(row, prim, 1), there)) - times_plain(
            v, wide(schur, width)
        )
        change = times_plain(first, wide(v[: 2 * prim], width))
        return row, schur, first, jnp.where(lane < 2 * prim, v, change)

    def add_second(j, total):
        row, _, _, p = parts(j)
        signs = (
            spot(row, unknown)
            - spot(pltpu.roll(row, prim, 1), unknown)
            - spot(pltpu.roll(row, 2 * prim, 1), unknown)
        )
        return total + pick_rows(p, signs)

    found_two = times_rows(loop(add_second, zero), inverse)
    row, schur, first, p = parts(0)
    second = pick_plain(found_two, spot(pltpu.roll(row, prim, 1), there)) - times_plain(
        p, wide(jnp.concatenate([schur, -schur, -schur], axis=0), width)
    )
    q[...] = first + pltpu.roll(first + second, 2 * prim, 1)


def finish(keep, recv, q_keep, q_recv, one, two, out):
    prim = one.shape[0]
    rows = keep.shape[0] - prim
    k_low, k_high = pick(keep[rows:, :], recv[rows:, :])
    right = jnp.concatenate([-k_low, -k_high, one[...], two[...]], axis=0)
    top, low = halves(right)
    here = member()
    for n, q, which in ((keep, q_keep, here), (recv, q_recv, 1 - here)):
        out[pl.ds(pl.multiple_of(which * rows, 8), rows), :] = n[:rows, :] + three(q[...], top, low)


def on_device(
    residual,
    inverse_slab,
    diagonal,
    primal_index,
    coarse_map,
    schur_small,
    constraint_basis,
    coarse_basis,
    coarse_inverse,
):
    levels = lax.axis_size("slab")
    subs = lax.axis_size("sub")
    assert levels == 4 and subs & (subs - 1) == 0

    def swap(x):
        return lax.ppermute(x, "slab", [(i, i ^ 1) for i in range(levels)])

    def rise(x):
        return lax.ppermute(x, "slab", [(0, 2), (1, 3)])

    def fall(x):
        return lax.ppermute(x, "slab", [(2, 0), (3, 1)])

    def gather(x, which):
        distance = subs // 2
        while distance:
            pairs = [
                (i * levels + k, (i ^ distance) * levels + k)
                for i in range(subs)
                for k in (2 * which, 2 * which + 1)
            ]
            other = lax.ppermute(x, ("sub", "slab"), pairs)
            x = jnp.concatenate([x, other], axis=0)
            distance //= 2
        return x

    vector = residual[0, 0]
    matrix = inverse_slab[0, 0]
    one, two = constraint_basis[0, 0], coarse_basis[0, 0]
    rows, size = vector.shape
    prim = primal_index.shape[-1]
    coarse_count, share = coarse_inverse.shape
    half = rows // 2
    block = half // BLOCKS
    extra = 2 * prim
    width = -(-3 * prim // LANES) * LANES
    packed = -(-half * width // (8 * size)) * 8
    assert half == extra and prim <= coarse_count and size % width == 0 and 4 * prim <= width

    def like(count, *heights):
        return [struct((h, size)) for h in heights for _ in range(count)]

    other_matrix = swap(matrix)

    (fixed,) = call(
        fix,
        [struct((share + prim + 8, coarse_count))],
        [coarse_inverse, schur_small[0], coarse_map],
        0.1,
        scratch=[
            pltpu.VMEM(coarse_inverse.shape, f32),
            pltpu.VMEM((prim, prim), f32),
            pltpu.VMEM(coarse_map.shape, jnp.int32),
            pltpu.SemaphoreType.DMA((3,)),
        ],
        hbm=(0, 1, 2),
    )
    fixed = gather(fixed, 1)

    own, keep, send = call(
        first_products,
        [struct((2, size, size), bf16)] + like(2, half + extra + 8),
        [matrix, vector, one, two, diagonal[0], primal_index[0]],
        2,
        scratch=[
            pltpu.VMEM((size, size), f32),
            pltpu.VMEM((rows + extra, size), f32),
            pltpu.VMEM((rows + extra, size), f32),
            pltpu.VMEM((1, size), f32),
            pltpu.VMEM((1, prim), jnp.int32),
            pltpu.SemaphoreType.DMA((5 + PIECES,)),
        ],
        hbm=(0, 1, 2, 3, 4, 5),
    )
    recv = swap(send)
    weights = call(
        split,
        [struct((2, 2, size, size), bf16)],
        [other_matrix, own],
        1,
        scratch=[pltpu.VMEM((size, size), f32), pltpu.SemaphoreType.DMA((PIECES,))],
        hbm=(0,),
    )
    place = jnp.arange(size, dtype=jnp.int32)
    own_spots = (primal_index[0, 0][:, None] == place).astype(f32)
    oth_spots = (recv[half + extra + 1, :prim][:, None] == place.astype(f32)).astype(f32)

    span = range(BLOCKS)
    f, carried = [], []
    for i in span[:-1]:
        f.append(call(start_chain, like(2, block), [keep, recv, *weights], 1))
        carried.append(rise(f[i][1]))
    *f_last, k_first, k_second = call(start_last, like(2, block, extra), [keep, recv, *weights], 1)
    f.append(f_last)
    carried.append(rise(f_last[1]))
    y_first, y_second, sent = call(
        adjoint_start,
        like(2, prim) + like(1, 2 * prim),
        [own_spots, oth_spots, k_second, *weights],
        2,
    )
    riding = rise(sent)

    n = []
    for i in span:
        n.append(
            call(
                functools.partial(top_one, i * block),
                like(2, block),
                [keep, recv, carried[i], *weights],
                3,
            )
        )
        carried[i] = fall(n[i][0])
    n_one, g = [], []
    for i in span:
        turned = call(
            turn,
            like(4, block),
            [keep, recv, *f[i], carried[i], *weights, *n[i]],
            4,
            aliases={5 + PARTS: 0, 6 + PARTS: 1},
        )
        n_one.append(turned[:2])
        g.append(turned[2:])
        carried[i] = rise(g[i][1])
        if i == 0:
            passed = [x for j in span for x in (n_one[0] if j == 0 else n[j])]
            y_first, y_second, sent = call(
                functools.partial(adjoint_top, width),
                like(2, prim) + like(1, prim + packed),
                [keep, recv, own_spots, oth_spots, riding, *weights, *passed, y_first, y_second],
                4,
                aliases={5 + PARTS + 2 * BLOCKS: 0, 6 + PARTS + 2 * BLOCKS: 1},
            )
            z_back = fall(sent)
    pieces = []
    for i in span:
        pieces += [*f[i], *g[i]]
    (values,) = call(
        score_turn,
        [struct((half, width))],
        [z_back, y_first, y_second, k_first, k_second, *pieces],
        1,
    )
    values = gather(values, 0)

    n_two = []
    for i in span:
        n_two.append(
            call(
                functools.partial(top_two, i == 0),
                like(2, block + prim if i == 0 else block),
                [keep, recv, *n_one[i], carried[i], riding, *weights],
                3,
            )
        )
        carried[i] = fall(n_two[i][0])
    for i in span:
        n_two[i] = call(
            functools.partial(back, i == 0),
            like(2, block + prim if i == 0 else block),
            [*g[i], k_first, k_second, carried[i], *weights, *n_two[i]],
            2,
            aliases={5 + PARTS: 0, 6 + PARTS: 1},
        )
    pieces = []
    for i in span:
        pieces += [*n_one[i], *n_two[i]]
    m_keep, m_send = call(settle, like(2, half + prim), pieces, 0.5)
    m_recv = swap(m_send)

    fixed = fall(fixed)
    (q,) = call(
        functools.partial(solve, subs, prim),
        [struct((half, width))],
        [values, fixed],
        0.5,
        limit=VMEM_LIMIT + 8 * (values.size + fixed.size),
    )
    q_upper = rise(q)
    q = jnp.where(pair() == 0, q, q_upper)
    q_recv = swap(q)
    (out,) = call(finish, [struct((rows, size))], [m_keep, m_recv, q, q_recv, one, two], 0.5)
    return out[None, None]


def solution(mesh):
    placed_as = (
        P("sub", "slab", None, None),
        P("sub", "slab", None, None),
        P("sub", "slab", None),
        P("sub", "slab", None),
        P("sub", None),
        P("sub", None, None),
        P("sub", "slab", None, None),
        P("sub", "slab", None, None),
        P(None, "sub"),
    )

    return jax.shard_map(
        on_device,
        mesh=mesh,
        in_specs=placed_as,
        out_specs=P("sub", "slab", None, None),
        check_vma=False,
    )
```

```python
import functools

import jax
import jax.numpy as jnp
from jax import lax
from jax.experimental import pallas as pl
from jax.experimental.pallas import tpu as pltpu
from jax.sharding import PartitionSpec as P


f32 = jnp.float32
bf16 = jnp.bfloat16
LANES = 128
BLOCKS = 2
PIECES = 4
PARTS = 1


def halves(x):
    top = x.astype(bf16)
    return top, (x - top.astype(f32)).astype(bf16)


def dot(left, right):
    return jnp.dot(left, right, preferred_element_type=f32)


def dot_rows(left, right):
    return lax.dot_general(left, right, (((1,), (1,)), ((), ())), preferred_element_type=f32)


def three(x, top_right, low_right, how=dot):
    rows = x.shape[0]
    top, low = halves(x)
    both = how(jnp.concatenate([top, low], axis=0), top_right)
    return both[:rows] + both[rows:] + how(top, low_right)


def times(x, weights, member):
    step = weights[0].shape[2]
    top, low = halves(x)
    both = jnp.concatenate([top, low], axis=0)
    rows = x.shape[0]
    first, second = 0.0, 0.0
    for i, piece in enumerate(weights):
        cols = slice(i * step, (i + 1) * step)
        first = first + dot(both[:, cols], piece[member, 0])
        second = second + dot(top[:, cols], piece[member, 1])
    return first[:rows] + first[rows:] + second


def times_transposed(x, weights, member):
    return jnp.concatenate(
        [three(x, piece[member, 0], piece[member, 1], dot_rows) for piece in weights], axis=1
    )


def member():
    return lax.axis_index("slab") & 1


def pair():
    return lax.axis_index("slab") >> 1


def spec(space):
    return pl.BlockSpec(memory_space=space)


def call(body, outs, args, work, aliases=None, scratch=(), hbm=(), limit=None):
    specs = [spec(pltpu.VMEM) for _ in args]
    args = list(args)
    for place in hbm:
        specs[place] = spec(pltpu.HBM)
        args[place] = pltpu.with_memory_space_constraint(args[place], pltpu.HBM)
    return pl.pallas_call(
        body,
        out_shape=outs,
        in_specs=specs,
        out_specs=[spec(pltpu.VMEM) for _ in outs],
        input_output_aliases=aliases or {},
        scratch_shapes=list(scratch),
        cost_estimate=pl.CostEstimate(flops=int(work * 8e8), bytes_accessed=0, transcendentals=0),
        compiler_params=pltpu.CompilerParams(vmem_limit_bytes=limit or VMEM_LIMIT),
    )(*args)


VMEM_LIMIT = 16 << 20


def struct(shape, dtype=f32):
    return jax.ShapeDtypeStruct(shape, dtype)


def pick(own, oth):
    first = member() == 0
    return jnp.where(first, own, oth), jnp.where(first, oth, own)


def hold(idle, before, after):
    @pl.when(idle)
    def _():
        for old, new in zip(before, after):
            new[...] = old[...]


def fix(inverse_far, schur_far, maps_far, out, inverse, schur, maps, sems):
    copies = [
        pltpu.make_async_copy(far, near, sems.at[i])
        for i, (far, near) in enumerate(
            ((inverse_far, inverse), (schur_far, schur), (maps_far, maps))
        )
    ]
    for copy in copies:
        copy.start()
    for copy in copies:
        copy.wait()
    share, prim = inverse.shape[0], schur.shape[0]
    out[:share, :] = inverse[...]
    out[share : share + prim, :] = jnp.zeros_like(out[share : share + prim, :])
    out[share : share + prim, :prim] = schur[...]
    out[share + prim :, :] = jnp.full_like(out[share + prim :, :], -1.0)
    out[share + prim : share + prim + 1, :prim] = maps[...].astype(f32)


def first_products(
    matrix, vector, one, two, diagonal_far, index_far, own, keep, send, buffer, x, total, diagonal, index, sems
):
    size = matrix.shape[0]
    step = size // PIECES
    rows, prim = vector.shape[0], one.shape[0]
    extra = 2 * prim
    copies = [
        pltpu.make_async_copy(vector, x.at[pl.ds(0, rows)], sems.at[0]),
        pltpu.make_async_copy(one, x.at[pl.ds(rows, prim)], sems.at[1]),
        pltpu.make_async_copy(two, x.at[pl.ds(rows + prim, prim)], sems.at[2]),
        pltpu.make_async_copy(diagonal_far, diagonal, sems.at[3]),
        pltpu.make_async_copy(index_far, index, sems.at[4]),
    ]
    pieces = [
        pltpu.make_async_copy(
            matrix.at[pl.ds(i * step, step)], buffer.at[pl.ds(i * step, step)], sems.at[5 + i]
        )
        for i in range(PIECES)
    ]
    for copy in copies + pieces:
        copy.start()
    for copy in copies:
        copy.wait()
    x[rows:, :] = x[rows:, :] * diagonal[...]
    for i, copy in enumerate(pieces):
        cols = pl.ds(i * step, step)
        copy.wait()
        top, low = halves(buffer[cols, :])
        own[0, cols, :] = top
        own[1, cols, :] = low
        part = three(x[:, cols], own[0, cols, :], own[1, cols, :])
        if i == 0:
            total[...] = part
        else:
            total[...] += part
    half = rows // 2
    here, there = member(), 1 - member()
    for out, which in ((keep, here), (send, there)):
        out[:half, :] = total[pl.ds(pl.multiple_of(which * half, 8), half), :]
        out[half : half + extra, :] = total[rows:, :]
        out[half + extra :, :] = jnp.zeros_like(out[half + extra :, :])
        out[half + extra : half + extra + 1, :] = diagonal[...]
        out[half + extra + 1 : half + extra + 2, :prim] = index[...].astype(f32)


def split(matrix, own, weights):
    here = member()
    weights[here] = own[...]
    top, low = halves(matrix[...])
    weights[1 - here, 0] = top
    weights[1 - here, 1] = low


def diagonals(keep, recv):
    place = keep.shape[0] - 8
    return pick(keep[place : place + 1, :], recv[place : place + 1, :])


def start_chain(keep, recv, *refs):
    weights, (f_first, f_second) = refs[:PARTS], refs[PARTS:]
    rows = f_first.shape[0]

    @pl.when(pair() == 0)
    def _():
        first, second = pick(keep[:rows, :], recv[:rows, :])
        f_first[...] = first
        f_second[...] = second + times(first, weights, 1)


def start_last(keep, recv, *refs):
    weights, (f_first, f_second, k_first, k_second) = refs[:PARTS], refs[PARTS:]
    rows, extra = f_first.shape[0], k_first.shape[0]
    stop = keep.shape[0] - 8

    @pl.when(pair() == 0)
    def _():
        at = stop - extra - rows
        first, second = pick(keep[at:stop, :], recv[at:stop, :])
        second = second + times(first, weights, 1)
        f_first[...] = first[:rows]
        f_second[...] = second[:rows]
        k_first[...] = first[rows:]
        k_second[...] = second[rows:]


def top_one(at, keep, recv, carried, *refs):
    weights, (n_first, n_second) = refs[:PARTS], refs[PARTS:]
    rows = n_first.shape[0]

    @pl.when(pair() == 1)
    def _():
        first, second = pick(keep[at : at + rows, :], recv[at : at + rows, :])
        first = first + times(carried[...], weights, 0)
        second = second + times(first, weights, 1)
        n_first[...] = first + times(second, weights, 0)
        n_second[...] = second


def top_two(with_basis, keep, recv, v_first, v_second, carried, *refs):
    riding, weights, (n_first, n_second) = refs[0], refs[1 : 1 + PARTS], refs[1 + PARTS :]
    rows = v_first.shape[0]
    few = riding.shape[0] // 2
    extra = 2 * few
    at = keep.shape[0] - 8 - extra

    @pl.when(pair() == 1)
    def _():
        d_first, d_second = diagonals(keep, recv)
        x = d_first * v_first[...] + carried[...]
        if with_basis:
            here = pl.ds(pl.multiple_of(at + member() * few, 8), few)
            k_first, k_second = pick(keep[here, :], recv[here, :])
            first = times(jnp.concatenate([x, riding[few:, :]], axis=0), weights, 0)
            k_first = first[rows:] + k_first
            y = d_second * v_second[...] + first[:rows]
            second = times(jnp.concatenate([y, k_first], axis=0), weights, 1)
            first = jnp.concatenate([first[:rows], k_first], axis=0)
            second = jnp.concatenate([second[:rows], second[rows:] + k_second], axis=0)
        else:
            first = times(x, weights, 0)
            second = times(d_second * v_second[...] + first, weights, 1)
        n_first[...] = first + times(second, weights, 0)
        n_second[...] = second


def down(f_first, f_second, carried, weights):
    second = f_second + times(carried, weights, 1)
    return f_first + times(second, weights, 0), second


def turn(keep, recv, f_first, f_second, carried, *refs):
    weights, old = refs[:PARTS], refs[PARTS : PARTS + 2]
    n_first, n_second, g_first, g_second = refs[PARTS + 2 :]

    @pl.when(pair() == 0)
    def _():
        first, second = down(f_first[...], f_second[...], carried[...], weights)
        n_second[...] = second
        n_first[...] = first
        d_first, d_second = diagonals(keep, recv)
        again = times(d_first * first, weights, 0)
        g_first[...] = again
        g_second[...] = times(d_second * second + again, weights, 1)

    hold(pair() != 0, old, (n_first, n_second))


def back(with_basis, f_first, f_second, k_first, k_second, carried, *refs):
    weights, old, (n_first, n_second) = refs[:PARTS], refs[PARTS : PARTS + 2], refs[PARTS + 2 :]
    few = k_first.shape[0] // 2

    @pl.when(pair() == 0)
    def _():
        first, second = f_first[...], f_second[...]
        if with_basis:
            here = pl.ds(pl.multiple_of(member() * few, 8), few)
            first = jnp.concatenate([first, k_first[here, :]], axis=0)
            second = jnp.concatenate([second, k_second[here, :]], axis=0)
        n_first[...], n_second[...] = down(first, second, carried[...], weights)

    hold(pair() != 0, old, (n_first, n_second))


def adjoint_start(own_spots, oth_spots, k_second, *refs):
    weights, (y_first, y_second, sent) = refs[:PARTS], refs[PARTS:]
    prim = y_first.shape[0]

    @pl.when(pair() == 0)
    def _():
        first, second = pick(own_spots[...], oth_spots[...])
        second = second + times_transposed(first, weights, 0)
        y_first[...] = first
        y_second[...] = second
        sent[:prim, :] = times_transposed(second, weights, 1)
        sent[prim:, :] = k_second[pl.ds(pl.multiple_of(member() * prim, 8), prim), :]


def placed(u, places, width):
    prim = u.shape[0]
    zero = jnp.zeros_like(u)
    rows = [u if i in places else zero for i in range(width // prim)]
    return jnp.concatenate(rows, axis=0)


def score(x, u):
    top, low = halves(u)
    return three(x, top, low, dot_rows)


def only(x, place, prim):
    lane = lax.broadcasted_iota(jnp.int32, x.shape, 1)
    return jnp.where((lane >= place * prim) & (lane < (place + 1) * prim), x, 0.0)


def pack(values, out, at):
    rows, width = values.shape
    per = out.shape[1] // width
    for j in range(rows // 8):
        row = at + (j // per) * 8
        out[row : row + 8, (j % per) * width : (j % per + 1) * width] = values[8 * j : 8 * j + 8, :]


def unpack(packed, at, rows, width):
    per = packed.shape[1] // width
    return jnp.concatenate(
        [
            packed[
                at + (j // per) * 8 : at + (j // per) * 8 + 8,
                (j % per) * width : (j % per + 1) * width,
            ]
            for j in range(rows // 8)
        ],
        axis=0,
    )


def adjoint_top(width, keep, recv, own_spots, oth_spots, carried, *refs):
    weights, refs = refs[:PARTS], refs[PARTS:]
    blocks, old, (y_first, y_second, sent) = refs[: 2 * BLOCKS], refs[2 * BLOCKS : -3], refs[-3:]
    prim = y_first.shape[0]

    @pl.when(pair() == 1)
    def _():
        first, second = pick(own_spots[...], oth_spots[...])
        first = first + carried[:prim, :]
        second = second + times_transposed(first, weights, 0)
        z_second = times_transposed(second, weights, 1)
        first = first + z_second
        z_first = times_transposed(first, weights, 0)
        sent[:prim, :] = z_first
        w_first, w_second = pick(keep[...], recv[...])
        stop = w_first.shape[0] - 8
        w = score(w_first[:stop], placed(first, (0, 2), width)) + score(
            w_second[:stop], placed(second, (0, 2), width)
        )
        d_first, d_second = diagonals(keep, recv)
        n_first = jnp.concatenate([r[...] for r in blocks[0::2]], axis=0)
        n_second = jnp.concatenate([r[...] for r in blocks[1::2]], axis=0)
        g = score(d_first * n_first, placed(z_first, (1,), width)) + score(
            d_second * n_second, placed(z_second, (1,), width)
        )
        half = n_first.shape[0]
        pack(only(w[:half], 0, prim) + g + only(w[half:], 2, prim), sent, prim)

    hold(pair() != 1, old, (y_first, y_second))


def score_turn(carried, y_first, y_second, k_first, k_second, *refs):
    blocks, values = refs[:-1], refs[-1]
    prim = y_first.shape[0]
    half, width = values.shape

    @pl.when(pair() == 0)
    def _():
        first = jnp.concatenate(
            [r[...] for r in blocks[0::4]] + [k_first[...]] + [r[...] for r in blocks[2::4]], axis=0
        )
        second = jnp.concatenate(
            [r[...] for r in blocks[1::4]] + [k_second[...]] + [r[...] for r in blocks[3::4]], axis=0
        )
        w = score(first, placed(y_first[...], (0, 1, 2), width)) + score(
            second, placed(y_second[...] + carried[:prim, :], (0, 1, 2), width)
        )
        extra = k_first.shape[0]
        values[...] = (
            unpack(carried, prim, half, width)
            + only(w[:half], 0, prim)
            + only(w[half : half + extra], 2, prim)
            + only(w[half + extra :], 1, prim)
        )


def settle(*refs):
    blocks, (keep, send) = refs[: 4 * BLOCKS], refs[4 * BLOCKS :]
    rows = blocks[0].shape[0]
    for i in range(BLOCKS):
        a1, b1, a2, b2 = blocks[4 * i : 4 * i + 4]
        here = slice(i * rows, (i + 1) * rows)
        keep[here, :], send[here, :] = pick(
            2.0 * a1[...] - a2[:rows, :], 2.0 * b1[...] - b2[:rows, :]
        )
    keep[BLOCKS * rows :, :], send[BLOCKS * rows :, :] = pick(blocks[2][rows:, :], blocks[3][rows:, :])


def wide(x, rows):
    return jnp.concatenate([x, jnp.zeros((rows - x.shape[0], x.shape[1]), f32)], axis=0)


def solve(subs, prim, values, fixed, q):
    half, width = q.shape
    count = fixed.shape[1]
    height = fixed.shape[0] // subs
    share = height - prim - 8
    me = lax.axis_index("sub")
    unknown = lax.broadcasted_iota(jnp.int32, (count, width), 0)
    block = unknown // share
    far = jnp.zeros_like(block)
    for bit in range(subs.bit_length() - 1):
        far = far | (((block >> bit) & 1) << (subs.bit_length() - 2 - bit))
    there = (far ^ me) * share + unknown % share
    unknown, there = unknown.astype(f32), there.astype(f32)
    lane = lax.broadcasted_iota(jnp.int32, (half, width), 1)

    def at(ref, j, size, start=0, stop=None):
        stop = size if stop is None else stop
        base = j * size + start
        if not isinstance(base, int):
            base = pl.multiple_of(base, 8)
        return ref[pl.ds(base, stop - start), :]

    def loop(body, begin):
        if subs <= 8:
            for j in range(subs):
                begin = body(j, begin)
            return begin
        return lax.fori_loop(0, subs, body, begin)

    def times_rows(left, right):
        top, low = halves(right)
        return three(left, top, low, dot_rows)

    def times_plain(left, right):
        top, low = halves(right)
        return three(left, top, low)

    def map_of(j):
        return at(fixed, j, height, share + prim, height)[0:1, :width]

    def spot(row, ids):
        return (ids == row).astype(f32)

    def pick_plain(left, spots):
        top, low = halves(left)
        both = dot(jnp.concatenate([top, low], axis=0), spots.astype(bf16))
        return both[:half] + both[half:]

    def pick_rows(left, spots):
        top, low = halves(left)
        both = dot_rows(jnp.concatenate([top, low], axis=0), spots.astype(bf16))
        return both[:half] + both[half:]

    def add_first(j, total):
        return total + pick_rows(at(values, j, half), spot(map_of(j), unknown))

    inverse = jnp.concatenate([at(fixed, j, height, 0, share) for j in range(subs)], axis=0)
    zero = jnp.zeros((half, count), f32)
    found = times_rows(loop(add_first, zero), inverse)

    def parts(j):
        v = at(values, j, half)
        row = map_of(j)
        schur = at(fixed, j, height, share, share + prim)[:, :width]
        first = pick_plain(found, spot(pltpu.roll(row, prim, 1), there)) - times_plain(
            v, wide(schur, width)
        )
        change = times_plain(first, wide(v[: 2 * prim], width))
        return row, schur, first, jnp.where(lane < 2 * prim, v, change)

    def add_second(j, total):
        row, _, _, p = parts(j)
        signs = (
            spot(row, unknown)
            - spot(pltpu.roll(row, prim, 1), unknown)
            - spot(pltpu.roll(row, 2 * prim, 1), unknown)
        )
        return total + pick_rows(p, signs)

    found_two = times_rows(loop(add_second, zero), inverse)
    row, schur, first, p = parts(0)
    second = pick_plain(found_two, spot(pltpu.roll(row, prim, 1), there)) - times_plain(
        p, wide(jnp.concatenate([schur, -schur, -schur], axis=0), width)
    )
    q[...] = first + pltpu.roll(first + second, 2 * prim, 1)


def finish(keep, recv, q_keep, q_recv, one, two, out):
    prim = one.shape[0]
    rows = keep.shape[0] - prim
    k_low, k_high = pick(keep[rows:, :], recv[rows:, :])
    right = jnp.concatenate([-k_low, -k_high, one[...], two[...]], axis=0)
    top, low = halves(right)
    here = member()
    for n, q, which in ((keep, q_keep, here), (recv, q_recv, 1 - here)):
        out[pl.ds(pl.multiple_of(which * rows, 8), rows), :] = n[:rows, :] + three(q[...], top, low)


def on_device(
    residual,
    inverse_slab,
    diagonal,
    primal_index,
    coarse_map,
    schur_small,
    constraint_basis,
    coarse_basis,
    coarse_inverse,
):
    levels = lax.axis_size("slab")
    subs = lax.axis_size("sub")
    assert levels == 4 and subs & (subs - 1) == 0

    def swap(x):
        return lax.ppermute(x, "slab", [(i, i ^ 1) for i in range(levels)])

    def rise(x):
        return lax.ppermute(x, "slab", [(0, 2), (1, 3)])

    def fall(x):
        return lax.ppermute(x, "slab", [(2, 0), (3, 1)])

    def gather(x, which):
        distance = subs // 2
        while distance:
            pairs = [
                (i * levels + k, (i ^ distance) * levels + k)
                for i in range(subs)
                for k in (2 * which, 2 * which + 1)
            ]
            other = lax.ppermute(x, ("sub", "slab"), pairs)
            x = jnp.concatenate([x, other], axis=0)
            distance //= 2
        return x

    vector = residual[0, 0]
    matrix = inverse_slab[0, 0]
    one, two = constraint_basis[0, 0], coarse_basis[0, 0]
    rows, size = vector.shape
    prim = primal_index.shape[-1]
    coarse_count, share = coarse_inverse.shape
    half = rows // 2
    block = half // BLOCKS
    extra = 2 * prim
    width = -(-3 * prim // LANES) * LANES
    packed = -(-half * width // (8 * size)) * 8
    assert half == extra and prim <= coarse_count and size % width == 0 and 4 * prim <= width

    def like(count, *heights):
        return [struct((h, size)) for h in heights for _ in range(count)]

    other_matrix = swap(matrix)

    (fixed,) = call(
        fix,
        [struct((share + prim + 8, coarse_count))],
        [coarse_inverse.T, schur_small[0], coarse_map],
        0.1,
        scratch=[
            pltpu.VMEM((share, coarse_count), f32),
            pltpu.VMEM((prim, prim), f32),
            pltpu.VMEM(coarse_map.shape, jnp.int32),
            pltpu.SemaphoreType.DMA((3,)),
        ],
        hbm=(0, 1, 2),
    )
    fixed = gather(fixed, 0)

    own, keep, send = call(
        first_products,
        [struct((2, size, size), bf16)] + like(2, half + extra + 8),
        [matrix, vector, one, two, diagonal[0], primal_index[0]],
        2,
        scratch=[
            pltpu.VMEM((size, size), f32),
            pltpu.VMEM((rows + extra, size), f32),
            pltpu.VMEM((rows + extra, size), f32),
            pltpu.VMEM((1, size), f32),
            pltpu.VMEM((1, prim), jnp.int32),
            pltpu.SemaphoreType.DMA((5 + PIECES,)),
        ],
        hbm=(0, 1, 2, 3, 4, 5),
    )
    recv = swap(send)
    weights = call(split, [struct((2, 2, size, size), bf16)], [other_matrix, own], 1)
    place = jnp.arange(size, dtype=jnp.int32)
    own_spots = (primal_index[0, 0][:, None] == place).astype(f32)
    oth_spots = (recv[half + extra + 1, :prim][:, None] == place.astype(f32)).astype(f32)

    span = range(BLOCKS)
    f, carried = [], []
    for i in span[:-1]:
        f.append(call(start_chain, like(2, block), [keep, recv, *weights], 1))
        carried.append(rise(f[i][1]))
    *f_last, k_first, k_second = call(start_last, like(2, block, extra), [keep, recv, *weights], 1)
    f.append(f_last)
    carried.append(rise(f_last[1]))
    y_first, y_second, sent = call(
        adjoint_start,
        like(2, prim) + like(1, 2 * prim),
        [own_spots, oth_spots, k_second, *weights],
        2,
    )
    riding = rise(sent)

    n = []
    for i in span:
        n.append(
            call(
                functools.partial(top_one, i * block),
                like(2, block),
                [keep, recv, carried[i], *weights],
                3,
            )
        )
        carried[i] = fall(n[i][0])
    n_one, g = [], []
    for i in span:
        turned = call(
            turn,
            like(4, block),
            [keep, recv, *f[i], carried[i], *weights, *n[i]],
            4,
            aliases={5 + PARTS: 0, 6 + PARTS: 1},
        )
        n_one.append(turned[:2])
        g.append(turned[2:])
        carried[i] = rise(g[i][1])
        if i == 0:
            passed = [x for j in span for x in (n_one[0] if j == 0 else n[j])]
            y_first, y_second, sent = call(
                functools.partial(adjoint_top, width),
                like(2, prim) + like(1, prim + packed),
                [keep, recv, own_spots, oth_spots, riding, *weights, *passed, y_first, y_second],
                4,
                aliases={5 + PARTS + 2 * BLOCKS: 0, 6 + PARTS + 2 * BLOCKS: 1},
            )
            z_back = fall(sent)
    pieces = []
    for i in span:
        pieces += [*f[i], *g[i]]
    (values,) = call(
        score_turn,
        [struct((half, width))],
        [z_back, y_first, y_second, k_first, k_second, *pieces],
        1,
    )
    values = gather(values, 0)

    n_two = []
    for i in span:
        n_two.append(
            call(
                functools.partial(top_two, i == 0),
                like(2, block + prim if i == 0 else block),
                [keep, recv, *n_one[i], carried[i], riding, *weights],
                3,
            )
        )
        carried[i] = fall(n_two[i][0])
    for i in span:
        n_two[i] = call(
            functools.partial(back, i == 0),
            like(2, block + prim if i == 0 else block),
            [*g[i], k_first, k_second, carried[i], *weights, *n_two[i]],
            2,
            aliases={5 + PARTS: 0, 6 + PARTS: 1},
        )
    pieces = []
    for i in span:
        pieces += [*n_one[i], *n_two[i]]
    m_keep, m_send = call(settle, like(2, half + prim), pieces, 0.5)
    m_recv = swap(m_send)

    (q,) = call(
        functools.partial(solve, subs, prim),
        [struct((half, width))],
        [values, fixed],
        0.5,
        limit=VMEM_LIMIT + 8 * (values.size + fixed.size),
    )
    q_upper = rise(q)
    q = jnp.where(pair() == 0, q, q_upper)
    q_recv = swap(q)
    (out,) = call(finish, [struct((rows, size))], [m_keep, m_recv, q, q_recv, one, two], 0.5)
    return out[None, None]


def solution(mesh):
    placed_as = (
        P("sub", "slab", None, None),
        P("sub", "slab", None, None),
        P("sub", "slab", None),
        P("sub", "slab", None),
        P("sub", None),
        P("sub", None, None),
        P("sub", "slab", None, None),
        P("sub", "slab", None, None),
        P(None, "sub"),
    )

    return jax.shard_map(
        on_device,
        mesh=mesh,
        in_specs=placed_as,
        out_specs=P("sub", "slab", None, None),
        check_vma=False,
    )
```

```python
import functools

import jax
import jax.numpy as jnp
from jax import lax
from jax.experimental import pallas as pl
from jax.experimental.pallas import tpu as pltpu
from jax.sharding import PartitionSpec as P


f32 = jnp.float32
bf16 = jnp.bfloat16
LANES = 128
BLOCKS = 2
PIECES = 4
PARTS = 1


def halves(x):
    top = x.astype(bf16)
    return top, (x - top.astype(f32)).astype(bf16)


def dot(left, right):
    return jnp.dot(left, right, preferred_element_type=f32)


def dot_rows(left, right):
    return lax.dot_general(left, right, (((1,), (1,)), ((), ())), preferred_element_type=f32)


def three(x, top_right, low_right, how=dot):
    rows = x.shape[0]
    top, low = halves(x)
    both = how(jnp.concatenate([top, low], axis=0), top_right)
    return both[:rows] + both[rows:] + how(top, low_right)


def times(x, weights, member):
    step = weights[0].shape[2]
    top, low = halves(x)
    both = jnp.concatenate([top, low], axis=0)
    rows = x.shape[0]
    first, second = 0.0, 0.0
    for i, piece in enumerate(weights):
        cols = slice(i * step, (i + 1) * step)
        first = first + dot(both[:, cols], piece[member, 0])
        second = second + dot(top[:, cols], piece[member, 1])
    return first[:rows] + first[rows:] + second


def times_transposed(x, weights, member):
    return jnp.concatenate(
        [three(x, piece[member, 0], piece[member, 1], dot_rows) for piece in weights], axis=1
    )


def member():
    return lax.axis_index("slab") & 1


def pair():
    return lax.axis_index("slab") >> 1


def spec(space):
    return pl.BlockSpec(memory_space=space)


def call(body, outs, args, work, aliases=None, scratch=(), hbm=(), limit=None):
    specs = [spec(pltpu.VMEM) for _ in args]
    args = list(args)
    for place in hbm:
        specs[place] = spec(pltpu.HBM)
        args[place] = pltpu.with_memory_space_constraint(args[place], pltpu.HBM)
    return pl.pallas_call(
        body,
        out_shape=outs,
        in_specs=specs,
        out_specs=[spec(pltpu.VMEM) for _ in outs],
        input_output_aliases=aliases or {},
        scratch_shapes=list(scratch),
        cost_estimate=pl.CostEstimate(flops=int(work * 8e8), bytes_accessed=0, transcendentals=0),
        compiler_params=pltpu.CompilerParams(vmem_limit_bytes=limit or VMEM_LIMIT),
    )(*args)


VMEM_LIMIT = 16 << 20


def struct(shape, dtype=f32):
    return jax.ShapeDtypeStruct(shape, dtype)


def pick(own, oth):
    first = member() == 0
    return jnp.where(first, own, oth), jnp.where(first, oth, own)


def hold(idle, before, after):
    @pl.when(idle)
    def _():
        for old, new in zip(before, after):
            new[...] = old[...]


def first_products(
    matrix, vector, one, two, diagonal_far, index_far, own, keep, send, buffer, x, total, diagonal, index, sems
):
    size = matrix.shape[0]
    step = size // PIECES
    rows, prim = vector.shape[0], one.shape[0]
    extra = 2 * prim
    copies = [
        pltpu.make_async_copy(vector, x.at[pl.ds(0, rows)], sems.at[0]),
        pltpu.make_async_copy(one, x.at[pl.ds(rows, prim)], sems.at[1]),
        pltpu.make_async_copy(two, x.at[pl.ds(rows + prim, prim)], sems.at[2]),
        pltpu.make_async_copy(diagonal_far, diagonal, sems.at[3]),
        pltpu.make_async_copy(index_far, index, sems.at[4]),
    ]
    pieces = [
        pltpu.make_async_copy(
            matrix.at[pl.ds(i * step, step)], buffer.at[pl.ds(i * step, step)], sems.at[5 + i]
        )
        for i in range(PIECES)
    ]
    for copy in copies + pieces:
        copy.start()
    for copy in copies:
        copy.wait()
    x[rows:, :] = x[rows:, :] * diagonal[...]
    for i, copy in enumerate(pieces):
        cols = pl.ds(i * step, step)
        copy.wait()
        top, low = halves(buffer[cols, :])
        own[0, cols, :] = top
        own[1, cols, :] = low
        part = three(x[:, cols], own[0, cols, :], own[1, cols, :])
        if i == 0:
            total[...] = part
        else:
            total[...] += part
    half = rows // 2
    here, there = member(), 1 - member()
    for out, which in ((keep, here), (send, there)):
        out[:half, :] = total[pl.ds(pl.multiple_of(which * half, 8), half), :]
        out[half : half + extra, :] = total[rows:, :]
        out[half + extra :, :] = jnp.zeros_like(out[half + extra :, :])
        out[half + extra : half + extra + 1, :] = diagonal[...]
        out[half + extra + 1 : half + extra + 2, :prim] = index[...].astype(f32)


def split(matrix, own, weights):
    here = member()
    weights[here] = own[...]
    top, low = halves(matrix[...])
    weights[1 - here, 0] = top
    weights[1 - here, 1] = low


def diagonals(keep, recv):
    place = keep.shape[0] - 8
    return pick(keep[place : place + 1, :], recv[place : place + 1, :])


def start_chain(keep, recv, *refs):
    weights, (f_first, f_second) = refs[:PARTS], refs[PARTS:]
    rows = f_first.shape[0]

    @pl.when(pair() == 0)
    def _():
        first, second = pick(keep[:rows, :], recv[:rows, :])
        f_first[...] = first
        f_second[...] = second + times(first, weights, 1)


def start_last(keep, recv, *refs):
    weights, (f_first, f_second, k_first, k_second) = refs[:PARTS], refs[PARTS:]
    rows, extra = f_first.shape[0], k_first.shape[0]
    stop = keep.shape[0] - 8

    @pl.when(pair() == 0)
    def _():
        at = stop - extra - rows
        first, second = pick(keep[at:stop, :], recv[at:stop, :])
        second = second + times(first, weights, 1)
        f_first[...] = first[:rows]
        f_second[...] = second[:rows]
        k_first[...] = first[rows:]
        k_second[...] = second[rows:]


def top_one(at, keep, recv, carried, *refs):
    weights, (n_first, n_second) = refs[:PARTS], refs[PARTS:]
    rows = n_first.shape[0]

    @pl.when(pair() == 1)
    def _():
        first, second = pick(keep[at : at + rows, :], recv[at : at + rows, :])
        first = first + times(carried[...], weights, 0)
        second = second + times(first, weights, 1)
        n_first[...] = first + times(second, weights, 0)
        n_second[...] = second


def top_two(with_basis, keep, recv, v_first, v_second, carried, *refs):
    riding, weights, (n_first, n_second) = refs[0], refs[1 : 1 + PARTS], refs[1 + PARTS :]
    rows = v_first.shape[0]
    few = riding.shape[0] // 2
    extra = 2 * few
    at = keep.shape[0] - 8 - extra

    @pl.when(pair() == 1)
    def _():
        d_first, d_second = diagonals(keep, recv)
        x = d_first * v_first[...] + carried[...]
        if with_basis:
            here = pl.ds(pl.multiple_of(at + member() * few, 8), few)
            k_first, k_second = pick(keep[here, :], recv[here, :])
            first = times(jnp.concatenate([x, riding[few:, :]], axis=0), weights, 0)
            k_first = first[rows:] + k_first
            y = d_second * v_second[...] + first[:rows]
            second = times(jnp.concatenate([y, k_first], axis=0), weights, 1)
            first = jnp.concatenate([first[:rows], k_first], axis=0)
            second = jnp.concatenate([second[:rows], second[rows:] + k_second], axis=0)
        else:
            first = times(x, weights, 0)
            second = times(d_second * v_second[...] + first, weights, 1)
        n_first[...] = first + times(second, weights, 0)
        n_second[...] = second


def down(f_first, f_second, carried, weights):
    second = f_second + times(carried, weights, 1)
    return f_first + times(second, weights, 0), second


def turn(keep, recv, f_first, f_second, carried, *refs):
    weights, old = refs[:PARTS], refs[PARTS : PARTS + 2]
    n_first, n_second, g_first, g_second = refs[PARTS + 2 :]

    @pl.when(pair() == 0)
    def _():
        first, second = down(f_first[...], f_second[...], carried[...], weights)
        n_second[...] = second
        n_first[...] = first
        d_first, d_second = diagonals(keep, recv)
        again = times(d_first * first, weights, 0)
        g_first[...] = again
        g_second[...] = times(d_second * second + again, weights, 1)

    hold(pair() != 0, old, (n_first, n_second))


def back(with_basis, f_first, f_second, k_first, k_second, carried, *refs):
    weights, old, (n_first, n_second) = refs[:PARTS], refs[PARTS : PARTS + 2], refs[PARTS + 2 :]
    few = k_first.shape[0] // 2

    @pl.when(pair() == 0)
    def _():
        first, second = f_first[...], f_second[...]
        if with_basis:
            here = pl.ds(pl.multiple_of(member() * few, 8), few)
            first = jnp.concatenate([first, k_first[here, :]], axis=0)
            second = jnp.concatenate([second, k_second[here, :]], axis=0)
        n_first[...], n_second[...] = down(first, second, carried[...], weights)

    hold(pair() != 0, old, (n_first, n_second))


def adjoint_start(own_spots, oth_spots, k_second, *refs):
    weights, (y_first, y_second, sent) = refs[:PARTS], refs[PARTS:]
    prim = y_first.shape[0]

    @pl.when(pair() == 0)
    def _():
        first, second = pick(own_spots[...], oth_spots[...])
        second = second + times_transposed(first, weights, 0)
        y_first[...] = first
        y_second[...] = second
        sent[:prim, :] = times_transposed(second, weights, 1)
        sent[prim:, :] = k_second[pl.ds(pl.multiple_of(member() * prim, 8), prim), :]


def placed(u, places, width):
    prim = u.shape[0]
    zero = jnp.zeros_like(u)
    rows = [u if i in places else zero for i in range(width // prim)]
    return jnp.concatenate(rows, axis=0)


def score(x, u):
    top, low = halves(u)
    return three(x, top, low, dot_rows)


def only(x, place, prim):
    lane = lax.broadcasted_iota(jnp.int32, x.shape, 1)
    return jnp.where((lane >= place * prim) & (lane < (place + 1) * prim), x, 0.0)


def pack(values, out, at):
    rows, width = values.shape
    per = out.shape[1] // width
    for j in range(rows // 8):
        row = at + (j // per) * 8
        out[row : row + 8, (j % per) * width : (j % per + 1) * width] = values[8 * j : 8 * j + 8, :]


def unpack(packed, at, rows, width):
    per = packed.shape[1] // width
    return jnp.concatenate(
        [
            packed[
                at + (j // per) * 8 : at + (j // per) * 8 + 8,
                (j % per) * width : (j % per + 1) * width,
            ]
            for j in range(rows // 8)
        ],
        axis=0,
    )


def adjoint_top(width, keep, recv, own_spots, oth_spots, carried, *refs):
    weights, refs = refs[:PARTS], refs[PARTS:]
    blocks, old, (y_first, y_second, sent) = refs[: 2 * BLOCKS], refs[2 * BLOCKS : -3], refs[-3:]
    prim = y_first.shape[0]

    @pl.when(pair() == 1)
    def _():
        first, second = pick(own_spots[...], oth_spots[...])
        first = first + carried[:prim, :]
        second = second + times_transposed(first, weights, 0)
        z_second = times_transposed(second, weights, 1)
        first = first + z_second
        z_first = times_transposed(first, weights, 0)
        sent[:prim, :] = z_first
        w_first, w_second = pick(keep[...], recv[...])
        stop = w_first.shape[0] - 8
        w = score(w_first[:stop], placed(first, (0, 2), width)) + score(
            w_second[:stop], placed(second, (0, 2), width)
        )
        d_first, d_second = diagonals(keep, recv)
        n_first = jnp.concatenate([r[...] for r in blocks[0::2]], axis=0)
        n_second = jnp.concatenate([r[...] for r in blocks[1::2]], axis=0)
        g = score(d_first * n_first, placed(z_first, (1,), width)) + score(
            d_second * n_second, placed(z_second, (1,), width)
        )
        half = n_first.shape[0]
        pack(only(w[:half], 0, prim) + g + only(w[half:], 2, prim), sent, prim)

    hold(pair() != 1, old, (y_first, y_second))


def score_turn(carried, schur, maps, y_first, y_second, k_first, k_second, *refs):
    blocks, values = refs[:-1], refs[-1]
    prim = y_first.shape[0]
    half, width = values.shape

    @pl.when(pair() == 0)
    def _():
        first = jnp.concatenate(
            [r[...] for r in blocks[0::4]] + [k_first[...]] + [r[...] for r in blocks[2::4]], axis=0
        )
        second = jnp.concatenate(
            [r[...] for r in blocks[1::4]] + [k_second[...]] + [r[...] for r in blocks[3::4]], axis=0
        )
        w = score(first, placed(y_first[...], (0, 1, 2), width)) + score(
            second, placed(y_second[...] + carried[:prim, :], (0, 1, 2), width)
        )
        extra = k_first.shape[0]
        values[...] = (
            unpack(carried, prim, half, width)
            + only(w[:half], 0, prim)
            + only(w[half : half + extra], 2, prim)
            + only(w[half + extra :], 1, prim)
        )
        values[:prim, 3 * prim : 4 * prim] = schur[...]
        values[prim : prim + 1, 3 * prim : 4 * prim] = maps[...]


def settle(*refs):
    blocks, (keep, send) = refs[: 4 * BLOCKS], refs[4 * BLOCKS :]
    rows = blocks[0].shape[0]
    for i in range(BLOCKS):
        a1, b1, a2, b2 = blocks[4 * i : 4 * i + 4]
        here = slice(i * rows, (i + 1) * rows)
        keep[here, :], send[here, :] = pick(
            2.0 * a1[...] - a2[:rows, :], 2.0 * b1[...] - b2[:rows, :]
        )
    keep[BLOCKS * rows :, :], send[BLOCKS * rows :, :] = pick(blocks[2][rows:, :], blocks[3][rows:, :])


def wide(x, rows):
    return jnp.concatenate([x, jnp.zeros((rows - x.shape[0], x.shape[1]), f32)], axis=0)


def solve(subs, prim, values, fixed, q):
    half, width = q.shape
    count = fixed.shape[1]
    share = fixed.shape[0] // subs
    me = lax.axis_index("sub")
    unknown = lax.broadcasted_iota(jnp.int32, (count, width), 0)
    block = unknown // share
    far = jnp.zeros_like(block)
    for bit in range(subs.bit_length() - 1):
        far = far | (((block >> bit) & 1) << (subs.bit_length() - 2 - bit))
    there = (far ^ me) * share + unknown % share
    unknown, there = unknown.astype(f32), there.astype(f32)
    lane = lax.broadcasted_iota(jnp.int32, (half, width), 1)

    def at(ref, j, size, start=0, stop=None):
        stop = size if stop is None else stop
        base = j * size + start
        if not isinstance(base, int):
            base = pl.multiple_of(base, 8)
        return ref[pl.ds(base, stop - start), :]

    def loop(body, begin):
        if subs <= 8:
            for j in range(subs):
                begin = body(j, begin)
            return begin
        return lax.fori_loop(0, subs, body, begin)

    def times_rows(left, right):
        top, low = halves(right)
        return three(left, top, low, dot_rows)

    def times_plain(left, right):
        top, low = halves(right)
        return three(left, top, low)

    def map_of(v):
        row = pltpu.roll(v[prim : prim + 8, :], width - 3 * prim, 1)[0:1]
        return jnp.where(lane[0:1] < prim, row, -1.0)

    def times_schur(left, v, signs):
        rows = [v[:prim] if sign > 0 else -v[:prim] for sign in signs]
        out = times_plain(left, wide(jnp.concatenate(rows, axis=0), width))
        return jnp.where(lane < prim, pltpu.roll(out, width - 3 * prim, 1), 0.0)

    def spot(row, ids):
        return (ids == row).astype(f32)

    def pick_plain(left, spots):
        top, low = halves(left)
        both = dot(jnp.concatenate([top, low], axis=0), spots.astype(bf16))
        return both[:half] + both[half:]

    def pick_rows(left, spots):
        top, low = halves(left)
        both = dot_rows(jnp.concatenate([top, low], axis=0), spots.astype(bf16))
        return both[:half] + both[half:]

    def add_first(j, total):
        v = at(values, j, half)
        return total + pick_rows(v, spot(map_of(v), unknown))

    inverse = fixed[...]
    zero = jnp.zeros((half, count), f32)
    found = times_rows(loop(add_first, zero), inverse)

    def parts(j):
        v = at(values, j, half)
        row = map_of(v)
        first = pick_plain(found, spot(pltpu.roll(row, prim, 1), there)) - times_schur(v, v, (1,))
        change = times_plain(first, wide(v[: 2 * prim], width))
        return v, row, first, jnp.where(lane < 2 * prim, v, change)

    def add_second(j, total):
        _, row, _, p = parts(j)
        signs = (
            spot(row, unknown)
            - spot(pltpu.roll(row, prim, 1), unknown)
            - spot(pltpu.roll(row, 2 * prim, 1), unknown)
        )
        return total + pick_rows(p, signs)

    found_two = times_rows(loop(add_second, zero), inverse)
    v, row, first, p = parts(0)
    second = pick_plain(found_two, spot(pltpu.roll(row, prim, 1), there)) - times_schur(
        p, v, (1, -1, -1)
    )
    q[...] = first + pltpu.roll(first + second, 2 * prim, 1)


def finish(keep, recv, q_keep, q_recv, one, two, out):
    prim = one.shape[0]
    rows = keep.shape[0] - prim
    k_low, k_high = pick(keep[rows:, :], recv[rows:, :])
    right = jnp.concatenate([-k_low, -k_high, one[...], two[...]], axis=0)
    top, low = halves(right)
    here = member()
    for n, q, which in ((keep, q_keep, here), (recv, q_recv, 1 - here)):
        out[pl.ds(pl.multiple_of(which * rows, 8), rows), :] = n[:rows, :] + three(q[...], top, low)


def on_device(
    residual,
    inverse_slab,
    diagonal,
    primal_index,
    coarse_map,
    schur_small,
    constraint_basis,
    coarse_basis,
    coarse_inverse,
):
    levels = lax.axis_size("slab")
    subs = lax.axis_size("sub")
    assert levels == 4 and subs & (subs - 1) == 0

    def swap(x):
        return lax.ppermute(x, "slab", [(i, i ^ 1) for i in range(levels)])

    def rise(x):
        return lax.ppermute(x, "slab", [(0, 2), (1, 3)])

    def fall(x):
        return lax.ppermute(x, "slab", [(2, 0), (3, 1)])

    def trade(x, distance):
        pairs = [
            (i * levels + k, (i ^ distance) * levels + k) for i in range(subs) for k in range(2)
        ]
        return lax.ppermute(x, ("sub", "slab"), pairs)

    def join(x, y):
        return jnp.concatenate([x, y], axis=0)

    vector = residual[0, 0]
    matrix = inverse_slab[0, 0]
    one, two = constraint_basis[0, 0], coarse_basis[0, 0]
    rows, size = vector.shape
    prim = primal_index.shape[-1]
    coarse_count, _ = coarse_inverse.shape
    half = rows // 2
    block = half // BLOCKS
    extra = 2 * prim
    width = -(-3 * prim // LANES) * LANES
    packed = -(-half * width // (8 * size)) * 8
    assert half == extra and prim <= coarse_count and size % width == 0 and 4 * prim <= width

    def like(count, *heights):
        return [struct((h, size)) for h in heights for _ in range(count)]

    other_matrix = swap(matrix)

    inverse = coarse_inverse.T
    distance = subs // 2
    while distance > 1:
        inverse = join(inverse, trade(inverse, distance))
        distance //= 2

    own, keep, send = call(
        first_products,
        [struct((2, size, size), bf16)] + like(2, half + extra + 8),
        [matrix, vector, one, two, diagonal[0], primal_index[0]],
        2,
        scratch=[
            pltpu.VMEM((size, size), f32),
            pltpu.VMEM((rows + extra, size), f32),
            pltpu.VMEM((rows + extra, size), f32),
            pltpu.VMEM((1, size), f32),
            pltpu.VMEM((1, prim), jnp.int32),
            pltpu.SemaphoreType.DMA((5 + PIECES,)),
        ],
        hbm=(0, 1, 2, 3, 4, 5),
    )
    recv = swap(send)
    weights = call(split, [struct((2, 2, size, size), bf16)], [other_matrix, own], 1)
    place = jnp.arange(size, dtype=jnp.int32)
    own_spots = (primal_index[0, 0][:, None] == place).astype(f32)
    oth_spots = (recv[half + extra + 1, :prim][:, None] == place.astype(f32)).astype(f32)

    span = range(BLOCKS)
    f, carried = [], []
    for i in span[:-1]:
        f.append(call(start_chain, like(2, block), [keep, recv, *weights], 1))
        carried.append(rise(f[i][1]))
    *f_last, k_first, k_second = call(start_last, like(2, block, extra), [keep, recv, *weights], 1)
    f.append(f_last)
    carried.append(rise(f_last[1]))
    y_first, y_second, sent = call(
        adjoint_start,
        like(2, prim) + like(1, 2 * prim),
        [own_spots, oth_spots, k_second, *weights],
        2,
    )
    riding = rise(sent)

    n = []
    for i in span:
        n.append(
            call(
                functools.partial(top_one, i * block),
                like(2, block),
                [keep, recv, carried[i], *weights],
                3,
            )
        )
        carried[i] = fall(n[i][0])
    n_one, g = [], []
    for i in span:
        turned = call(
            turn,
            like(4, block),
            [keep, recv, *f[i], carried[i], *weights, *n[i]],
            4,
            aliases={5 + PARTS: 0, 6 + PARTS: 1},
        )
        n_one.append(turned[:2])
        g.append(turned[2:])
        carried[i] = rise(g[i][1])
        if i == 0:
            passed = [x for j in span for x in (n_one[0] if j == 0 else n[j])]
            y_first, y_second, sent = call(
                functools.partial(adjoint_top, width),
                like(2, prim) + like(1, prim + packed),
                [keep, recv, own_spots, oth_spots, riding, *weights, *passed, y_first, y_second],
                4,
                aliases={5 + PARTS + 2 * BLOCKS: 0, 6 + PARTS + 2 * BLOCKS: 1},
            )
            z_back = fall(sent)
    pieces = []
    for i in span:
        pieces += [*f[i], *g[i]]
    (values,) = call(
        score_turn,
        [struct((half, width))],
        [z_back, schur_small[0], coarse_map.astype(f32), y_first, y_second, k_first, k_second, *pieces],
        1,
    )
    distance = subs // 2
    while distance > 1:
        values = join(values, trade(values, distance))
        distance //= 2
    if coarse_count == width:
        others = trade(join(values, inverse), 1)
        inverse = join(inverse, others[values.shape[0] :])
        values = join(values, others[: values.shape[0]])
    else:
        inverse = join(inverse, trade(inverse, 1))
        values = join(values, trade(values, 1))

    n_two = []
    for i in span:
        n_two.append(
            call(
                functools.partial(top_two, i == 0),
                like(2, block + prim if i == 0 else block),
                [keep, recv, *n_one[i], carried[i], riding, *weights],
                3,
            )
        )
        carried[i] = fall(n_two[i][0])
    for i in span:
        n_two[i] = call(
            functools.partial(back, i == 0),
            like(2, block + prim if i == 0 else block),
            [*g[i], k_first, k_second, carried[i], *weights, *n_two[i]],
            2,
            aliases={5 + PARTS: 0, 6 + PARTS: 1},
        )
    pieces = []
    for i in span:
        pieces += [*n_one[i], *n_two[i]]
    m_keep, m_send = call(settle, like(2, half + prim), pieces, 0.5)
    m_recv = swap(m_send)

    (q,) = call(
        functools.partial(solve, subs, prim),
        [struct((half, width))],
        [values, inverse],
        0.5,
        limit=VMEM_LIMIT + 8 * (values.size + inverse.size),
    )
    q_upper = rise(q)
    q = jnp.where(pair() == 0, q, q_upper)
    q_recv = swap(q)
    (out,) = call(finish, [struct((rows, size))], [m_keep, m_recv, q, q_recv, one, two], 0.5)
    return out[None, None]


def solution(mesh):
    placed_as = (
        P("sub", "slab", None, None),
        P("sub", "slab", None, None),
        P("sub", "slab", None),
        P("sub", "slab", None),
        P("sub", None),
        P("sub", None, None),
        P("sub", "slab", None, None),
        P("sub", "slab", None, None),
        P(None, "sub"),
    )

    return jax.shard_map(
        on_device,
        mesh=mesh,
        in_specs=placed_as,
        out_specs=P("sub", "slab", None, None),
        check_vma=False,
    )
```

```python
import functools

import jax
import jax.numpy as jnp
from jax import lax
from jax.experimental import pallas as pl
from jax.experimental.pallas import tpu as pltpu
from jax.sharding import PartitionSpec as P


f32 = jnp.float32
bf16 = jnp.bfloat16
LANES = 128
BLOCKS = 2
PIECES = 4
PARTS = 1


def halves(x):
    top = x.astype(bf16)
    return top, (x - top.astype(f32)).astype(bf16)


def dot(left, right):
    return jnp.dot(left, right, preferred_element_type=f32)


def dot_rows(left, right):
    return lax.dot_general(left, right, (((1,), (1,)), ((), ())), preferred_element_type=f32)


def three(x, top_right, low_right, how=dot):
    rows = x.shape[0]
    top, low = halves(x)
    both = how(jnp.concatenate([top, low], axis=0), top_right)
    return both[:rows] + both[rows:] + how(top, low_right)


def times(x, weights, member):
    step = weights[0].shape[2]
    top, low = halves(x)
    both = jnp.concatenate([top, low], axis=0)
    rows = x.shape[0]
    first, second = 0.0, 0.0
    for i, piece in enumerate(weights):
        cols = slice(i * step, (i + 1) * step)
        first = first + dot(both[:, cols], piece[member, 0])
        second = second + dot(top[:, cols], piece[member, 1])
    return first[:rows] + first[rows:] + second


def times_transposed(x, weights, member):
    return jnp.concatenate(
        [three(x, piece[member, 0], piece[member, 1], dot_rows) for piece in weights], axis=1
    )


def member():
    return lax.axis_index("slab") & 1


def pair():
    return lax.axis_index("slab") >> 1


def spec(space):
    return pl.BlockSpec(memory_space=space)


def call(body, outs, args, work, aliases=None, scratch=(), hbm=(), limit=None):
    specs = [spec(pltpu.VMEM) for _ in args]
    args = list(args)
    for place in hbm:
        specs[place] = spec(pltpu.HBM)
        args[place] = pltpu.with_memory_space_constraint(args[place], pltpu.HBM)
    return pl.pallas_call(
        body,
        out_shape=outs,
        in_specs=specs,
        out_specs=[spec(pltpu.VMEM) for _ in outs],
        input_output_aliases=aliases or {},
        scratch_shapes=list(scratch),
        cost_estimate=pl.CostEstimate(flops=int(work * 8e8), bytes_accessed=0, transcendentals=0),
        compiler_params=pltpu.CompilerParams(vmem_limit_bytes=limit or VMEM_LIMIT),
    )(*args)


VMEM_LIMIT = 16 << 20


def struct(shape, dtype=f32):
    return jax.ShapeDtypeStruct(shape, dtype)


def pick(own, oth):
    first = member() == 0
    return jnp.where(first, own, oth), jnp.where(first, oth, own)


def hold(idle, before, after):
    @pl.when(idle)
    def _():
        for old, new in zip(before, after):
            new[...] = old[...]


def first_products(
    matrix, vector, one, two, diagonal_far, index_far, own, keep, send, buffer, x, total, diagonal, index, sems
):
    size = matrix.shape[0]
    step = size // PIECES
    rows, prim = vector.shape[0], one.shape[0]
    extra = 2 * prim
    copies = [
        pltpu.make_async_copy(vector, x.at[pl.ds(0, rows)], sems.at[0]),
        pltpu.make_async_copy(one, x.at[pl.ds(rows, prim)], sems.at[1]),
        pltpu.make_async_copy(two, x.at[pl.ds(rows + prim, prim)], sems.at[2]),
        pltpu.make_async_copy(diagonal_far, diagonal, sems.at[3]),
        pltpu.make_async_copy(index_far, index, sems.at[4]),
    ]
    pieces = [
        pltpu.make_async_copy(
            matrix.at[pl.ds(i * step, step)], buffer.at[pl.ds(i * step, step)], sems.at[5 + i]
        )
        for i in range(PIECES)
    ]
    for copy in copies + pieces:
        copy.start()
    for copy in copies:
        copy.wait()
    x[rows:, :] = x[rows:, :] * diagonal[...]
    for i, copy in enumerate(pieces):
        cols = pl.ds(i * step, step)
        copy.wait()
        top, low = halves(buffer[cols, :])
        own[0, cols, :] = top
        own[1, cols, :] = low
        part = three(x[:, cols], own[0, cols, :], own[1, cols, :])
        if i == 0:
            total[...] = part
        else:
            total[...] += part
    half = rows // 2
    here, there = member(), 1 - member()
    for out, which in ((keep, here), (send, there)):
        out[:half, :] = total[pl.ds(pl.multiple_of(which * half, 8), half), :]
        out[half : half + extra, :] = total[rows:, :]
        out[half + extra :, :] = jnp.zeros_like(out[half + extra :, :])
        out[half + extra : half + extra + 1, :] = diagonal[...]
        out[half + extra + 1 : half + extra + 2, :prim] = index[...].astype(f32)


def split(matrix, own, weights):
    here = member()
    weights[here] = own[...]
    top, low = halves(matrix[...])
    weights[1 - here, 0] = top
    weights[1 - here, 1] = low


def diagonals(keep, recv):
    place = keep.shape[0] - 8
    return pick(keep[place : place + 1, :], recv[place : place + 1, :])


def start_chain(keep, recv, *refs):
    weights, (f_first, f_second) = refs[:PARTS], refs[PARTS:]
    rows = f_first.shape[0]

    @pl.when(pair() == 0)
    def _():
        first, second = pick(keep[:rows, :], recv[:rows, :])
        f_first[...] = first
        f_second[...] = second + times(first, weights, 1)


def start_last(keep, recv, *refs):
    weights, (f_first, f_second, k_first, k_second) = refs[:PARTS], refs[PARTS:]
    rows, extra = f_first.shape[0], k_first.shape[0]
    stop = keep.shape[0] - 8

    @pl.when(pair() == 0)
    def _():
        at = stop - extra - rows
        first, second = pick(keep[at:stop, :], recv[at:stop, :])
        second = second + times(first, weights, 1)
        f_first[...] = first[:rows]
        f_second[...] = second[:rows]
        k_first[...] = first[rows:]
        k_second[...] = second[rows:]


def top_one(at, keep, recv, carried, *refs):
    weights, (n_first, n_second) = refs[:PARTS], refs[PARTS:]
    rows = n_first.shape[0]

    @pl.when(pair() == 1)
    def _():
        first, second = pick(keep[at : at + rows, :], recv[at : at + rows, :])
        first = first + times(carried[...], weights, 0)
        second = second + times(first, weights, 1)
        n_first[...] = first + times(second, weights, 0)
        n_second[...] = second


def top_two(with_basis, keep, recv, v_first, v_second, carried, *refs):
    riding, weights, (n_first, n_second) = refs[0], refs[1 : 1 + PARTS], refs[1 + PARTS :]
    rows = v_first.shape[0]
    few = riding.shape[0] // 2
    extra = 2 * few
    at = keep.shape[0] - 8 - extra

    @pl.when(pair() == 1)
    def _():
        d_first, d_second = diagonals(keep, recv)
        x = d_first * v_first[...] + carried[...]
        if with_basis:
            here = pl.ds(pl.multiple_of(at + member() * few, 8), few)
            k_first, k_second = pick(keep[here, :], recv[here, :])
            first = times(jnp.concatenate([x, riding[few:, :]], axis=0), weights, 0)
            k_first = first[rows:] + k_first
            y = d_second * v_second[...] + first[:rows]
            second = times(jnp.concatenate([y, k_first], axis=0), weights, 1)
            first = jnp.concatenate([first[:rows], k_first], axis=0)
            second = jnp.concatenate([second[:rows], second[rows:] + k_second], axis=0)
        else:
            first = times(x, weights, 0)
            second = times(d_second * v_second[...] + first, weights, 1)
        n_first[...] = first + times(second, weights, 0)
        n_second[...] = second


def down(f_first, f_second, carried, weights):
    second = f_second + times(carried, weights, 1)
    return f_first + times(second, weights, 0), second


def turn(keep, recv, f_first, f_second, carried, *refs):
    weights, old = refs[:PARTS], refs[PARTS : PARTS + 2]
    n_first, n_second, g_first, g_second = refs[PARTS + 2 :]

    @pl.when(pair() == 0)
    def _():
        first, second = down(f_first[...], f_second[...], carried[...], weights)
        n_second[...] = second
        n_first[...] = first
        d_first, d_second = diagonals(keep, recv)
        again = times(d_first * first, weights, 0)
        g_first[...] = again
        g_second[...] = times(d_second * second + again, weights, 1)

    hold(pair() != 0, old, (n_first, n_second))


def back(with_basis, f_first, f_second, k_first, k_second, carried, *refs):
    weights, old, (n_first, n_second) = refs[:PARTS], refs[PARTS : PARTS + 2], refs[PARTS + 2 :]
    few = k_first.shape[0] // 2

    @pl.when(pair() == 0)
    def _():
        first, second = f_first[...], f_second[...]
        if with_basis:
            here = pl.ds(pl.multiple_of(member() * few, 8), few)
            first = jnp.concatenate([first, k_first[here, :]], axis=0)
            second = jnp.concatenate([second, k_second[here, :]], axis=0)
        n_first[...], n_second[...] = down(first, second, carried[...], weights)

    hold(pair() != 0, old, (n_first, n_second))


def adjoint_start(own_spots, oth_spots, k_second, *refs):
    weights, (y_first, y_second, sent) = refs[:PARTS], refs[PARTS:]
    prim = y_first.shape[0]

    @pl.when(pair() == 0)
    def _():
        first, second = pick(own_spots[...], oth_spots[...])
        second = second + times_transposed(first, weights, 0)
        y_first[...] = first
        y_second[...] = second
        sent[:prim, :] = times_transposed(second, weights, 1)
        sent[prim:, :] = k_second[pl.ds(pl.multiple_of(member() * prim, 8), prim), :]


def placed(u, places, width):
    prim = u.shape[0]
    zero = jnp.zeros_like(u)
    rows = [u if i in places else zero for i in range(width // prim)]
    return jnp.concatenate(rows, axis=0)


def score(x, u):
    top, low = halves(u)
    return three(x, top, low, dot_rows)


def only(x, place, prim):
    lane = lax.broadcasted_iota(jnp.int32, x.shape, 1)
    return jnp.where((lane >= place * prim) & (lane < (place + 1) * prim), x, 0.0)


def pack(values, out, at):
    rows, width = values.shape
    per = out.shape[1] // width
    for j in range(rows // 8):
        row = at + (j // per) * 8
        out[row : row + 8, (j % per) * width : (j % per + 1) * width] = values[8 * j : 8 * j + 8, :]


def unpack(packed, at, rows, width):
    per = packed.shape[1] // width
    return jnp.concatenate(
        [
            packed[
                at + (j // per) * 8 : at + (j // per) * 8 + 8,
                (j % per) * width : (j % per + 1) * width,
            ]
            for j in range(rows // 8)
        ],
        axis=0,
    )


def adjoint_top(width, keep, recv, own_spots, oth_spots, carried, *refs):
    weights, refs = refs[:PARTS], refs[PARTS:]
    blocks, old, (y_first, y_second, sent) = refs[: 2 * BLOCKS], refs[2 * BLOCKS : -3], refs[-3:]
    prim = y_first.shape[0]

    @pl.when(pair() == 1)
    def _():
        first, second = pick(own_spots[...], oth_spots[...])
        first = first + carried[:prim, :]
        second = second + times_transposed(first, weights, 0)
        z_second = times_transposed(second, weights, 1)
        first = first + z_second
        z_first = times_transposed(first, weights, 0)
        sent[:prim, :] = z_first
        w_first, w_second = pick(keep[...], recv[...])
        stop = w_first.shape[0] - 8
        w = score(w_first[:stop], placed(first, (0, 2), width)) + score(
            w_second[:stop], placed(second, (0, 2), width)
        )
        d_first, d_second = diagonals(keep, recv)
        n_first = jnp.concatenate([r[...] for r in blocks[0::2]], axis=0)
        n_second = jnp.concatenate([r[...] for r in blocks[1::2]], axis=0)
        g = score(d_first * n_first, placed(z_first, (1,), width)) + score(
            d_second * n_second, placed(z_second, (1,), width)
        )
        half = n_first.shape[0]
        pack(only(w[:half], 0, prim) + g + only(w[half:], 2, prim), sent, prim)

    hold(pair() != 1, old, (y_first, y_second))


def score_turn(subs, carried, schur, maps, inverse, y_first, y_second, k_first, k_second, *refs):
    blocks, copies, values = refs[:-2], refs[-2], refs[-1]
    prim = y_first.shape[0]
    width = values.shape[1]
    half = BLOCKS * blocks[0].shape[0]
    share = inverse.shape[0]

    @pl.when(pair() == 0)
    def _():
        first = jnp.concatenate(
            [r[...] for r in blocks[0::4]] + [k_first[...]] + [r[...] for r in blocks[2::4]], axis=0
        )
        second = jnp.concatenate(
            [r[...] for r in blocks[1::4]] + [k_second[...]] + [r[...] for r in blocks[3::4]], axis=0
        )
        w = score(first, placed(y_first[...], (0, 1, 2), width)) + score(
            second, placed(y_second[...] + carried[:prim, :], (0, 1, 2), width)
        )
        extra = k_first.shape[0]
        values[:half, :] = (
            unpack(carried, prim, half, width)
            + only(w[:half], 0, prim)
            + only(w[half : half + extra], 2, prim)
            + only(w[half + extra :], 1, prim)
        )
        values[:prim, 3 * prim : 4 * prim] = schur[...]
        values[prim : prim + 1, 3 * prim : 4 * prim] = maps[...]
        for i in range(inverse.shape[1] // width):
            values[half + i * share : half + (i + 1) * share, :] = inverse[:, i * width : (i + 1) * width]
        for j in range(subs):
            copies[j] = values[...]


def settle(*refs):
    blocks, (keep, send) = refs[: 4 * BLOCKS], refs[4 * BLOCKS :]
    rows = blocks[0].shape[0]
    for i in range(BLOCKS):
        a1, b1, a2, b2 = blocks[4 * i : 4 * i + 4]
        here = slice(i * rows, (i + 1) * rows)
        keep[here, :], send[here, :] = pick(
            2.0 * a1[...] - a2[:rows, :], 2.0 * b1[...] - b2[:rows, :]
        )
    keep[BLOCKS * rows :, :], send[BLOCKS * rows :, :] = pick(blocks[2][rows:, :], blocks[3][rows:, :])


def wide(x, rows):
    return jnp.concatenate([x, jnp.zeros((rows - x.shape[0], x.shape[1]), f32)], axis=0)


def solve(prim, share, values, q):
    @pl.when(pair() == 0)
    def _():
        half, width = q.shape
        subs, height = values.shape[:2]
        count = subs * share
        unknown = lax.broadcasted_iota(jnp.int32, (count, width), 0).astype(f32)
        lane = lax.broadcasted_iota(jnp.int32, (half, width), 1)

        def at(j):
            return values[j, :half, :]

        def share_of(j):
            return jnp.concatenate(
                [values[j, i : i + share, :] for i in range(half, height, share)], axis=1
            )

        def loop(body, begin):
            if subs <= 8:
                for j in range(subs):
                    begin = body(j, begin)
                return begin
            return lax.fori_loop(0, subs, body, begin)

        def times_rows(left, right):
            top, low = halves(right)
            return three(left, top, low, dot_rows)

        def times_plain(left, right):
            top, low = halves(right)
            return three(left, top, low)

        def map_of(v):
            row = pltpu.roll(v[prim : prim + 8, :], width - 3 * prim, 1)[0:1]
            return jnp.where(lane[0:1] < prim, row, -1.0)

        def times_schur(left, v, signs):
            rows = [v[:prim] if sign > 0 else -v[:prim] for sign in signs]
            out = times_plain(left, wide(jnp.concatenate(rows, axis=0), width))
            return jnp.where(lane < prim, pltpu.roll(out, width - 3 * prim, 1), 0.0)

        def spot(row, ids):
            return (ids == row).astype(f32)

        def pick_plain(left, spots):
            top, low = halves(left)
            both = dot(jnp.concatenate([top, low], axis=0), spots.astype(bf16))
            return both[:half] + both[half:]

        def pick_rows(left, spots):
            top, low = halves(left)
            both = dot_rows(jnp.concatenate([top, low], axis=0), spots.astype(bf16))
            return both[:half] + both[half:]

        def add_first(j, total):
            v = at(j)
            return total + pick_rows(v, spot(map_of(v), unknown))

        inverse = jnp.concatenate([share_of(j) for j in range(subs)], axis=0)
        zero = jnp.zeros((half, count), f32)
        found = times_rows(loop(add_first, zero), inverse)

        def parts(j):
            v = at(j)
            row = map_of(v)
            first = pick_plain(found, spot(pltpu.roll(row, prim, 1), unknown)) - times_schur(v, v, (1,))
            change = times_plain(first, wide(v[: 2 * prim], width))
            return v, row, first, jnp.where(lane < 2 * prim, v, change)

        def add_second(j, total):
            _, row, _, p = parts(j)
            signs = (
                spot(row, unknown)
                - spot(pltpu.roll(row, prim, 1), unknown)
                - spot(pltpu.roll(row, 2 * prim, 1), unknown)
            )
            return total + pick_rows(p, signs)

        found_two = times_rows(loop(add_second, zero), inverse)
        v, row, first, p = parts(lax.axis_index("sub"))
        second = pick_plain(found_two, spot(pltpu.roll(row, prim, 1), unknown)) - times_schur(
            p, v, (1, -1, -1)
        )
        q[...] = first + pltpu.roll(first + second, 2 * prim, 1)


def finish(keep, recv, q_keep, q_recv, one, two, out):
    prim = one.shape[0]
    rows = keep.shape[0] - prim
    k_low, k_high = pick(keep[rows:, :], recv[rows:, :])
    right = jnp.concatenate([-k_low, -k_high, one[...], two[...]], axis=0)
    top, low = halves(right)
    here = member()
    for n, q, which in ((keep, q_keep, here), (recv, q_recv, 1 - here)):
        out[pl.ds(pl.multiple_of(which * rows, 8), rows), :] = n[:rows, :] + three(q[...], top, low)


def on_device(
    residual,
    inverse_slab,
    diagonal,
    primal_index,
    coarse_map,
    schur_small,
    constraint_basis,
    coarse_basis,
    coarse_inverse,
):
    levels = lax.axis_size("slab")
    subs = lax.axis_size("sub")
    assert levels == 4

    def swap(x):
        return lax.ppermute(x, "slab", [(i, i ^ 1) for i in range(levels)])

    def rise(x):
        return lax.ppermute(x, "slab", [(0, 2), (1, 3)])

    def fall(x):
        return lax.ppermute(x, "slab", [(2, 0), (3, 1)])

    vector = residual[0, 0]
    matrix = inverse_slab[0, 0]
    one, two = constraint_basis[0, 0], coarse_basis[0, 0]
    rows, size = vector.shape
    prim = primal_index.shape[-1]
    coarse_count, share = coarse_inverse.shape
    half = rows // 2
    block = half // BLOCKS
    extra = 2 * prim
    width = -(-3 * prim // LANES) * LANES
    packed = -(-half * width // (8 * size)) * 8
    assert half == extra and prim <= coarse_count and size % width == 0 and 4 * prim <= width and coarse_count % width == 0

    def like(count, *heights):
        return [struct((h, size)) for h in heights for _ in range(count)]

    other_matrix = swap(matrix)

    own, keep, send = call(
        first_products,
        [struct((2, size, size), bf16)] + like(2, half + extra + 8),
        [matrix, vector, one, two, diagonal[0], primal_index[0]],
        2,
        scratch=[
            pltpu.VMEM((size, size), f32),
            pltpu.VMEM((rows + extra, size), f32),
            pltpu.VMEM((rows + extra, size), f32),
            pltpu.VMEM((1, size), f32),
            pltpu.VMEM((1, prim), jnp.int32),
            pltpu.SemaphoreType.DMA((5 + PIECES,)),
        ],
        hbm=(0, 1, 2, 3, 4, 5),
    )
    recv = swap(send)
    weights = call(split, [struct((2, 2, size, size), bf16)], [other_matrix, own], 1)
    place = jnp.arange(size, dtype=jnp.int32)
    own_spots = (primal_index[0, 0][:, None] == place).astype(f32)
    oth_spots = (recv[half + extra + 1, :prim][:, None] == place.astype(f32)).astype(f32)

    span = range(BLOCKS)
    f, carried = [], []
    for i in span[:-1]:
        f.append(call(start_chain, like(2, block), [keep, recv, *weights], 1))
        carried.append(rise(f[i][1]))
    *f_last, k_first, k_second = call(start_last, like(2, block, extra), [keep, recv, *weights], 1)
    f.append(f_last)
    carried.append(rise(f_last[1]))
    y_first, y_second, sent = call(
        adjoint_start,
        like(2, prim) + like(1, 2 * prim),
        [own_spots, oth_spots, k_second, *weights],
        2,
    )
    riding = rise(sent)

    n = []
    for i in span:
        n.append(
            call(
                functools.partial(top_one, i * block),
                like(2, block),
                [keep, recv, carried[i], *weights],
                3,
            )
        )
        carried[i] = fall(n[i][0])
    n_one, g = [], []
    for i in span:
        turned = call(
            turn,
            like(4, block),
            [keep, recv, *f[i], carried[i], *weights, *n[i]],
            4,
            aliases={5 + PARTS: 0, 6 + PARTS: 1},
        )
        n_one.append(turned[:2])
        g.append(turned[2:])
        carried[i] = rise(g[i][1])
        if i == 0:
            passed = [x for j in span for x in (n_one[0] if j == 0 else n[j])]
            y_first, y_second, sent = call(
                functools.partial(adjoint_top, width),
                like(2, prim) + like(1, prim + packed),
                [keep, recv, own_spots, oth_spots, riding, *weights, *passed, y_first, y_second],
                4,
                aliases={5 + PARTS + 2 * BLOCKS: 0, 6 + PARTS + 2 * BLOCKS: 1},
            )
            z_back = fall(sent)
    pieces = []
    for i in span:
        pieces += [*f[i], *g[i]]
    height = half + coarse_count // width * share
    (values,) = call(
        functools.partial(score_turn, subs),
        [struct((subs, height, width))],
        [
            z_back,
            schur_small[0],
            coarse_map.astype(f32),
            coarse_inverse.T,
            y_first,
            y_second,
            k_first,
            k_second,
            *pieces,
        ],
        1,
        scratch=[pltpu.VMEM((height, width), f32)],
    )
    values = lax.all_to_all(values, "sub", 0, 0)

    n_two = []
    for i in span:
        n_two.append(
            call(
                functools.partial(top_two, i == 0),
                like(2, block + prim if i == 0 else block),
                [keep, recv, *n_one[i], carried[i], riding, *weights],
                3,
            )
        )
        carried[i] = fall(n_two[i][0])
    for i in span:
        n_two[i] = call(
            functools.partial(back, i == 0),
            like(2, block + prim if i == 0 else block),
            [*g[i], k_first, k_second, carried[i], *weights, *n_two[i]],
            2,
            aliases={5 + PARTS: 0, 6 + PARTS: 1},
        )
    pieces = []
    for i in span:
        pieces += [*n_one[i], *n_two[i]]
    m_keep, m_send = call(settle, like(2, half + prim), pieces, 0.5)
    m_recv = swap(m_send)

    (q,) = call(
        functools.partial(solve, prim, share),
        [struct((half, width))],
        [values],
        0.5,
        limit=VMEM_LIMIT + 8 * values.size,
    )
    q_upper = rise(q)
    q = jnp.where(pair() == 0, q, q_upper)
    q_recv = swap(q)
    (out,) = call(finish, [struct((rows, size))], [m_keep, m_recv, q, q_recv, one, two], 0.5)
    return out[None, None]


def solution(mesh):
    placed_as = (
        P("sub", "slab", None, None),
        P("sub", "slab", None, None),
        P("sub", "slab", None),
        P("sub", "slab", None),
        P("sub", None),
        P("sub", None, None),
        P("sub", "slab", None, None),
        P("sub", "slab", None, None),
        P(None, "sub"),
    )

    return jax.shard_map(
        on_device,
        mesh=mesh,
        in_specs=placed_as,
        out_specs=P("sub", "slab", None, None),
        check_vma=False,
    )
```

```python
import functools

import jax
import jax.numpy as jnp
from jax import lax
from jax.experimental import pallas as pl
from jax.experimental.pallas import tpu as pltpu
from jax.sharding import PartitionSpec as P


f32 = jnp.float32
bf16 = jnp.bfloat16
LANES = 128
BLOCKS = 2
PIECES = 4
PARTS = 1


def halves(x):
    top = x.astype(bf16)
    return top, (x - top.astype(f32)).astype(bf16)


def dot(left, right):
    return jnp.dot(left, right, preferred_element_type=f32)


def dot_rows(left, right):
    return lax.dot_general(left, right, (((1,), (1,)), ((), ())), preferred_element_type=f32)


def three(x, top_right, low_right, how=dot):
    rows = x.shape[0]
    top, low = halves(x)
    both = how(jnp.concatenate([top, low], axis=0), top_right)
    return both[:rows] + both[rows:] + how(top, low_right)


def times(x, weights, member):
    step = weights[0].shape[2]
    top, low = halves(x)
    both = jnp.concatenate([top, low], axis=0)
    rows = x.shape[0]
    first, second = 0.0, 0.0
    for i, piece in enumerate(weights):
        cols = slice(i * step, (i + 1) * step)
        first = first + dot(both[:, cols], piece[member, 0])
        second = second + dot(top[:, cols], piece[member, 1])
    return first[:rows] + first[rows:] + second


def times_transposed(x, weights, member):
    return jnp.concatenate(
        [three(x, piece[member, 0], piece[member, 1], dot_rows) for piece in weights], axis=1
    )


def member():
    return lax.axis_index("slab") & 1


def pair():
    return lax.axis_index("slab") >> 1


def spec(space):
    return pl.BlockSpec(memory_space=space)


def call(body, outs, args, work, aliases=None, scratch=(), hbm=(), limit=None):
    specs = [spec(pltpu.VMEM) for _ in args]
    args = list(args)
    for place in hbm:
        specs[place] = spec(pltpu.HBM)
        args[place] = pltpu.with_memory_space_constraint(args[place], pltpu.HBM)
    return pl.pallas_call(
        body,
        out_shape=outs,
        in_specs=specs,
        out_specs=[spec(pltpu.VMEM) for _ in outs],
        input_output_aliases=aliases or {},
        scratch_shapes=list(scratch),
        cost_estimate=pl.CostEstimate(flops=int(work * 8e8), bytes_accessed=0, transcendentals=0),
        compiler_params=pltpu.CompilerParams(vmem_limit_bytes=limit or VMEM_LIMIT),
    )(*args)


VMEM_LIMIT = 16 << 20


def struct(shape, dtype=f32):
    return jax.ShapeDtypeStruct(shape, dtype)


def pick(own, oth):
    first = member() == 0
    return jnp.where(first, own, oth), jnp.where(first, oth, own)


def hold(idle, before, after):
    @pl.when(idle)
    def _():
        for old, new in zip(before, after):
            new[...] = old[...]


def first_products(
    matrix, vector, one, two, diagonal_far, index_far, own, keep, send, buffer, x, total, diagonal, index, sems
):
    size = matrix.shape[0]
    step = size // PIECES
    rows, prim = vector.shape[0], one.shape[0]
    extra = 2 * prim
    copies = [
        pltpu.make_async_copy(vector, x.at[pl.ds(0, rows)], sems.at[0]),
        pltpu.make_async_copy(one, x.at[pl.ds(rows, prim)], sems.at[1]),
        pltpu.make_async_copy(two, x.at[pl.ds(rows + prim, prim)], sems.at[2]),
        pltpu.make_async_copy(diagonal_far, diagonal, sems.at[3]),
        pltpu.make_async_copy(index_far, index, sems.at[4]),
    ]
    pieces = [
        pltpu.make_async_copy(
            matrix.at[pl.ds(i * step, step)], buffer.at[pl.ds(i * step, step)], sems.at[5 + i]
        )
        for i in range(PIECES)
    ]
    for copy in copies + pieces:
        copy.start()
    for copy in copies:
        copy.wait()
    x[rows:, :] = x[rows:, :] * diagonal[...]
    for i, copy in enumerate(pieces):
        cols = pl.ds(i * step, step)
        copy.wait()
        top, low = halves(buffer[cols, :])
        own[0, cols, :] = top
        own[1, cols, :] = low
        part = three(x[:, cols], own[0, cols, :], own[1, cols, :])
        if i == 0:
            total[...] = part
        else:
            total[...] += part
    half = rows // 2
    here, there = member(), 1 - member()
    for out, which in ((keep, here), (send, there)):
        out[:half, :] = total[pl.ds(pl.multiple_of(which * half, 8), half), :]
        out[half : half + extra, :] = total[rows:, :]
        out[half + extra :, :] = jnp.zeros_like(out[half + extra :, :])
        out[half + extra : half + extra + 1, :] = diagonal[...]
        out[half + extra + 1 : half + extra + 2, :prim] = index[...].astype(f32)


def split(matrix, own, weights):
    here = member()
    weights[here] = own[...]
    top, low = halves(matrix[...])
    weights[1 - here, 0] = top
    weights[1 - here, 1] = low


def diagonals(keep, recv):
    place = keep.shape[0] - 8
    return pick(keep[place : place + 1, :], recv[place : place + 1, :])


def start_chain(keep, recv, *refs):
    weights, (f_first, f_second) = refs[:PARTS], refs[PARTS:]
    rows = f_first.shape[0]

    @pl.when(pair() == 0)
    def _():
        first, second = pick(keep[:rows, :], recv[:rows, :])
        f_first[...] = first
        f_second[...] = second + times(first, weights, 1)


def start_last(keep, recv, *refs):
    weights, (f_first, f_second, k_first, k_second) = refs[:PARTS], refs[PARTS:]
    rows, extra = f_first.shape[0], k_first.shape[0]
    stop = keep.shape[0] - 8

    @pl.when(pair() == 0)
    def _():
        at = stop - extra - rows
        first, second = pick(keep[at:stop, :], recv[at:stop, :])
        second = second + times(first, weights, 1)
        f_first[...] = first[:rows]
        f_second[...] = second[:rows]
        k_first[...] = first[rows:]
        k_second[...] = second[rows:]


def top_one(at, keep, recv, carried, *refs):
    weights, (n_first, n_second) = refs[:PARTS], refs[PARTS:]
    rows = n_first.shape[0]

    @pl.when(pair() == 1)
    def _():
        first, second = pick(keep[at : at + rows, :], recv[at : at + rows, :])
        first = first + times(carried[...], weights, 0)
        second = second + times(first, weights, 1)
        n_first[...] = first + times(second, weights, 0)
        n_second[...] = second


def top_two(with_basis, keep, recv, v_first, v_second, carried, *refs):
    riding, weights, (n_first, n_second) = refs[0], refs[1 : 1 + PARTS], refs[1 + PARTS :]
    rows = v_first.shape[0]
    few = riding.shape[0] // 2
    extra = 2 * few
    at = keep.shape[0] - 8 - extra

    @pl.when(pair() == 1)
    def _():
        d_first, d_second = diagonals(keep, recv)
        x = d_first * v_first[...] + carried[...]
        if with_basis:
            here = pl.ds(pl.multiple_of(at + member() * few, 8), few)
            k_first, k_second = pick(keep[here, :], recv[here, :])
            first = times(jnp.concatenate([x, riding[few:, :]], axis=0), weights, 0)
            k_first = first[rows:] + k_first
            y = d_second * v_second[...] + first[:rows]
            second = times(jnp.concatenate([y, k_first], axis=0), weights, 1)
            first = jnp.concatenate([first[:rows], k_first], axis=0)
            second = jnp.concatenate([second[:rows], second[rows:] + k_second], axis=0)
        else:
            first = times(x, weights, 0)
            second = times(d_second * v_second[...] + first, weights, 1)
        n_first[...] = first + times(second, weights, 0)
        n_second[...] = second


def down(f_first, f_second, carried, weights):
    second = f_second + times(carried, weights, 1)
    return f_first + times(second, weights, 0), second


def turn(keep, recv, f_first, f_second, carried, *refs):
    weights, old = refs[:PARTS], refs[PARTS : PARTS + 2]
    n_first, n_second, g_first, g_second = refs[PARTS + 2 :]

    @pl.when(pair() == 0)
    def _():
        first, second = down(f_first[...], f_second[...], carried[...], weights)
        n_second[...] = second
        n_first[...] = first
        d_first, d_second = diagonals(keep, recv)
        again = times(d_first * first, weights, 0)
        g_first[...] = again
        g_second[...] = times(d_second * second + again, weights, 1)

    hold(pair() != 0, old, (n_first, n_second))


def back(with_basis, f_first, f_second, k_first, k_second, carried, *refs):
    weights, old, (n_first, n_second) = refs[:PARTS], refs[PARTS : PARTS + 2], refs[PARTS + 2 :]
    few = k_first.shape[0] // 2

    @pl.when(pair() == 0)
    def _():
        first, second = f_first[...], f_second[...]
        if with_basis:
            here = pl.ds(pl.multiple_of(member() * few, 8), few)
            first = jnp.concatenate([first, k_first[here, :]], axis=0)
            second = jnp.concatenate([second, k_second[here, :]], axis=0)
        n_first[...], n_second[...] = down(first, second, carried[...], weights)

    hold(pair() != 0, old, (n_first, n_second))


def adjoint_start(own_spots, oth_spots, k_second, *refs):
    weights, (y_first, y_second, sent) = refs[:PARTS], refs[PARTS:]
    prim = y_first.shape[0]

    @pl.when(pair() == 0)
    def _():
        first, second = pick(own_spots[...], oth_spots[...])
        second = second + times_transposed(first, weights, 0)
        y_first[...] = first
        y_second[...] = second
        sent[:prim, :] = times_transposed(second, weights, 1)
        sent[prim:, :] = k_second[pl.ds(pl.multiple_of(member() * prim, 8), prim), :]


def placed(u, places, width):
    prim = u.shape[0]
    zero = jnp.zeros_like(u)
    rows = [u if i in places else zero for i in range(width // prim)]
    return jnp.concatenate(rows, axis=0)


def score(x, u):
    top, low = halves(u)
    return three(x, top, low, dot_rows)


def only(x, place, prim):
    lane = lax.broadcasted_iota(jnp.int32, x.shape, 1)
    return jnp.where((lane >= place * prim) & (lane < (place + 1) * prim), x, 0.0)


def pack(values, out, at):
    rows, width = values.shape
    per = out.shape[1] // width
    for j in range(rows // 8):
        row = at + (j // per) * 8
        out[row : row + 8, (j % per) * width : (j % per + 1) * width] = values[8 * j : 8 * j + 8, :]


def unpack(packed, at, rows, width):
    per = packed.shape[1] // width
    return jnp.concatenate(
        [
            packed[
                at + (j // per) * 8 : at + (j // per) * 8 + 8,
                (j % per) * width : (j % per + 1) * width,
            ]
            for j in range(rows // 8)
        ],
        axis=0,
    )


def adjoint_top(width, keep, recv, own_spots, oth_spots, carried, *refs):
    weights, refs = refs[:PARTS], refs[PARTS:]
    blocks, old, (y_first, y_second, sent) = refs[: 2 * BLOCKS], refs[2 * BLOCKS : -3], refs[-3:]
    prim = y_first.shape[0]

    @pl.when(pair() == 1)
    def _():
        first, second = pick(own_spots[...], oth_spots[...])
        first = first + carried[:prim, :]
        second = second + times_transposed(first, weights, 0)
        z_second = times_transposed(second, weights, 1)
        first = first + z_second
        z_first = times_transposed(first, weights, 0)
        sent[:prim, :] = z_first
        w_first, w_second = pick(keep[...], recv[...])
        stop = w_first.shape[0] - 8
        w = score(w_first[:stop], placed(first, (0, 2), width)) + score(
            w_second[:stop], placed(second, (0, 2), width)
        )
        d_first, d_second = diagonals(keep, recv)
        n_first = jnp.concatenate([r[...] for r in blocks[0::2]], axis=0)
        n_second = jnp.concatenate([r[...] for r in blocks[1::2]], axis=0)
        g = score(d_first * n_first, placed(z_first, (1,), width)) + score(
            d_second * n_second, placed(z_second, (1,), width)
        )
        half = n_first.shape[0]
        pack(only(w[:half], 0, prim) + g + only(w[half:], 2, prim), sent, prim)

    hold(pair() != 1, old, (y_first, y_second))


def score_turn(subs, carried, schur, maps, inverse, y_first, y_second, k_first, k_second, *refs):
    blocks, copies, values = refs[:-2], refs[-2], refs[-1]
    prim = y_first.shape[0]
    width = values.shape[1]
    half = BLOCKS * blocks[0].shape[0]
    share = inverse.shape[0]

    @pl.when(pair() == 0)
    def _():
        first = jnp.concatenate(
            [r[...] for r in blocks[0::4]] + [k_first[...]] + [r[...] for r in blocks[2::4]], axis=0
        )
        second = jnp.concatenate(
            [r[...] for r in blocks[1::4]] + [k_second[...]] + [r[...] for r in blocks[3::4]], axis=0
        )
        w = score(first, placed(y_first[...], (0, 1, 2), width)) + score(
            second, placed(y_second[...] + carried[:prim, :], (0, 1, 2), width)
        )
        extra = k_first.shape[0]
        values[:half, :] = (
            unpack(carried, prim, half, width)
            + only(w[:half], 0, prim)
            + only(w[half : half + extra], 2, prim)
            + only(w[half + extra :], 1, prim)
        )
        values[:prim, 3 * prim : 4 * prim] = schur[...]
        values[prim : prim + 1, 3 * prim : 4 * prim] = maps[...]
        for i in range(inverse.shape[1] // width):
            values[half + i * share : half + (i + 1) * share, :] = inverse[:, i * width : (i + 1) * width]
        for j in range(subs):
            copies[j] = values[...]


def settle(*refs):
    blocks, (keep, send) = refs[: 4 * BLOCKS], refs[4 * BLOCKS :]
    rows = blocks[0].shape[0]
    for i in range(BLOCKS):
        a1, b1, a2, b2 = blocks[4 * i : 4 * i + 4]
        here = slice(i * rows, (i + 1) * rows)
        keep[here, :], send[here, :] = pick(
            2.0 * a1[...] - a2[:rows, :], 2.0 * b1[...] - b2[:rows, :]
        )
    keep[BLOCKS * rows :, :], send[BLOCKS * rows :, :] = pick(blocks[2][rows:, :], blocks[3][rows:, :])


def wide(x, rows):
    return jnp.concatenate([x, jnp.zeros((rows - x.shape[0], x.shape[1]), f32)], axis=0)


def solve(prim, share, values, q):
    @pl.when(pair() == 0)
    def _():
        half, width = q.shape
        subs, height = values.shape[:2]
        count = subs * share
        unknown = lax.broadcasted_iota(jnp.int32, (count, width), 0).astype(f32)
        lane = lax.broadcasted_iota(jnp.int32, (half, width), 1)

        def at(j):
            return values[j, :half, :]

        def share_of(j):
            return jnp.concatenate(
                [values[j, i : i + share, :] for i in range(half, height, share)], axis=1
            )

        def loop(body, begin):
            if subs <= 8:
                for j in range(subs):
                    begin = body(j, begin)
                return begin
            return lax.fori_loop(0, subs, body, begin)

        def times_rows(left, right):
            top, low = halves(right)
            return three(left, top, low, dot_rows)

        def times_plain(left, right):
            top, low = halves(right)
            return three(left, top, low)

        def map_of(v):
            row = pltpu.roll(v[prim : prim + 8, :], width - 3 * prim, 1)[0:1]
            return jnp.where(lane[0:1] < prim, row, -1.0)

        def times_schur(left, v, signs):
            rows = [v[:prim] if sign > 0 else -v[:prim] for sign in signs]
            out = times_plain(left, wide(jnp.concatenate(rows, axis=0), width))
            return jnp.where(lane < prim, pltpu.roll(out, width - 3 * prim, 1), 0.0)

        def spot(row, ids):
            return (ids == row).astype(f32)

        def pick_plain(left, spots):
            top, low = halves(left)
            both = dot(jnp.concatenate([top, low], axis=0), spots.astype(bf16))
            return both[:half] + both[half:]

        def pick_rows(left, spots):
            top, low = halves(left)
            both = dot_rows(jnp.concatenate([top, low], axis=0), spots.astype(bf16))
            return both[:half] + both[half:]

        def add_first(j, total):
            v = at(j)
            return total + pick_rows(v, spot(map_of(v), unknown))

        inverse = jnp.concatenate([share_of(j) for j in range(subs)], axis=0)
        zero = jnp.zeros((half, count), f32)
        found = times_rows(loop(add_first, zero), inverse)

        def parts(j):
            v = at(j)
            row = map_of(v)
            first = pick_plain(found, spot(pltpu.roll(row, prim, 1), unknown)) - times_schur(v, v, (1,))
            change = times_plain(first, wide(v[: 2 * prim], width))
            return v, row, first, jnp.where(lane < 2 * prim, v, change)

        def add_second(j, total):
            _, row, _, p = parts(j)
            signs = (
                spot(row, unknown)
                - spot(pltpu.roll(row, prim, 1), unknown)
                - spot(pltpu.roll(row, 2 * prim, 1), unknown)
            )
            return total + pick_rows(p, signs)

        found_two = times_rows(loop(add_second, zero), inverse)
        v, row, first, p = parts(lax.axis_index("sub"))
        second = pick_plain(found_two, spot(pltpu.roll(row, prim, 1), unknown)) - times_schur(
            p, v, (1, -1, -1)
        )
        q[...] = first + pltpu.roll(first + second, 2 * prim, 1)


def solve_packed(prim, share, values, q):
    @pl.when(pair() == 0)
    def _():
        half, width = q.shape
        subs, height = values.shape[:2]
        count = subs * share
        per = width // prim
        total = subs * prim
        v = [values[j, :half, :] for j in range(subs)]
        inverse = jnp.concatenate(
            [
                jnp.concatenate(
                    [values[j, i : i + share, :] for i in range(half, height, share)], axis=1
                )
                for j in range(subs)
            ],
            axis=0,
        )

        def moved(x, group, j):
            shift = (j % per - group) * prim % width
            x = pltpu.roll(x, shift, 1) if shift else x
            lane = lax.broadcasted_iota(jnp.int32, x.shape, 1)
            place = j % per * prim
            return jnp.where((lane >= place) & (lane < place + prim), x, 0.0)

        def side_by_side(pieces, group):
            spans = []
            for start in range(0, subs, per):
                span = moved(pieces[start], group, start)
                for j in range(start + 1, start + per):
                    span = span + moved(pieces[j], group, j)
                spans.append(span)
            return jnp.concatenate(spans, axis=1)

        def diagonal(pieces, group):
            rows = []
            for j, piece in enumerate(pieces):
                zero = jnp.zeros((prim, width), f32)
                spans = [zero] * (subs // per)
                spans[j // per] = moved(piece, group, j)
                rows.append(jnp.concatenate(spans, axis=1))
            return halves(jnp.concatenate(rows, axis=0))

        p_one = side_by_side(v, 0)
        p_shift = side_by_side(v, 1)
        row = side_by_side([x[prim : prim + 8] for x in v], 3)[0:1]
        unknown = lax.broadcasted_iota(jnp.int32, (count, total), 0).astype(f32)
        spots = (unknown == row).astype(f32).astype(bf16)
        schur = diagonal([x[:prim] for x in v], 3)
        x_one = diagonal([x[:prim] for x in v], 2)
        x_two = diagonal([x[prim : 2 * prim] for x in v], 2)
        top, low = halves(inverse)

        def exact(left, how):
            a, b = halves(left)
            both = how(jnp.concatenate([a, b], axis=0), spots)
            return both[:half] + both[half:]

        def found_of(p):
            return three(exact(p, dot_rows), top, low, dot_rows)

        multiplier = three(p_one, *schur)
        base = p_one - p_shift + three(multiplier, *x_one)
        picked = exact(found_of(p_one), dot)
        p_two = base - three(picked, *x_two)
        multiplier_two = three(p_two, *schur)
        picked_two = exact(found_of(p_two), dot)
        me = lax.axis_index("sub")
        lane = lax.broadcasted_iota(jnp.int32, (half, total), 1)
        mine = (lane >= me * prim) & (lane < (me + 1) * prim)

        def own(x):
            x = jnp.where(mine, x, 0.0)
            span = x[:, :width]
            for start in range(width, total, width):
                span = span + x[:, start : start + width]
            out = span
            for k in range(1, per):
                out = out + pltpu.roll(span, width - k * prim, 1)
            first = lax.broadcasted_iota(jnp.int32, out.shape, 1) < prim
            return jnp.where(first, out, 0.0)

        one = pltpu.roll(own(picked), prim, 1) - own(multiplier)
        two = pltpu.roll(own(picked_two), prim, 1) - own(multiplier_two)
        q[...] = one + pltpu.roll(one + two, 2 * prim, 1)


def finish(keep, recv, q_keep, q_recv, one, two, out):
    prim = one.shape[0]
    rows = keep.shape[0] - prim
    k_low, k_high = pick(keep[rows:, :], recv[rows:, :])
    right = jnp.concatenate([-k_low, -k_high, one[...], two[...]], axis=0)
    top, low = halves(right)
    here = member()
    for n, q, which in ((keep, q_keep, here), (recv, q_recv, 1 - here)):
        out[pl.ds(pl.multiple_of(which * rows, 8), rows), :] = n[:rows, :] + three(q[...], top, low)


def on_device(
    residual,
    inverse_slab,
    diagonal,
    primal_index,
    coarse_map,
    schur_small,
    constraint_basis,
    coarse_basis,
    coarse_inverse,
):
    levels = lax.axis_size("slab")
    subs = lax.axis_size("sub")
    assert levels == 4

    def swap(x):
        return lax.ppermute(x, "slab", [(i, i ^ 1) for i in range(levels)])

    def rise(x):
        return lax.ppermute(x, "slab", [(0, 2), (1, 3)])

    def fall(x):
        return lax.ppermute(x, "slab", [(2, 0), (3, 1)])

    vector = residual[0, 0]
    matrix = inverse_slab[0, 0]
    one, two = constraint_basis[0, 0], coarse_basis[0, 0]
    rows, size = vector.shape
    prim = primal_index.shape[-1]
    coarse_count, share = coarse_inverse.shape
    half = rows // 2
    block = half // BLOCKS
    extra = 2 * prim
    width = -(-3 * prim // LANES) * LANES
    packed = -(-half * width // (8 * size)) * 8
    assert half == extra and prim <= coarse_count and size % width == 0 and 4 * prim <= width and coarse_count % width == 0

    def like(count, *heights):
        return [struct((h, size)) for h in heights for _ in range(count)]

    other_matrix = swap(matrix)

    own, keep, send = call(
        first_products,
        [struct((2, size, size), bf16)] + like(2, half + extra + 8),
        [matrix, vector, one, two, diagonal[0], primal_index[0]],
        2,
        scratch=[
            pltpu.VMEM((size, size), f32),
            pltpu.VMEM((rows + extra, size), f32),
            pltpu.VMEM((rows + extra, size), f32),
            pltpu.VMEM((1, size), f32),
            pltpu.VMEM((1, prim), jnp.int32),
            pltpu.SemaphoreType.DMA((5 + PIECES,)),
        ],
        hbm=(0, 1, 2, 3, 4, 5),
    )
    recv = swap(send)
    weights = call(split, [struct((2, 2, size, size), bf16)], [other_matrix, own], 1)
    place = jnp.arange(size, dtype=jnp.int32)
    own_spots = (primal_index[0, 0][:, None] == place).astype(f32)
    oth_spots = (recv[half + extra + 1, :prim][:, None] == place.astype(f32)).astype(f32)

    span = range(BLOCKS)
    f, carried = [], []
    for i in span[:-1]:
        f.append(call(start_chain, like(2, block), [keep, recv, *weights], 1))
        carried.append(rise(f[i][1]))
    *f_last, k_first, k_second = call(start_last, like(2, block, extra), [keep, recv, *weights], 1)
    f.append(f_last)
    carried.append(rise(f_last[1]))
    y_first, y_second, sent = call(
        adjoint_start,
        like(2, prim) + like(1, 2 * prim),
        [own_spots, oth_spots, k_second, *weights],
        2,
    )
    riding = rise(sent)

    n = []
    for i in span:
        n.append(
            call(
                functools.partial(top_one, i * block),
                like(2, block),
                [keep, recv, carried[i], *weights],
                3,
            )
        )
        carried[i] = fall(n[i][0])
    n_one, g = [], []
    for i in span:
        turned = call(
            turn,
            like(4, block),
            [keep, recv, *f[i], carried[i], *weights, *n[i]],
            4,
            aliases={5 + PARTS: 0, 6 + PARTS: 1},
        )
        n_one.append(turned[:2])
        g.append(turned[2:])
        carried[i] = rise(g[i][1])
        if i == 0:
            passed = [x for j in span for x in (n_one[0] if j == 0 else n[j])]
            y_first, y_second, sent = call(
                functools.partial(adjoint_top, width),
                like(2, prim) + like(1, prim + packed),
                [keep, recv, own_spots, oth_spots, riding, *weights, *passed, y_first, y_second],
                4,
                aliases={5 + PARTS + 2 * BLOCKS: 0, 6 + PARTS + 2 * BLOCKS: 1},
            )
            z_back = fall(sent)
    pieces = []
    for i in span:
        pieces += [*f[i], *g[i]]
    height = half + coarse_count // width * share
    (values,) = call(
        functools.partial(score_turn, subs),
        [struct((subs, height, width))],
        [
            z_back,
            schur_small[0],
            coarse_map.astype(f32),
            coarse_inverse.T,
            y_first,
            y_second,
            k_first,
            k_second,
            *pieces,
        ],
        1,
        scratch=[pltpu.VMEM((height, width), f32)],
    )
    values = lax.all_to_all(values, "sub", 0, 0)

    n_two = []
    for i in span:
        n_two.append(
            call(
                functools.partial(top_two, i == 0),
                like(2, block + prim if i == 0 else block),
                [keep, recv, *n_one[i], carried[i], riding, *weights],
                3,
            )
        )
        carried[i] = fall(n_two[i][0])
    for i in span:
        n_two[i] = call(
            functools.partial(back, i == 0),
            like(2, block + prim if i == 0 else block),
            [*g[i], k_first, k_second, carried[i], *weights, *n_two[i]],
            2,
            aliases={5 + PARTS: 0, 6 + PARTS: 1},
        )
    pieces = []
    for i in span:
        pieces += [*n_one[i], *n_two[i]]
    m_keep, m_send = call(settle, like(2, half + prim), pieces, 0.5)
    m_recv = swap(m_send)

    packs = subs <= 8 and width % prim == 0 and subs % (width // prim) == 0
    (q,) = call(
        functools.partial(solve_packed if packs else solve, prim, share),
        [struct((half, width))],
        [values],
        0.5,
        limit=VMEM_LIMIT + 8 * values.size,
    )
    q_upper = rise(q)
    q = jnp.where(pair() == 0, q, q_upper)
    q_recv = swap(q)
    (out,) = call(finish, [struct((rows, size))], [m_keep, m_recv, q, q_recv, one, two], 0.5)
    return out[None, None]


def solution(mesh):
    placed_as = (
        P("sub", "slab", None, None),
        P("sub", "slab", None, None),
        P("sub", "slab", None),
        P("sub", "slab", None),
        P("sub", None),
        P("sub", None, None),
        P("sub", "slab", None, None),
        P("sub", "slab", None, None),
        P(None, "sub"),
    )

    return jax.shard_map(
        on_device,
        mesh=mesh,
        in_specs=placed_as,
        out_specs=P("sub", "slab", None, None),
        check_vma=False,
    )
```

```python
import functools

import jax
import jax.numpy as jnp
from jax import lax
from jax.experimental import pallas as pl
from jax.experimental.pallas import tpu as pltpu
from jax.sharding import PartitionSpec as P


f32 = jnp.float32
bf16 = jnp.bfloat16
LANES = 128
SPLIT = (1, 3)
BLOCKS = len(SPLIT)
PIECES = 4
PARTS = 1


def halves(x):
    top = x.astype(bf16)
    return top, (x - top.astype(f32)).astype(bf16)


def dot(left, right):
    return jnp.dot(left, right, preferred_element_type=f32)


def dot_rows(left, right):
    return lax.dot_general(left, right, (((1,), (1,)), ((), ())), preferred_element_type=f32)


def three(x, top_right, low_right, how=dot):
    rows = x.shape[0]
    top, low = halves(x)
    both = how(jnp.concatenate([top, low], axis=0), top_right)
    return both[:rows] + both[rows:] + how(top, low_right)


def times(x, weights, member):
    step = weights[0].shape[2]
    top, low = halves(x)
    both = jnp.concatenate([top, low], axis=0)
    rows = x.shape[0]
    first, second = 0.0, 0.0
    for i, piece in enumerate(weights):
        cols = slice(i * step, (i + 1) * step)
        first = first + dot(both[:, cols], piece[member, 0])
        second = second + dot(top[:, cols], piece[member, 1])
    return first[:rows] + first[rows:] + second


def times_transposed(x, weights, member):
    return jnp.concatenate(
        [three(x, piece[member, 0], piece[member, 1], dot_rows) for piece in weights], axis=1
    )


def member():
    return lax.axis_index("slab") & 1


def pair():
    return lax.axis_index("slab") >> 1


def spec(space):
    return pl.BlockSpec(memory_space=space)


def call(body, outs, args, work, aliases=None, scratch=(), hbm=(), limit=None):
    specs = [spec(pltpu.VMEM) for _ in args]
    args = list(args)
    for place in hbm:
        specs[place] = spec(pltpu.HBM)
        args[place] = pltpu.with_memory_space_constraint(args[place], pltpu.HBM)
    return pl.pallas_call(
        body,
        out_shape=outs,
        in_specs=specs,
        out_specs=[spec(pltpu.VMEM) for _ in outs],
        input_output_aliases=aliases or {},
        scratch_shapes=list(scratch),
        cost_estimate=pl.CostEstimate(flops=int(work * 8e8), bytes_accessed=0, transcendentals=0),
        compiler_params=pltpu.CompilerParams(vmem_limit_bytes=limit or VMEM_LIMIT),
    )(*args)


VMEM_LIMIT = 16 << 20


def struct(shape, dtype=f32):
    return jax.ShapeDtypeStruct(shape, dtype)


def pick(own, oth):
    first = member() == 0
    return jnp.where(first, own, oth), jnp.where(first, oth, own)


def hold(idle, before, after):
    @pl.when(idle)
    def _():
        for old, new in zip(before, after):
            new[...] = old[...]


def first_products(
    matrix, vector, one, two, diagonal_far, index_far, own, keep, send, buffer, x, total, diagonal, index, sems
):
    size = matrix.shape[0]
    step = size // PIECES
    rows, prim = vector.shape[0], one.shape[0]
    extra = 2 * prim
    copies = [
        pltpu.make_async_copy(vector, x.at[pl.ds(0, rows)], sems.at[0]),
        pltpu.make_async_copy(one, x.at[pl.ds(rows, prim)], sems.at[1]),
        pltpu.make_async_copy(two, x.at[pl.ds(rows + prim, prim)], sems.at[2]),
        pltpu.make_async_copy(diagonal_far, diagonal, sems.at[3]),
        pltpu.make_async_copy(index_far, index, sems.at[4]),
    ]
    pieces = [
        pltpu.make_async_copy(
            matrix.at[pl.ds(i * step, step)], buffer.at[pl.ds(i * step, step)], sems.at[5 + i]
        )
        for i in range(PIECES)
    ]
    for copy in copies + pieces:
        copy.start()
    for copy in copies:
        copy.wait()
    x[rows:, :] = x[rows:, :] * diagonal[...]
    for i, copy in enumerate(pieces):
        cols = pl.ds(i * step, step)
        copy.wait()
        top, low = halves(buffer[cols, :])
        own[0, cols, :] = top
        own[1, cols, :] = low
        part = three(x[:, cols], own[0, cols, :], own[1, cols, :])
        if i == 0:
            total[...] = part
        else:
            total[...] += part
    half = rows // 2
    here, there = member(), 1 - member()
    for out, which in ((keep, here), (send, there)):
        out[:half, :] = total[pl.ds(pl.multiple_of(which * half, 8), half), :]
        out[half : half + extra, :] = total[rows:, :]
        out[half + extra :, :] = jnp.zeros_like(out[half + extra :, :])
        out[half + extra : half + extra + 1, :] = diagonal[...]
        out[half + extra + 1 : half + extra + 2, :prim] = index[...].astype(f32)


def split(matrix, own, weights):
    here = member()
    weights[here] = own[...]
    top, low = halves(matrix[...])
    weights[1 - here, 0] = top
    weights[1 - here, 1] = low


def diagonals(keep, recv):
    place = keep.shape[0] - 8
    return pick(keep[place : place + 1, :], recv[place : place + 1, :])


def start_chain(keep, recv, *refs):
    weights, (f_first, f_second) = refs[:PARTS], refs[PARTS:]
    rows = f_first.shape[0]

    @pl.when(pair() == 0)
    def _():
        first, second = pick(keep[:rows, :], recv[:rows, :])
        f_first[...] = first
        f_second[...] = second + times(first, weights, 1)


def start_last(keep, recv, *refs):
    weights, (f_first, f_second, k_first, k_second) = refs[:PARTS], refs[PARTS:]
    rows, extra = f_first.shape[0], k_first.shape[0]
    stop = keep.shape[0] - 8

    @pl.when(pair() == 0)
    def _():
        at = stop - extra - rows
        first, second = pick(keep[at:stop, :], recv[at:stop, :])
        second = second + times(first, weights, 1)
        f_first[...] = first[:rows]
        f_second[...] = second[:rows]
        k_first[...] = first[rows:]
        k_second[...] = second[rows:]


def top_one(at, keep, recv, carried, *refs):
    weights, (n_first, n_second) = refs[:PARTS], refs[PARTS:]
    rows = n_first.shape[0]

    @pl.when(pair() == 1)
    def _():
        first, second = pick(keep[at : at + rows, :], recv[at : at + rows, :])
        first = first + times(carried[...], weights, 0)
        second = second + times(first, weights, 1)
        n_first[...] = first + times(second, weights, 0)
        n_second[...] = second


def top_two(with_basis, keep, recv, v_first, v_second, carried, *refs):
    weights, (n_first, n_second) = refs[:PARTS], refs[PARTS:]
    rows = v_first.shape[0]
    few = carried.shape[0] - rows
    extra = 2 * few
    at = keep.shape[0] - 8 - extra

    @pl.when(pair() == 1)
    def _():
        d_first, d_second = diagonals(keep, recv)
        x = d_first * v_first[...] + carried[:rows, :]
        if with_basis:
            here = pl.ds(pl.multiple_of(at + member() * few, 8), few)
            k_first, k_second = pick(keep[here, :], recv[here, :])
            first = times(jnp.concatenate([x, carried[rows:, :]], axis=0), weights, 0)
            k_first = first[rows:] + k_first
            y = d_second * v_second[...] + first[:rows]
            second = times(jnp.concatenate([y, k_first], axis=0), weights, 1)
            first = jnp.concatenate([first[:rows], k_first], axis=0)
            second = jnp.concatenate([second[:rows], second[rows:] + k_second], axis=0)
        else:
            first = times(x, weights, 0)
            second = times(d_second * v_second[...] + first, weights, 1)
        n_first[...] = first + times(second, weights, 0)
        n_second[...] = second


def down(f_first, f_second, carried, weights):
    second = f_second + times(carried, weights, 1)
    return f_first + times(second, weights, 0), second


def turn(keep, recv, f_first, f_second, k_second, carried, *refs):
    weights, old = refs[:PARTS], refs[PARTS : PARTS + 2]
    n_first, n_second, g_first, g_second, *sent = refs[PARTS + 2 :]

    @pl.when(pair() == 0)
    def _():
        first, second = down(f_first[...], f_second[...], carried[...], weights)
        n_second[...] = second
        n_first[...] = first
        d_first, d_second = diagonals(keep, recv)
        again = times(d_first * first, weights, 0)
        g_first[...] = again
        last = times(d_second * second + again, weights, 1)
        g_second[...] = last
        for out in sent:
            rows = last.shape[0]
            few = out.shape[0] - rows
            out[:rows, :] = last
            out[rows:, :] = k_second[pl.ds(pl.multiple_of(member() * few, 8), few), :]

    hold(pair() != 0, old, (n_first, n_second))


def back(with_basis, f_first, f_second, k_first, k_second, carried, *refs):
    weights, old, (n_first, n_second) = refs[:PARTS], refs[PARTS : PARTS + 2], refs[PARTS + 2 :]
    few = k_first.shape[0] // 2

    @pl.when(pair() == 0)
    def _():
        first, second = f_first[...], f_second[...]
        if with_basis:
            here = pl.ds(pl.multiple_of(member() * few, 8), few)
            first = jnp.concatenate([first, k_first[here, :]], axis=0)
            second = jnp.concatenate([second, k_second[here, :]], axis=0)
        n_first[...], n_second[...] = down(first, second, carried[...], weights)

    hold(pair() != 0, old, (n_first, n_second))


def adjoint_start(own_spots, oth_spots, *refs):
    weights, (y_first, y_second, sent) = refs[:PARTS], refs[PARTS:]

    @pl.when(pair() == 0)
    def _():
        first, second = pick(own_spots[...], oth_spots[...])
        second = second + times_transposed(first, weights, 0)
        y_first[...] = first
        y_second[...] = second
        sent[...] = times_transposed(second, weights, 1)


def placed(u, places, width):
    prim = u.shape[0]
    zero = jnp.zeros_like(u)
    rows = [u if i in places else zero for i in range(width // prim)]
    return jnp.concatenate(rows, axis=0)


def score(x, u):
    top, low = halves(u)
    return three(x, top, low, dot_rows)


def only(x, place, prim):
    lane = lax.broadcasted_iota(jnp.int32, x.shape, 1)
    return jnp.where((lane >= place * prim) & (lane < (place + 1) * prim), x, 0.0)


def pack(values, out, at):
    rows, width = values.shape
    per = out.shape[1] // width
    for j in range(rows // 8):
        row = at + (j // per) * 8
        out[row : row + 8, (j % per) * width : (j % per + 1) * width] = values[8 * j : 8 * j + 8, :]


def unpack(packed, at, rows, width):
    per = packed.shape[1] // width
    return jnp.concatenate(
        [
            packed[
                at + (j // per) * 8 : at + (j // per) * 8 + 8,
                (j % per) * width : (j % per + 1) * width,
            ]
            for j in range(rows // 8)
        ],
        axis=0,
    )


def adjoint_top(width, keep, recv, own_spots, oth_spots, carried, *refs):
    weights, refs = refs[:PARTS], refs[PARTS:]
    blocks, old, (y_first, y_second, sent) = refs[: 2 * BLOCKS], refs[2 * BLOCKS : -3], refs[-3:]
    prim = y_first.shape[0]

    @pl.when(pair() == 1)
    def _():
        first, second = pick(own_spots[...], oth_spots[...])
        first = first + carried[...]
        second = second + times_transposed(first, weights, 0)
        z_second = times_transposed(second, weights, 1)
        first = first + z_second
        z_first = times_transposed(first, weights, 0)
        sent[:prim, :] = z_first
        w_first, w_second = pick(keep[...], recv[...])
        stop = w_first.shape[0] - 8
        w = score(w_first[:stop], placed(first, (0, 2), width)) + score(
            w_second[:stop], placed(second, (0, 2), width)
        )
        d_first, d_second = diagonals(keep, recv)
        n_first = jnp.concatenate([r[...] for r in blocks[0::2]], axis=0)
        n_second = jnp.concatenate([r[...] for r in blocks[1::2]], axis=0)
        g = score(d_first * n_first, placed(z_first, (1,), width)) + score(
            d_second * n_second, placed(z_second, (1,), width)
        )
        half = n_first.shape[0]
        pack(only(w[:half], 0, prim) + g + only(w[half:], 2, prim), sent, prim)

    hold(pair() != 1, old, (y_first, y_second))


def score_turn(subs, carried, schur, maps, inverse, y_first, y_second, k_first, k_second, *refs):
    blocks, copies, values = refs[:-2], refs[-2], refs[-1]
    prim = y_first.shape[0]
    width = values.shape[1]
    half = sum(r.shape[0] for r in blocks[0::4])
    share = inverse.shape[0]

    @pl.when(pair() == 0)
    def _():
        first = jnp.concatenate(
            [r[...] for r in blocks[0::4]] + [k_first[...]] + [r[...] for r in blocks[2::4]], axis=0
        )
        second = jnp.concatenate(
            [r[...] for r in blocks[1::4]] + [k_second[...]] + [r[...] for r in blocks[3::4]], axis=0
        )
        w = score(first, placed(y_first[...], (0, 1, 2), width)) + score(
            second, placed(y_second[...] + carried[:prim, :], (0, 1, 2), width)
        )
        extra = k_first.shape[0]
        values[:half, :] = (
            unpack(carried, prim, half, width)
            + only(w[:half], 0, prim)
            + only(w[half : half + extra], 2, prim)
            + only(w[half + extra :], 1, prim)
        )
        values[:prim, 3 * prim : 4 * prim] = schur[...]
        values[prim : prim + 1, 3 * prim : 4 * prim] = maps[...]
        for i in range(inverse.shape[1] // width):
            values[half + i * share : half + (i + 1) * share, :] = inverse[:, i * width : (i + 1) * width]
        for j in range(subs):
            copies[j] = values[...]


def settle(*refs):
    blocks, (keep, send) = refs[: 4 * BLOCKS], refs[4 * BLOCKS :]
    at = 0
    for i in range(BLOCKS):
        a1, b1, a2, b2 = blocks[4 * i : 4 * i + 4]
        rows = a1.shape[0]
        keep[at : at + rows, :], send[at : at + rows, :] = pick(
            2.0 * a1[...] - a2[:rows, :], 2.0 * b1[...] - b2[:rows, :]
        )
        at += rows
    rows = blocks[0].shape[0]
    keep[at:, :], send[at:, :] = pick(blocks[2][rows:, :], blocks[3][rows:, :])


def wide(x, rows):
    return jnp.concatenate([x, jnp.zeros((rows - x.shape[0], x.shape[1]), f32)], axis=0)


def solve(prim, share, values, q):
    @pl.when(pair() == 0)
    def _():
        half, width = q.shape
        subs, height = values.shape[:2]
        count = subs * share
        unknown = lax.broadcasted_iota(jnp.int32, (count, width), 0).astype(f32)
        lane = lax.broadcasted_iota(jnp.int32, (half, width), 1)

        def at(j):
            return values[j, :half, :]

        def share_of(j):
            return jnp.concatenate(
                [values[j, i : i + share, :] for i in range(half, height, share)], axis=1
            )

        def loop(body, begin):
            if subs <= 8:
                for j in range(subs):
                    begin = body(j, begin)
                return begin
            return lax.fori_loop(0, subs, body, begin)

        def times_rows(left, right):
            top, low = halves(right)
            return three(left, top, low, dot_rows)

        def times_plain(left, right):
            top, low = halves(right)
            return three(left, top, low)

        def map_of(v):
            row = pltpu.roll(v[prim : prim + 8, :], width - 3 * prim, 1)[0:1]
            return jnp.where(lane[0:1] < prim, row, -1.0)

        def times_schur(left, v, signs):
            rows = [v[:prim] if sign > 0 else -v[:prim] for sign in signs]
            out = times_plain(left, wide(jnp.concatenate(rows, axis=0), width))
            return jnp.where(lane < prim, pltpu.roll(out, width - 3 * prim, 1), 0.0)

        def spot(row, ids):
            return (ids == row).astype(f32)

        def pick_plain(left, spots):
            top, low = halves(left)
            both = dot(jnp.concatenate([top, low], axis=0), spots.astype(bf16))
            return both[:half] + both[half:]

        def pick_rows(left, spots):
            top, low = halves(left)
            both = dot_rows(jnp.concatenate([top, low], axis=0), spots.astype(bf16))
            return both[:half] + both[half:]

        def add_first(j, total):
            v = at(j)
            return total + pick_rows(v, spot(map_of(v), unknown))

        inverse = jnp.concatenate([share_of(j) for j in range(subs)], axis=0)
        zero = jnp.zeros((half, count), f32)
        found = times_rows(loop(add_first, zero), inverse)

        def parts(j):
            v = at(j)
            row = map_of(v)
            first = pick_plain(found, spot(pltpu.roll(row, prim, 1), unknown)) - times_schur(v, v, (1,))
            change = times_plain(first, wide(v[: 2 * prim], width))
            return v, row, first, jnp.where(lane < 2 * prim, v, change)

        def add_second(j, total):
            _, row, _, p = parts(j)
            signs = (
                spot(row, unknown)
                - spot(pltpu.roll(row, prim, 1), unknown)
                - spot(pltpu.roll(row, 2 * prim, 1), unknown)
            )
            return total + pick_rows(p, signs)

        found_two = times_rows(loop(add_second, zero), inverse)
        v, row, first, p = parts(lax.axis_index("sub"))
        second = pick_plain(found_two, spot(pltpu.roll(row, prim, 1), unknown)) - times_schur(
            p, v, (1, -1, -1)
        )
        q[...] = first + pltpu.roll(first + second, 2 * prim, 1)


def solve_packed(prim, share, values, q):
    @pl.when(pair() == 0)
    def _():
        half, width = q.shape
        subs, height = values.shape[:2]
        count = subs * share
        per = width // prim
        total = subs * prim
        v = [values[j, :half, :] for j in range(subs)]
        inverse = jnp.concatenate(
            [
                jnp.concatenate(
                    [values[j, i : i + share, :] for i in range(half, height, share)], axis=1
                )
                for j in range(subs)
            ],
            axis=0,
        )

        def moved(x, group, j):
            shift = (j % per - group) * prim % width
            x = pltpu.roll(x, shift, 1) if shift else x
            lane = lax.broadcasted_iota(jnp.int32, x.shape, 1)
            place = j % per * prim
            return jnp.where((lane >= place) & (lane < place + prim), x, 0.0)

        def side_by_side(pieces, group):
            spans = []
            for start in range(0, subs, per):
                span = moved(pieces[start], group, start)
                for j in range(start + 1, start + per):
                    span = span + moved(pieces[j], group, j)
                spans.append(span)
            return jnp.concatenate(spans, axis=1)

        def diagonal(pieces, group):
            rows = []
            for j, piece in enumerate(pieces):
                zero = jnp.zeros((prim, width), f32)
                spans = [zero] * (subs // per)
                spans[j // per] = moved(piece, group, j)
                rows.append(jnp.concatenate(spans, axis=1))
            return halves(jnp.concatenate(rows, axis=0))

        p_one = side_by_side(v, 0)
        p_shift = side_by_side(v, 1)
        row = side_by_side([x[prim : prim + 8] for x in v], 3)[0:1]
        unknown = lax.broadcasted_iota(jnp.int32, (count, total), 0).astype(f32)
        spots = (unknown == row).astype(f32).astype(bf16)
        schur = diagonal([x[:prim] for x in v], 3)
        x_one = diagonal([x[:prim] for x in v], 2)
        x_two = diagonal([x[prim : 2 * prim] for x in v], 2)
        top, low = halves(inverse)

        def exact(left, how):
            a, b = halves(left)
            both = how(jnp.concatenate([a, b], axis=0), spots)
            return both[:half] + both[half:]

        def found_of(p):
            return three(exact(p, dot_rows), top, low, dot_rows)

        multiplier = three(p_one, *schur)
        base = p_one - p_shift + three(multiplier, *x_one)
        picked = exact(found_of(p_one), dot)
        p_two = base - three(picked, *x_two)
        multiplier_two = three(p_two, *schur)
        picked_two = exact(found_of(p_two), dot)
        me = lax.axis_index("sub")
        lane = lax.broadcasted_iota(jnp.int32, (half, total), 1)
        mine = (lane >= me * prim) & (lane < (me + 1) * prim)

        def own(x):
            x = jnp.where(mine, x, 0.0)
            span = x[:, :width]
            for start in range(width, total, width):
                span = span + x[:, start : start + width]
            out = span
            for k in range(1, per):
                out = out + pltpu.roll(span, width - k * prim, 1)
            first = lax.broadcasted_iota(jnp.int32, out.shape, 1) < prim
            return jnp.where(first, out, 0.0)

        one = pltpu.roll(own(picked), prim, 1) - own(multiplier)
        two = pltpu.roll(own(picked_two), prim, 1) - own(multiplier_two)
        q[...] = one + pltpu.roll(one + two, 2 * prim, 1)


def finish(keep, recv, q_keep, q_recv, one, two, out):
    prim = one.shape[0]
    rows = keep.shape[0] - prim
    k_low, k_high = pick(keep[rows:, :], recv[rows:, :])
    right = jnp.concatenate([-k_low, -k_high, one[...], two[...]], axis=0)
    top, low = halves(right)
    here = member()
    for n, q, which in ((keep, q_keep, here), (recv, q_recv, 1 - here)):
        out[pl.ds(pl.multiple_of(which * rows, 8), rows), :] = n[:rows, :] + three(q[...], top, low)


def on_device(
    residual,
    inverse_slab,
    diagonal,
    primal_index,
    coarse_map,
    schur_small,
    constraint_basis,
    coarse_basis,
    coarse_inverse,
):
    levels = lax.axis_size("slab")
    subs = lax.axis_size("sub")
    assert levels == 4

    def swap(x):
        return lax.ppermute(x, "slab", [(i, i ^ 1) for i in range(levels)])

    def rise(x):
        return lax.ppermute(x, "slab", [(0, 2), (1, 3)])

    def fall(x):
        return lax.ppermute(x, "slab", [(2, 0), (3, 1)])

    vector = residual[0, 0]
    matrix = inverse_slab[0, 0]
    one, two = constraint_basis[0, 0], coarse_basis[0, 0]
    rows, size = vector.shape
    prim = primal_index.shape[-1]
    coarse_count, share = coarse_inverse.shape
    half = rows // 2
    sizes = [half * part // sum(SPLIT) for part in SPLIT]
    starts = [sum(sizes[:i]) for i in range(BLOCKS)]
    extra = 2 * prim
    width = -(-3 * prim // LANES) * LANES
    packed = -(-half * width // (8 * size)) * 8
    assert half == extra and prim <= coarse_count and size % width == 0 and 4 * prim <= width and coarse_count % width == 0

    def like(count, *heights):
        return [struct((h, size)) for h in heights for _ in range(count)]

    other_matrix = swap(matrix)

    own, keep, send = call(
        first_products,
        [struct((2, size, size), bf16)] + like(2, half + extra + 8),
        [matrix, vector, one, two, diagonal[0], primal_index[0]],
        2,
        scratch=[
            pltpu.VMEM((size, size), f32),
            pltpu.VMEM((rows + extra, size), f32),
            pltpu.VMEM((rows + extra, size), f32),
            pltpu.VMEM((1, size), f32),
            pltpu.VMEM((1, prim), jnp.int32),
            pltpu.SemaphoreType.DMA((5 + PIECES,)),
        ],
        hbm=(0, 1, 2, 3, 4, 5),
    )
    recv = swap(send)
    weights = call(split, [struct((2, 2, size, size), bf16)], [other_matrix, own], 1)
    place = jnp.arange(size, dtype=jnp.int32)
    own_spots = (primal_index[0, 0][:, None] == place).astype(f32)
    oth_spots = (recv[half + extra + 1, :prim][:, None] == place.astype(f32)).astype(f32)

    span = range(BLOCKS)
    last = BLOCKS - 1
    f, carried = [], []
    for i in span[:-1]:
        f.append(call(start_chain, like(2, sizes[i]), [keep, recv, *weights], 1))
        carried.append(rise(f[i][1]))
    *f_last, k_first, k_second = call(
        start_last, like(2, sizes[last], extra), [keep, recv, *weights], 1
    )
    f.append(f_last)
    carried.append(rise(f_last[1]))
    y_first, y_second, sent = call(
        adjoint_start, like(3, prim), [own_spots, oth_spots, *weights], 2
    )
    riding = rise(sent)

    n = []
    for i in span:
        n.append(
            call(
                functools.partial(top_one, starts[i]),
                like(2, sizes[i]),
                [keep, recv, carried[i], *weights],
                3,
            )
        )
        carried[i] = fall(n[i][0])
    n_one, g = [], []
    for i in span:
        turned = call(
            turn,
            like(4, sizes[i]) + (like(1, sizes[i] + prim) if i == 0 else []),
            [keep, recv, *f[i], k_second, carried[i], *weights, *n[i]],
            4,
            aliases={6 + PARTS: 0, 7 + PARTS: 1},
        )
        n_one.append(turned[:2])
        g.append(turned[2:4])
        carried[i] = rise(turned[-1])
        if i == 0:
            passed = [x for j in span for x in (n_one[0] if j == 0 else n[j])]
            y_first, y_second, sent = call(
                functools.partial(adjoint_top, width),
                like(2, prim) + like(1, prim + packed),
                [keep, recv, own_spots, oth_spots, riding, *weights, *passed, y_first, y_second],
                4,
                aliases={5 + PARTS + 2 * BLOCKS: 0, 6 + PARTS + 2 * BLOCKS: 1},
            )
            z_back = fall(sent)
    pieces = []
    for i in span:
        pieces += [*f[i], *g[i]]
    height = half + coarse_count // width * share
    (values,) = call(
        functools.partial(score_turn, subs),
        [struct((subs, height, width))],
        [
            z_back,
            schur_small[0],
            coarse_map.astype(f32),
            coarse_inverse.T,
            y_first,
            y_second,
            k_first,
            k_second,
            *pieces,
        ],
        1,
        scratch=[pltpu.VMEM((height, width), f32)],
    )
    values = lax.all_to_all(values, "sub", 0, 0)

    n_two = []
    for i in span:
        n_two.append(
            call(
                functools.partial(top_two, i == 0),
                like(2, sizes[i] + prim if i == 0 else sizes[i]),
                [keep, recv, *n_one[i], carried[i], *weights],
                3,
            )
        )
        carried[i] = fall(n_two[i][0])
    for i in span:
        n_two[i] = call(
            functools.partial(back, i == 0),
            like(2, sizes[i] + prim if i == 0 else sizes[i]),
            [*g[i], k_first, k_second, carried[i], *weights, *n_two[i]],
            2,
            aliases={5 + PARTS: 0, 6 + PARTS: 1},
        )
    pieces = []
    for i in span:
        pieces += [*n_one[i], *n_two[i]]
    m_keep, m_send = call(settle, like(2, half + prim), pieces, 0.5)
    m_recv = swap(m_send)

    packs = subs <= 8 and width % prim == 0 and subs % (width // prim) == 0
    (q,) = call(
        functools.partial(solve_packed if packs else solve, prim, share),
        [struct((half, width))],
        [values],
        0.5,
        limit=VMEM_LIMIT + 8 * values.size,
    )
    q_upper = rise(q)
    q = jnp.where(pair() == 0, q, q_upper)
    q_recv = swap(q)
    (out,) = call(finish, [struct((rows, size))], [m_keep, m_recv, q, q_recv, one, two], 0.5)
    return out[None, None]


def solution(mesh):
    placed_as = (
        P("sub", "slab", None, None),
        P("sub", "slab", None, None),
        P("sub", "slab", None),
        P("sub", "slab", None),
        P("sub", None),
        P("sub", None, None),
        P("sub", "slab", None, None),
        P("sub", "slab", None, None),
        P(None, "sub"),
    )

    return jax.shard_map(
        on_device,
        mesh=mesh,
        in_specs=placed_as,
        out_specs=P("sub", "slab", None, None),
        check_vma=False,
    )
```

```python
import functools

import jax
import jax.numpy as jnp
from jax import lax
from jax.experimental import pallas as pl
from jax.experimental.pallas import tpu as pltpu
from jax.sharding import PartitionSpec as P


f32 = jnp.float32
bf16 = jnp.bfloat16
LANES = 128
SPLIT = (1, 3)
BLOCKS = len(SPLIT)
PIECES = 4
PARTS = 1


def halves(x):
    top = x.astype(bf16)
    return top, (x - top.astype(f32)).astype(bf16)


def dot(left, right):
    return jnp.dot(left, right, preferred_element_type=f32)


def dot_rows(left, right):
    return lax.dot_general(left, right, (((1,), (1,)), ((), ())), preferred_element_type=f32)


def three(x, top_right, low_right, how=dot):
    rows = x.shape[0]
    top, low = halves(x)
    both = how(jnp.concatenate([top, low], axis=0), top_right)
    return both[:rows] + both[rows:] + how(top, low_right)


def times(x, weights, member):
    step = weights[0].shape[2]
    top, low = halves(x)
    both = jnp.concatenate([top, low], axis=0)
    rows = x.shape[0]
    first, second = 0.0, 0.0
    for i, piece in enumerate(weights):
        cols = slice(i * step, (i + 1) * step)
        first = first + dot(both[:, cols], piece[member, 0])
        second = second + dot(top[:, cols], piece[member, 1])
    return first[:rows] + first[rows:] + second


def times_transposed(x, weights, member):
    return jnp.concatenate(
        [three(x, piece[member, 0], piece[member, 1], dot_rows) for piece in weights], axis=1
    )


def member():
    return lax.axis_index("slab") & 1


def pair():
    return lax.axis_index("slab") >> 1


def spec(space):
    return pl.BlockSpec(memory_space=space)


def call(body, outs, args, work, aliases=None, scratch=(), hbm=(), limit=None):
    specs = [spec(pltpu.VMEM) for _ in args]
    args = list(args)
    for place in hbm:
        specs[place] = spec(pltpu.HBM)
        args[place] = pltpu.with_memory_space_constraint(args[place], pltpu.HBM)
    return pl.pallas_call(
        body,
        out_shape=outs,
        in_specs=specs,
        out_specs=[spec(pltpu.VMEM) for _ in outs],
        input_output_aliases=aliases or {},
        scratch_shapes=list(scratch),
        cost_estimate=pl.CostEstimate(flops=int(work * 8e8), bytes_accessed=0, transcendentals=0),
        compiler_params=pltpu.CompilerParams(vmem_limit_bytes=limit or VMEM_LIMIT),
    )(*args)


VMEM_LIMIT = 16 << 20


def struct(shape, dtype=f32):
    return jax.ShapeDtypeStruct(shape, dtype)


def pick(own, oth):
    first = member() == 0
    return jnp.where(first, own, oth), jnp.where(first, oth, own)


def hold(idle, before, after):
    @pl.when(idle)
    def _():
        for old, new in zip(before, after):
            new[...] = old[...]


def first_products(
    matrix, vector, one, two, diagonal_far, index_far, own, keep, send, buffer, x, total, diagonal, index, sems
):
    size = matrix.shape[0]
    step = size // PIECES
    rows, prim = vector.shape[0], one.shape[0]
    extra = 2 * prim
    copies = [
        pltpu.make_async_copy(vector, x.at[pl.ds(0, rows)], sems.at[0]),
        pltpu.make_async_copy(one, x.at[pl.ds(rows, prim)], sems.at[1]),
        pltpu.make_async_copy(two, x.at[pl.ds(rows + prim, prim)], sems.at[2]),
        pltpu.make_async_copy(diagonal_far, diagonal, sems.at[3]),
        pltpu.make_async_copy(index_far, index, sems.at[4]),
    ]
    pieces = [
        pltpu.make_async_copy(
            matrix.at[pl.ds(i * step, step)], buffer.at[pl.ds(i * step, step)], sems.at[5 + i]
        )
        for i in range(PIECES)
    ]
    for copy in copies + pieces:
        copy.start()
    for copy in copies:
        copy.wait()
    x[rows:, :] = x[rows:, :] * diagonal[...]
    for i, copy in enumerate(pieces):
        cols = pl.ds(i * step, step)
        copy.wait()
        top, low = halves(buffer[cols, :])
        own[0, cols, :] = top
        own[1, cols, :] = low
        part = three(x[:, cols], own[0, cols, :], own[1, cols, :])
        if i == 0:
            total[...] = part
        else:
            total[...] += part
    half = rows // 2
    here, there = member(), 1 - member()
    for out, which in ((keep, here), (send, there)):
        out[:half, :] = total[pl.ds(pl.multiple_of(which * half, 8), half), :]
        out[half : half + extra, :] = total[rows:, :]
        out[half + extra :, :] = jnp.zeros_like(out[half + extra :, :])
        out[half + extra : half + extra + 1, :] = diagonal[...]
        out[half + extra + 1 : half + extra + 2, :prim] = index[...].astype(f32)


def split(matrix, own, weights):
    here = member()
    weights[here] = own[...]
    top, low = halves(matrix[...])
    weights[1 - here, 0] = top
    weights[1 - here, 1] = low


def diagonals(keep, recv):
    place = keep.shape[0] - 8
    return pick(keep[place : place + 1, :], recv[place : place + 1, :])


def start_chain(keep, recv, *refs):
    weights, (f_first, f_second) = refs[:PARTS], refs[PARTS:]
    rows = f_first.shape[0]

    @pl.when(pair() == 0)
    def _():
        first, second = pick(keep[:rows, :], recv[:rows, :])
        f_first[...] = first
        f_second[...] = second + times(first, weights, 1)


def start_last(keep, recv, *refs):
    weights, (f_first, f_second, k_first, k_second) = refs[:PARTS], refs[PARTS:]
    rows, extra = f_first.shape[0], k_first.shape[0]
    stop = keep.shape[0] - 8

    @pl.when(pair() == 0)
    def _():
        at = stop - extra - rows
        first, second = pick(keep[at:stop, :], recv[at:stop, :])
        second = second + times(first, weights, 1)
        f_first[...] = first[:rows]
        f_second[...] = second[:rows]
        k_first[...] = first[rows:]
        k_second[...] = second[rows:]


def top_one(at, keep, recv, carried, *refs):
    weights, (n_first, n_second) = refs[:PARTS], refs[PARTS:]
    rows = n_first.shape[0]

    @pl.when(pair() == 1)
    def _():
        first, second = pick(keep[at : at + rows, :], recv[at : at + rows, :])
        first = first + times(carried[...], weights, 0)
        second = second + times(first, weights, 1)
        n_first[...] = first + times(second, weights, 0)
        n_second[...] = second


def top_two(with_basis, keep, recv, v_first, v_second, carried, *refs):
    weights, (n_first, n_second) = refs[:PARTS], refs[PARTS:]
    rows = v_first.shape[0]
    few = carried.shape[0] - rows
    extra = 2 * few
    at = keep.shape[0] - 8 - extra

    @pl.when(pair() == 1)
    def _():
        d_first, d_second = diagonals(keep, recv)
        x = d_first * v_first[...] + carried[:rows, :]
        if with_basis:
            here = pl.ds(pl.multiple_of(at + member() * few, 8), few)
            k_first, k_second = pick(keep[here, :], recv[here, :])
            first = times(jnp.concatenate([x, carried[rows:, :]], axis=0), weights, 0)
            k_first = first[rows:] + k_first
            y = d_second * v_second[...] + first[:rows]
            second = times(jnp.concatenate([y, k_first], axis=0), weights, 1)
            first = jnp.concatenate([first[:rows], k_first], axis=0)
            second = jnp.concatenate([second[:rows], second[rows:] + k_second], axis=0)
        else:
            first = times(x, weights, 0)
            second = times(d_second * v_second[...] + first, weights, 1)
        n_first[...] = first + times(second, weights, 0)
        n_second[...] = second


def down(f_first, f_second, carried, weights):
    second = f_second + times(carried, weights, 1)
    return f_first + times(second, weights, 0), second


def turn(keep, recv, f_first, f_second, k_second, carried, *refs):
    weights, old = refs[:PARTS], refs[PARTS : PARTS + 2]
    n_first, n_second, g_first, g_second, *sent = refs[PARTS + 2 :]

    @pl.when(pair() == 0)
    def _():
        first, second = down(f_first[...], f_second[...], carried[...], weights)
        n_second[...] = second
        n_first[...] = first
        d_first, d_second = diagonals(keep, recv)
        again = times(d_first * first, weights, 0)
        g_first[...] = again
        last = times(d_second * second + again, weights, 1)
        g_second[...] = last
        for out in sent:
            rows = last.shape[0]
            few = out.shape[0] - rows
            out[:rows, :] = last
            out[rows:, :] = k_second[pl.ds(pl.multiple_of(member() * few, 8), few), :]

    hold(pair() != 0, old, (n_first, n_second))


def back(with_basis, f_first, f_second, k_first, k_second, carried, *refs):
    weights, old, (n_first, n_second) = refs[:PARTS], refs[PARTS : PARTS + 2], refs[PARTS + 2 :]
    few = k_first.shape[0] // 2

    @pl.when(pair() == 0)
    def _():
        first, second = f_first[...], f_second[...]
        if with_basis:
            here = pl.ds(pl.multiple_of(member() * few, 8), few)
            first = jnp.concatenate([first, k_first[here, :]], axis=0)
            second = jnp.concatenate([second, k_second[here, :]], axis=0)
        n_first[...], n_second[...] = down(first, second, carried[...], weights)

    hold(pair() != 0, old, (n_first, n_second))


def adjoint_start(own_spots, oth_spots, *refs):
    weights, (y_first, y_second, sent) = refs[:PARTS], refs[PARTS:]

    @pl.when(pair() == 0)
    def _():
        first, second = pick(own_spots[...], oth_spots[...])
        second = second + times_transposed(first, weights, 0)
        y_first[...] = first
        y_second[...] = second
        sent[...] = times_transposed(second, weights, 1)


def placed(u, places, width):
    prim = u.shape[0]
    zero = jnp.zeros_like(u)
    rows = [u if i in places else zero for i in range(width // prim)]
    return jnp.concatenate(rows, axis=0)


def score(x, u):
    top, low = halves(u)
    return three(x, top, low, dot_rows)


def only(x, place, prim):
    lane = lax.broadcasted_iota(jnp.int32, x.shape, 1)
    return jnp.where((lane >= place * prim) & (lane < (place + 1) * prim), x, 0.0)


def pack(values, out, at):
    rows, width = values.shape
    per = out.shape[1] // width
    for j in range(rows // 8):
        row = at + (j // per) * 8
        out[row : row + 8, (j % per) * width : (j % per + 1) * width] = values[8 * j : 8 * j + 8, :]


def unpack(packed, at, rows, width):
    per = packed.shape[1] // width
    return jnp.concatenate(
        [
            packed[
                at + (j // per) * 8 : at + (j // per) * 8 + 8,
                (j % per) * width : (j % per + 1) * width,
            ]
            for j in range(rows // 8)
        ],
        axis=0,
    )


def adjoint_top(width, keep, recv, own_spots, oth_spots, carried, *refs):
    weights, refs = refs[:PARTS], refs[PARTS:]
    blocks, old, (y_first, y_second, sent) = refs[: 2 * BLOCKS], refs[2 * BLOCKS : -3], refs[-3:]
    prim = y_first.shape[0]

    @pl.when(pair() == 1)
    def _():
        first, second = pick(own_spots[...], oth_spots[...])
        first = first + carried[...]
        second = second + times_transposed(first, weights, 0)
        z_second = times_transposed(second, weights, 1)
        first = first + z_second
        z_first = times_transposed(first, weights, 0)
        sent[:prim, :] = z_first
        w_first, w_second = pick(keep[...], recv[...])
        stop = w_first.shape[0] - 8
        w = score(w_first[:stop], placed(first, (0, 2), width)) + score(
            w_second[:stop], placed(second, (0, 2), width)
        )
        d_first, d_second = diagonals(keep, recv)
        n_first = jnp.concatenate([r[...] for r in blocks[0::2]], axis=0)
        n_second = jnp.concatenate([r[...] for r in blocks[1::2]], axis=0)
        g = score(d_first * n_first, placed(z_first, (1,), width)) + score(
            d_second * n_second, placed(z_second, (1,), width)
        )
        half = n_first.shape[0]
        pack(only(w[:half], 0, prim) + g + only(w[half:], 2, prim), sent, prim)

    hold(pair() != 1, old, (y_first, y_second))


def score_turn(subs, carried, schur, maps, inverse, y_first, y_second, k_first, k_second, *refs):
    blocks, copies, values = refs[:-2], refs[-2], refs[-1]
    prim = y_first.shape[0]
    width = values.shape[1]
    half = sum(r.shape[0] for r in blocks[0::4])
    share = inverse.shape[0]

    @pl.when(pair() == 0)
    def _():
        first = jnp.concatenate(
            [r[...] for r in blocks[0::4]] + [k_first[...]] + [r[...] for r in blocks[2::4]], axis=0
        )
        second = jnp.concatenate(
            [r[...] for r in blocks[1::4]] + [k_second[...]] + [r[...] for r in blocks[3::4]], axis=0
        )
        w = score(first, placed(y_first[...], (0, 1, 2), width)) + score(
            second, placed(y_second[...] + carried[:prim, :], (0, 1, 2), width)
        )
        extra = k_first.shape[0]
        values[:half, :] = (
            unpack(carried, prim, half, width)
            + only(w[:half], 0, prim)
            + only(w[half : half + extra], 2, prim)
            + only(w[half + extra :], 1, prim)
        )
        values[:prim, 3 * prim : 4 * prim] = schur[...]
        values[prim : prim + 1, 3 * prim : 4 * prim] = maps[...]
        for i in range(inverse.shape[1] // width):
            values[half + i * share : half + (i + 1) * share, :] = inverse[:, i * width : (i + 1) * width]
        for j in range(subs):
            copies[j] = values[...]


def settle(*refs):
    blocks, (keep, send) = refs[: 4 * BLOCKS], refs[4 * BLOCKS :]
    at = 0
    for i in range(BLOCKS):
        a1, b1, a2, b2 = blocks[4 * i : 4 * i + 4]
        rows = a1.shape[0]
        keep[at : at + rows, :], send[at : at + rows, :] = pick(
            2.0 * a1[...] - a2[:rows, :], 2.0 * b1[...] - b2[:rows, :]
        )
        at += rows
    rows = blocks[0].shape[0]
    keep[at:, :], send[at:, :] = pick(blocks[2][rows:, :], blocks[3][rows:, :])


def wide(x, rows):
    return jnp.concatenate([x, jnp.zeros((rows - x.shape[0], x.shape[1]), f32)], axis=0)


def solve(prim, share, values, q):
    @pl.when(pair() == 0)
    def _():
        half, width = q.shape
        subs, height = values.shape[:2]
        count = subs * share
        unknown = lax.broadcasted_iota(jnp.int32, (count, width), 0).astype(f32)
        lane = lax.broadcasted_iota(jnp.int32, (half, width), 1)

        def at(j):
            return values[j, :half, :]

        def share_of(j):
            return jnp.concatenate(
                [values[j, i : i + share, :] for i in range(half, height, share)], axis=1
            )

        def loop(body, begin):
            if subs <= 8:
                for j in range(subs):
                    begin = body(j, begin)
                return begin
            return lax.fori_loop(0, subs, body, begin)

        def times_rows(left, right):
            top, low = halves(right)
            return three(left, top, low, dot_rows)

        def times_plain(left, right):
            top, low = halves(right)
            return three(left, top, low)

        def map_of(v):
            row = pltpu.roll(v[prim : prim + 8, :], width - 3 * prim, 1)[0:1]
            return jnp.where(lane[0:1] < prim, row, -1.0)

        def times_schur(left, v, signs):
            rows = [v[:prim] if sign > 0 else -v[:prim] for sign in signs]
            out = times_plain(left, wide(jnp.concatenate(rows, axis=0), width))
            return jnp.where(lane < prim, pltpu.roll(out, width - 3 * prim, 1), 0.0)

        def spot(row, ids):
            return (ids == row).astype(f32)

        def pick_plain(left, spots):
            top, low = halves(left)
            both = dot(jnp.concatenate([top, low], axis=0), spots.astype(bf16))
            return both[:half] + both[half:]

        def pick_rows(left, spots):
            top, low = halves(left)
            both = dot_rows(jnp.concatenate([top, low], axis=0), spots.astype(bf16))
            return both[:half] + both[half:]

        def add_first(j, total):
            v = at(j)
            return total + pick_rows(v, spot(map_of(v), unknown))

        inverse = jnp.concatenate([share_of(j) for j in range(subs)], axis=0)
        zero = jnp.zeros((half, count), f32)
        found = times_rows(loop(add_first, zero), inverse)

        def parts(j):
            v = at(j)
            row = map_of(v)
            first = pick_plain(found, spot(pltpu.roll(row, prim, 1), unknown)) - times_schur(v, v, (1,))
            change = times_plain(first, wide(v[: 2 * prim], width))
            return v, row, first, jnp.where(lane < 2 * prim, v, change)

        def add_second(j, total):
            _, row, _, p = parts(j)
            signs = (
                spot(row, unknown)
                - spot(pltpu.roll(row, prim, 1), unknown)
                - spot(pltpu.roll(row, 2 * prim, 1), unknown)
            )
            return total + pick_rows(p, signs)

        found_two = times_rows(loop(add_second, zero), inverse)
        v, row, first, p = parts(lax.axis_index("sub"))
        second = pick_plain(found_two, spot(pltpu.roll(row, prim, 1), unknown)) - times_schur(
            p, v, (1, -1, -1)
        )
        q[...] = first + pltpu.roll(first + second, 2 * prim, 1)


def solve_packed(prim, share, values, q):
    @pl.when(pair() == 0)
    def _():
        half, width = q.shape
        subs, height = values.shape[:2]
        count = subs * share
        per = width // prim
        total = subs * prim
        v = [values[j, :half, :] for j in range(subs)]
        inverse = jnp.concatenate(
            [
                jnp.concatenate(
                    [values[j, i : i + share, :] for i in range(half, height, share)], axis=1
                )
                for j in range(subs)
            ],
            axis=0,
        )

        def moved(x, group, j):
            shift = (j % per - group) * prim % width
            x = pltpu.roll(x, shift, 1) if shift else x
            lane = lax.broadcasted_iota(jnp.int32, x.shape, 1)
            place = j % per * prim
            return jnp.where((lane >= place) & (lane < place + prim), x, 0.0)

        def side_by_side(pieces, group):
            spans = []
            for start in range(0, subs, per):
                span = moved(pieces[start], group, start)
                for j in range(start + 1, start + per):
                    span = span + moved(pieces[j], group, j)
                spans.append(span)
            return jnp.concatenate(spans, axis=1)

        def diagonal(pieces, group):
            rows = []
            for j, piece in enumerate(pieces):
                zero = jnp.zeros((prim, width), f32)
                spans = [zero] * (subs // per)
                spans[j // per] = moved(piece, group, j)
                rows.append(jnp.concatenate(spans, axis=1))
            return halves(jnp.concatenate(rows, axis=0))

        p_one = side_by_side(v, 0)
        p_shift = side_by_side(v, 1)
        row = side_by_side([x[prim : prim + 8] for x in v], 3)[0:1]
        unknown = lax.broadcasted_iota(jnp.int32, (count, total), 0).astype(f32)
        spots = (unknown == row).astype(f32).astype(bf16)
        schur = diagonal([x[:prim] for x in v], 3)
        x_one = diagonal([x[:prim] for x in v], 2)
        x_two = diagonal([x[prim : 2 * prim] for x in v], 2)
        top, low = halves(inverse)

        def exact(left, how):
            a, b = halves(left)
            both = how(jnp.concatenate([a, b], axis=0), spots)
            return both[:half] + both[half:]

        def found_of(p):
            return three(exact(p, dot_rows), top, low, dot_rows)

        multiplier = three(p_one, *schur)
        base = p_one - p_shift + three(multiplier, *x_one)
        picked = exact(found_of(p_one), dot)
        p_two = base - three(picked, *x_two)
        multiplier_two = three(p_two, *schur)
        picked_two = exact(found_of(p_two), dot)
        me = lax.axis_index("sub")
        lane = lax.broadcasted_iota(jnp.int32, (half, total), 1)
        mine = (lane >= me * prim) & (lane < (me + 1) * prim)

        def own(x):
            x = jnp.where(mine, x, 0.0)
            span = x[:, :width]
            for start in range(width, total, width):
                span = span + x[:, start : start + width]
            out = span
            for k in range(1, per):
                out = out + pltpu.roll(span, width - k * prim, 1)
            first = lax.broadcasted_iota(jnp.int32, out.shape, 1) < prim
            return jnp.where(first, out, 0.0)

        one = pltpu.roll(own(picked), prim, 1) - own(multiplier)
        two = pltpu.roll(own(picked_two), prim, 1) - own(multiplier_two)
        q[...] = one + pltpu.roll(one + two, 2 * prim, 1)


def finish_own(keep, recv, q, one, two, part, top, low):
    prim = one.shape[0]
    rows = keep.shape[0] - prim
    k_low, k_high = pick(keep[rows:, :], recv[rows:, :])
    top[...], low[...] = halves(jnp.concatenate([-k_low, -k_high, one[...], two[...]], axis=0))
    part[...] = keep[:rows, :] + three(q[...], top[...], low[...])


def finish(part, recv, q, top, low, out):
    rows = part.shape[0]
    here = member()
    out[pl.ds(pl.multiple_of(here * rows, 8), rows), :] = part[...]
    out[pl.ds(pl.multiple_of((1 - here) * rows, 8), rows), :] = recv[:rows, :] + three(
        q[...], top[...], low[...]
    )


def on_device(
    residual,
    inverse_slab,
    diagonal,
    primal_index,
    coarse_map,
    schur_small,
    constraint_basis,
    coarse_basis,
    coarse_inverse,
):
    levels = lax.axis_size("slab")
    subs = lax.axis_size("sub")
    assert levels == 4

    def swap(x):
        return lax.ppermute(x, "slab", [(i, i ^ 1) for i in range(levels)])

    def rise(x):
        return lax.ppermute(x, "slab", [(0, 2), (1, 3)])

    def fall(x):
        return lax.ppermute(x, "slab", [(2, 0), (3, 1)])

    vector = residual[0, 0]
    matrix = inverse_slab[0, 0]
    one, two = constraint_basis[0, 0], coarse_basis[0, 0]
    rows, size = vector.shape
    prim = primal_index.shape[-1]
    coarse_count, share = coarse_inverse.shape
    half = rows // 2
    sizes = [half * part // sum(SPLIT) for part in SPLIT]
    starts = [sum(sizes[:i]) for i in range(BLOCKS)]
    extra = 2 * prim
    width = -(-3 * prim // LANES) * LANES
    packed = -(-half * width // (8 * size)) * 8
    assert half == extra and prim <= coarse_count and size % width == 0 and 4 * prim <= width and coarse_count % width == 0

    def like(count, *heights):
        return [struct((h, size)) for h in heights for _ in range(count)]

    other_matrix = swap(matrix)

    own, keep, send = call(
        first_products,
        [struct((2, size, size), bf16)] + like(2, half + extra + 8),
        [matrix, vector, one, two, diagonal[0], primal_index[0]],
        2,
        scratch=[
            pltpu.VMEM((size, size), f32),
            pltpu.VMEM((rows + extra, size), f32),
            pltpu.VMEM((rows + extra, size), f32),
            pltpu.VMEM((1, size), f32),
            pltpu.VMEM((1, prim), jnp.int32),
            pltpu.SemaphoreType.DMA((5 + PIECES,)),
        ],
        hbm=(0, 1, 2, 3, 4, 5),
    )
    recv = swap(send)
    weights = call(split, [struct((2, 2, size, size), bf16)], [other_matrix, own], 1)
    place = jnp.arange(size, dtype=jnp.int32)
    own_spots = (primal_index[0, 0][:, None] == place).astype(f32)
    oth_spots = (recv[half + extra + 1, :prim][:, None] == place.astype(f32)).astype(f32)

    span = range(BLOCKS)
    last = BLOCKS - 1
    f, carried = [], []
    for i in span[:-1]:
        f.append(call(start_chain, like(2, sizes[i]), [keep, recv, *weights], 1))
        carried.append(rise(f[i][1]))
    *f_last, k_first, k_second = call(
        start_last, like(2, sizes[last], extra), [keep, recv, *weights], 1
    )
    f.append(f_last)
    carried.append(rise(f_last[1]))
    y_first, y_second, sent = call(
        adjoint_start, like(3, prim), [own_spots, oth_spots, *weights], 2
    )
    riding = rise(sent)

    n = []
    for i in span:
        n.append(
            call(
                functools.partial(top_one, starts[i]),
                like(2, sizes[i]),
                [keep, recv, carried[i], *weights],
                3,
            )
        )
        carried[i] = fall(n[i][0])
    n_one, g = [], []
    for i in span:
        turned = call(
            turn,
            like(4, sizes[i]) + (like(1, sizes[i] + prim) if i == 0 else []),
            [keep, recv, *f[i], k_second, carried[i], *weights, *n[i]],
            4,
            aliases={6 + PARTS: 0, 7 + PARTS: 1},
        )
        n_one.append(turned[:2])
        g.append(turned[2:4])
        carried[i] = rise(turned[-1])
        if i == 0:
            passed = [x for j in span for x in (n_one[0] if j == 0 else n[j])]
            y_first, y_second, sent = call(
                functools.partial(adjoint_top, width),
                like(2, prim) + like(1, prim + packed),
                [keep, recv, own_spots, oth_spots, riding, *weights, *passed, y_first, y_second],
                4,
                aliases={5 + PARTS + 2 * BLOCKS: 0, 6 + PARTS + 2 * BLOCKS: 1},
            )
            z_back = fall(sent)
    pieces = []
    for i in span:
        pieces += [*f[i], *g[i]]
    height = half + coarse_count // width * share
    (values,) = call(
        functools.partial(score_turn, subs),
        [struct((subs, height, width))],
        [
            z_back,
            schur_small[0],
            coarse_map.astype(f32),
            coarse_inverse.T,
            y_first,
            y_second,
            k_first,
            k_second,
            *pieces,
        ],
        1,
        scratch=[pltpu.VMEM((height, width), f32)],
    )
    values = lax.all_to_all(values, "sub", 0, 0)

    n_two = []
    for i in span:
        n_two.append(
            call(
                functools.partial(top_two, i == 0),
                like(2, sizes[i] + prim if i == 0 else sizes[i]),
                [keep, recv, *n_one[i], carried[i], *weights],
                3,
            )
        )
        carried[i] = fall(n_two[i][0])
    for i in span:
        n_two[i] = call(
            functools.partial(back, i == 0),
            like(2, sizes[i] + prim if i == 0 else sizes[i]),
            [*g[i], k_first, k_second, carried[i], *weights, *n_two[i]],
            2,
            aliases={5 + PARTS: 0, 6 + PARTS: 1},
        )
    pieces = []
    for i in span:
        pieces += [*n_one[i], *n_two[i]]
    m_keep, m_send = call(settle, like(2, half + prim), pieces, 0.5)
    m_recv = swap(m_send)

    packs = subs <= 8 and width % prim == 0 and subs % (width // prim) == 0
    (q,) = call(
        functools.partial(solve_packed if packs else solve, prim, share),
        [struct((half, width))],
        [values],
        0.5,
        limit=VMEM_LIMIT + 8 * values.size,
    )
    q_upper = rise(q)
    q = jnp.where(pair() == 0, q, q_upper)
    q_recv = swap(q)
    part, top, low = call(
        finish_own,
        like(1, half) + [struct((4 * prim, size), bf16)] * 2,
        [m_keep, m_recv, q, one, two],
        0.3,
    )
    (out,) = call(finish, [struct((rows, size))], [part, m_recv, q_recv, top, low], 0.5)
    return out[None, None]


def solution(mesh):
    placed_as = (
        P("sub", "slab", None, None),
        P("sub", "slab", None, None),
        P("sub", "slab", None),
        P("sub", "slab", None),
        P("sub", None),
        P("sub", None, None),
        P("sub", "slab", None, None),
        P("sub", "slab", None, None),
        P(None, "sub"),
    )

    return jax.shard_map(
        on_device,
        mesh=mesh,
        in_specs=placed_as,
        out_specs=P("sub", "slab", None, None),
        check_vma=False,
    )
```
